32 devices in a mesh: dp: 16 (over z, y, x), mp: 2 (over core).
Axes of the slice: x: 2, y: 2, z: 4, core: 2. Of those that a mesh axis runs over, the one named last changes fastest.
Arguments:
- block_input: bfloat16 [4096, 1792], P(('dp', 'mp')), may hold values from -45 to 45
- attn_gain: bfloat16 [1792], P('dp'), may hold values from 0.25 to 1.75
- query_weight: bfloat16 [1792, 1024], P('dp', 'mp')
- key_weight: bfloat16 [1792, 128], P('dp', 'mp')
- value_weight: bfloat16 [1792, 128], P('dp', 'mp'), may hold values from -0.125 to 0.125
- output_weight: bfloat16 [1024, 1792], P(('mp', 'dp')), may hold values from -1.5 to 1.5
- ffn_gain: bfloat16 [1792], P('dp'), may hold values from 0.25 to 1.75
- gate_weight: bfloat16 [1792, 2816], P('dp', 'mp'), may hold values from -0.125 to 0.125
- up_weight: bfloat16 [1792, 2816], P('dp', 'mp'), may hold values from -0.125 to 0.125
- down_weight: bfloat16 [2816, 1792], P(('mp', 'dp')), may hold values from -0.109375 to 0.109375
- output_cotangent: bfloat16 [4096, 1792], P(('dp', 'mp')), may hold values from -6 to 6
Outputs:
- block_output: bfloat16 [4096, 1792], P(('dp', 'mp'))
- input_grad: float32 [4096, 1792], P(('dp', 'mp'))
- attn_gain_grad: float32 [1792], P('dp')
- query_grad: float32 [1792, 1024], P('dp', 'mp')
- key_grad: float32 [1792, 128], P('dp', 'mp')
- value_grad: float32 [1792, 128], P('dp', 'mp')
- output_weight_grad: float32 [1024, 1792], P(('mp', 'dp'))
- ffn_gain_grad: float32 [1792], P('dp')
- gate_grad: float32 [1792, 2816], P('dp', 'mp')
- up_grad: float32 [1792, 2816], P('dp', 'mp')
- down_grad: float32 [2816, 1792], P(('mp', 'dp'))
The draws below stay inside these ranges and needn't reach their ends.
All inputs are finite; a program needn't handle non-finite values.
Results may differ from the reference program's by a relative error of at most 0.012.
The reference program's roundings to bfloat16 on the way count: a program that leaves them out, or rounds other values in their place, can miss the bound.
Values may be sent and summed in bfloat16 or wider, within the bound.
A program may use at most 128 MiB of HBM per device.

```python
import jax
import jax.numpy as jnp
from jax import lax

D = 1792
HQ = 16
KV = 2
HD = 64
FF = 2816
LEN = 256
TOKENS = 4096
N_DP = 16


def draw_block_input(key, part):
    base_key = jax.random.fold_in(key, 101)
    base = jnp.clip(jax.random.normal(base_key, (TOKENS, D), jnp.float32), -4.0, 4.0)
    row_scale = jnp.exp(jax.random.uniform(jax.random.fold_in(key, 102), (TOKENS, 1), jnp.float32, -1.2, 1.2))
    column_scale = jnp.exp(jax.random.uniform(jax.random.fold_in(key, 103), (1, D), jnp.float32, -1.2, 1.2))
    return (base * row_scale * column_scale).astype(jnp.bfloat16)


def paired_projection(key):
    query_part = jnp.clip(jax.random.normal(jax.random.fold_in(key, 201), (D, HQ * HD), jnp.float32), -4.0, 4.0) * D ** (-0.5)
    key_part = jnp.clip(jax.random.normal(jax.random.fold_in(key, 202), (D, KV * HD), jnp.float32), -4.0, 4.0) * D ** (-0.5)
    return (query_part, key_part)


def draw_query_weight(key, part):
    return paired_projection(key)[0].astype(jnp.bfloat16)


def draw_key_weight(key, part):
    return paired_projection(key)[1].astype(jnp.bfloat16)


def with_spikes(entries, stream_key, source, target, blocks, factor):
    owner, partner = [(jnp.arange(entries.shape[dim]) // (entries.shape[dim] // blocks)).reshape([-1 if axis == dim else 1 for axis in range(entries.ndim)]) for dim in (source, target)]
    chosen = jax.random.permutation(stream_key, blocks)[partner]
    strong = (owner == chosen) | (owner == (partner + blocks // 2) % blocks)
    return jnp.where(strong, factor * entries, entries)


def steps_of(rng, dims, pieces, smallest, largest):
    level = 1.0
    for axis_at, shards_of in pieces:
        draws = jax.random.uniform(jax.random.fold_in(jax.random.fold_in(rng, 6), axis_at), (shards_of,), jnp.float32, smallest / len(pieces), largest / len(pieces))
        level = level * jnp.repeat(jnp.exp(draws), dims[axis_at] // shards_of).reshape((-1,) + (1,) * (len(dims) - 1 - axis_at))
    return level


def bell_draw(own_key, dims, spread, reach, cuts=(), kind=jnp.bfloat16):
    array = spread * jax.random.normal(own_key, dims, jnp.float32)
    if cuts:
        array = array * steps_of(own_key, dims, cuts, -0.22, 0.18)
    return jnp.clip(array, -reach, reach).astype(kind)


def noise_with(rng, dims, spread, limit, pieces, heavy, held_as=jnp.bfloat16):
    values = spread * jax.random.normal(rng, dims, jnp.float32)
    if pieces:
        values = values * steps_of(rng, dims, pieces, -0.22, 0.18)
    return jnp.clip(with_spikes(values, jax.random.fold_in(rng, 3), *heavy), -limit, limit).astype(held_as)


def setup_inputs(seed: int = 0) -> dict:
    key_of = jax.random.split(jax.random.key(seed), 12)
    block_input = draw_block_input(jax.random.fold_in(key_of[11], 71), 0)
    attn_gain = jnp.clip(1.0 + 0.15 * jax.random.normal(key_of[1], (D,), jnp.float32), 0.25, 1.75).astype(jnp.bfloat16)
    query_weight = draw_query_weight(jax.random.fold_in(key_of[11], 71), 0)
    key_weight = draw_key_weight(jax.random.fold_in(key_of[11], 71), 0)
    value_weight = bell_draw(key_of[4], (D, KV * HD), D ** -0.5, 0.125, ((0, 16), (1, 2)))
    output_weight = bell_draw(key_of[5], (HQ * HD, D), (HQ * HD * 4 // LEN) ** -0.5, 1.5, ((0, 32),))
    ffn_gain = jnp.clip(1.0 + 0.15 * jax.random.normal(key_of[6], (D,), jnp.float32), 0.25, 1.75).astype(jnp.bfloat16)
    gate_weight = bell_draw(key_of[7], (D, FF), D ** -0.5, 0.125, ((0, 16), (1, 2)))
    up_weight = bell_draw(key_of[8], (D, FF), D ** -0.5, 0.125, ((0, 16), (1, 2)))
    down_weight = bell_draw(key_of[9], (FF, D), FF ** -0.5, 0.109375, ((0, 32),))
    output_cotangent = noise_with(key_of[10], (TOKENS, D), 1.0, 6.0, ((0, 32),), (0, 1, 32, 2.75))
    return {"block_input": block_input, "attn_gain": attn_gain, "query_weight": query_weight, "key_weight": key_weight, "value_weight": value_weight, "output_weight": output_weight, "ffn_gain": ffn_gain, "gate_weight": gate_weight, "up_weight": up_weight, "down_weight": down_weight, "output_cotangent": output_cotangent}


EPSILON = 1e-05
ROPE_BASE = 10000.0

def rope_tables(length, head_dim):
    half_dim = head_dim // 2
    position = jnp.arange(length, dtype=jnp.float32)
    inverse = ROPE_BASE ** (-(jnp.arange(half_dim, dtype=jnp.float32) * (2.0 / head_dim)))
    angle = position[:, None] * inverse[None, :]
    return (jnp.cos(angle), jnp.sin(angle))

def rotate(values, cosine, sine):
    half_dim = values.shape[-1] // 2
    first_half = values[..., :half_dim]
    second_half = values[..., half_dim:]
    cos_part = cosine[:, None, :]
    sin_part = sine[:, None, :]
    return jnp.concatenate([first_half * cos_part - second_half * sin_part, second_half * cos_part + first_half * sin_part], axis=-1)

def unrotate(values, cosine, sine):
    half_dim = values.shape[-1] // 2
    first_half = values[..., :half_dim]
    second_half = values[..., half_dim:]
    cos_part = cosine[:, None, :]
    sin_part = sine[:, None, :]
    return jnp.concatenate([first_half * cos_part + second_half * sin_part, second_half * cos_part - first_half * sin_part], axis=-1)

def norm_scale(values):
    return lax.rsqrt(lax.optimization_barrier(jnp.mean(values * values, axis=-1, keepdims=True)) + EPSILON)

def norm_backward(values, inverse, gain, normed_cot):
    scaled = normed_cot * gain.astype(jnp.float32)[None, :]
    gain_grad = lax.optimization_barrier(jnp.sum(normed_cot * values * inverse, axis=0))
    values_grad = inverse * scaled - values * (inverse * inverse * inverse) * lax.optimization_barrier(jnp.mean(scaled * values, axis=-1, keepdims=True))
    return (gain_grad, values_grad)

def causal_scores(query_group, key_group):
    scale = query_group.shape[-1] ** (-0.5)
    scores = jnp.einsum('qgd,kd->gqk', query_group.astype(jnp.float32), key_group.astype(jnp.float32)) * scale
    length = key_group.shape[0]
    visible = lax.broadcasted_iota(jnp.int32, (length, length), 0) >= lax.broadcasted_iota(jnp.int32, (length, length), 1)
    return jnp.where(visible[None], scores, -jnp.inf)

def attend_forward(parts):
    query_group, key_group, value_group = parts
    scores = causal_scores(query_group, key_group)
    top_score = lax.optimization_barrier(jnp.max(scores, axis=-1, keepdims=True))
    log_norm = top_score + jnp.log(lax.optimization_barrier(jnp.sum(jnp.exp(scores - top_score), axis=-1, keepdims=True)))
    probs_b = jnp.exp(scores - log_norm).astype(jnp.bfloat16)
    attended = jnp.einsum('gqk,kd->qgd', probs_b.astype(jnp.float32), value_group.astype(jnp.float32)).astype(jnp.bfloat16)
    return (attended, log_norm[..., 0])

def attend_backward(parts):
    query_group, key_group, value_group, attended, log_norm, attended_cot = parts
    scale = query_group.shape[-1] ** (-0.5)
    scores = causal_scores(query_group, key_group)
    probs = jnp.exp(scores - log_norm[..., None])
    probs_b = probs.astype(jnp.bfloat16)
    cot_f32 = attended_cot.astype(jnp.float32)
    value_cot = jnp.einsum('gqk,qgd->kd', probs_b.astype(jnp.float32), cot_f32)
    probs_cot = jnp.einsum('qgd,kd->gqk', cot_f32, value_group.astype(jnp.float32))
    delta = lax.optimization_barrier(jnp.sum(cot_f32 * attended.astype(jnp.float32), axis=-1)).T
    score_cot = (probs * (probs_cot - delta[:, :, None])).astype(jnp.bfloat16)
    score_f32 = score_cot.astype(jnp.float32)
    query_cot = jnp.einsum('gqk,kd->qgd', score_f32, key_group.astype(jnp.float32)) * scale
    key_cot = jnp.einsum('gqk,qgd->kd', score_f32, query_group.astype(jnp.float32)) * scale
    return (query_cot, key_cot, value_cot)

def reference(block_input, attn_gain, query_weight, key_weight, value_weight, output_weight, ffn_gain, gate_weight, up_weight, down_weight, output_cotangent):
    cosine, sine = rope_tables(LEN, HD)
    group_size = HQ // KV
    inputs = block_input.reshape(N_DP, LEN, D)
    cotangents = output_cotangent.reshape(N_DP, LEN, D)

    def one_sequence(totals, pair):
        seq_input, seq_cot = pair
        input_f32 = seq_input.astype(jnp.float32)
        inv_one = norm_scale(input_f32)
        normed_one = (input_f32 * inv_one * attn_gain.astype(jnp.float32)[None, :]).astype(jnp.bfloat16)
        query_raw = jnp.dot(normed_one, query_weight, preferred_element_type=jnp.float32)
        key_raw = jnp.dot(normed_one, key_weight, preferred_element_type=jnp.float32)
        value_raw = jnp.dot(normed_one, value_weight, preferred_element_type=jnp.float32)
        query_rot = rotate(query_raw.reshape(LEN, HQ, HD), cosine, sine).astype(jnp.bfloat16)
        key_rot = rotate(key_raw.reshape(LEN, KV, HD), cosine, sine).astype(jnp.bfloat16)
        value_b = value_raw.astype(jnp.bfloat16)
        query_groups = query_rot.reshape(LEN, KV, group_size, HD).transpose(1, 0, 2, 3)
        key_groups = key_rot.transpose(1, 0, 2)
        value_groups = value_b.reshape(LEN, KV, HD).transpose(1, 0, 2)
        attended, log_norm = lax.map(attend_forward, (query_groups, key_groups, value_groups))
        attn_rows = attended.transpose(1, 0, 2, 3).reshape(LEN, HQ * HD)
        residual = input_f32 + jnp.dot(attn_rows, output_weight, preferred_element_type=jnp.float32)
        inv_two = norm_scale(residual)
        normed_two = (residual * inv_two * ffn_gain.astype(jnp.float32)[None, :]).astype(jnp.bfloat16)
        gate_raw = jnp.dot(normed_two, gate_weight, preferred_element_type=jnp.float32)
        up_raw = jnp.dot(normed_two, up_weight, preferred_element_type=jnp.float32)
        sigma = jax.nn.sigmoid(gate_raw)
        hidden = (gate_raw * sigma * up_raw).astype(jnp.bfloat16)
        seq_output = (residual + jnp.dot(hidden, down_weight, preferred_element_type=jnp.float32)).astype(jnp.bfloat16)
        hidden_cot = jnp.dot(seq_cot, down_weight.T, preferred_element_type=jnp.float32)
        down_grad = jnp.dot(hidden.T, seq_cot, preferred_element_type=jnp.float32)
        gate_cot = (hidden_cot * up_raw * sigma * (1.0 + gate_raw * (1.0 - sigma))).astype(jnp.bfloat16)
        up_cot = (hidden_cot * gate_raw * sigma).astype(jnp.bfloat16)
        gate_grad = jnp.dot(normed_two.T, gate_cot, preferred_element_type=jnp.float32)
        up_grad = jnp.dot(normed_two.T, up_cot, preferred_element_type=jnp.float32)
        normed_two_cot = jnp.dot(gate_cot, gate_weight.T, preferred_element_type=jnp.float32) + jnp.dot(up_cot, up_weight.T, preferred_element_type=jnp.float32)
        ffn_gain_grad, residual_part = norm_backward(residual, inv_two, ffn_gain, normed_two_cot)
        residual_cot = seq_cot.astype(jnp.float32) + residual_part
        residual_cot_b = residual_cot.astype(jnp.bfloat16)
        output_weight_grad = jnp.dot(attn_rows.T, residual_cot_b, preferred_element_type=jnp.float32)
        attended_cot = jnp.dot(residual_cot_b, output_weight.T, preferred_element_type=jnp.float32).astype(jnp.bfloat16)
        cot_groups = attended_cot.reshape(LEN, KV, group_size, HD).transpose(1, 0, 2, 3)
        query_parts, key_parts, value_parts = lax.map(attend_backward, (query_groups, key_groups, value_groups, attended, log_norm, cot_groups))
        query_cot = unrotate(query_parts.transpose(1, 0, 2, 3).reshape(LEN, HQ, HD), cosine, sine).reshape(LEN, HQ * HD).astype(jnp.bfloat16)
        key_cot = unrotate(key_parts.transpose(1, 0, 2), cosine, sine).reshape(LEN, KV * HD).astype(jnp.bfloat16)
        value_cot = value_parts.transpose(1, 0, 2).reshape(LEN, KV * HD).astype(jnp.bfloat16)
        query_grad = jnp.dot(normed_one.T, query_cot, preferred_element_type=jnp.float32)
        key_grad = jnp.dot(normed_one.T, key_cot, preferred_element_type=jnp.float32)
        value_grad = jnp.dot(normed_one.T, value_cot, preferred_element_type=jnp.float32)
        normed_one_cot = jnp.dot(query_cot, query_weight.T, preferred_element_type=jnp.float32)
        normed_one_cot = normed_one_cot + jnp.dot(key_cot, key_weight.T, preferred_element_type=jnp.float32)
        normed_one_cot = normed_one_cot + jnp.dot(value_cot, value_weight.T, preferred_element_type=jnp.float32)
        attn_gain_grad, input_part = norm_backward(input_f32, inv_one, attn_gain, normed_one_cot)
        input_grad = residual_cot + input_part
        grads = (attn_gain_grad, query_grad, key_grad, value_grad, output_weight_grad, ffn_gain_grad, gate_grad, up_grad, down_grad)
        totals = jax.tree.map(lambda left, right: left + right, totals, grads)
        return (totals, (seq_output, input_grad))
    initial = (jnp.zeros((D,), jnp.float32), jnp.zeros((D, HQ * HD), jnp.float32), jnp.zeros((D, KV * HD), jnp.float32), jnp.zeros((D, KV * HD), jnp.float32), jnp.zeros((HQ * HD, D), jnp.float32), jnp.zeros((D,), jnp.float32), jnp.zeros((D, FF), jnp.float32), jnp.zeros((D, FF), jnp.float32), jnp.zeros((FF, D), jnp.float32))
    totals, stacked = lax.scan(one_sequence, initial, (inputs, cotangents))
    outputs, input_grads = stacked
    return (outputs.reshape(TOKENS, D), input_grads.reshape(TOKENS, D), totals[0], totals[1], totals[2], totals[3], totals[4], totals[5], totals[6], totals[7], totals[8])
```

```python
import jax
import jax.numpy as jnp
from jax import lax
from jax.sharding import PartitionSpec as P

HD = 64


EPSILON = 1e-05
ROPE_BASE = 10000.0


def rope_tables(length, head_dim):
    half_dim = head_dim // 2
    position = jnp.arange(length, dtype=jnp.float32)
    inverse = ROPE_BASE ** (-(jnp.arange(half_dim, dtype=jnp.float32) * (2.0 / head_dim)))
    angle = position[:, None] * inverse[None, :]
    return (jnp.cos(angle), jnp.sin(angle))


def rotate(values, cosine, sine):
    half_dim = values.shape[-1] // 2
    first_half = values[..., :half_dim]
    second_half = values[..., half_dim:]
    cos_part = cosine[:, None, :]
    sin_part = sine[:, None, :]
    return jnp.concatenate(
        [
            first_half * cos_part - second_half * sin_part,
            second_half * cos_part + first_half * sin_part,
        ],
        axis=-1,
    )


def unrotate(values, cosine, sine):
    half_dim = values.shape[-1] // 2
    first_half = values[..., :half_dim]
    second_half = values[..., half_dim:]
    cos_part = cosine[:, None, :]
    sin_part = sine[:, None, :]
    return jnp.concatenate(
        [
            first_half * cos_part + second_half * sin_part,
            second_half * cos_part - first_half * sin_part,
        ],
        axis=-1,
    )


def norm_scale(values):
    return lax.rsqrt(jnp.mean(values * values, axis=-1, keepdims=True) + EPSILON)


def norm_backward(values, inverse, gain, normed_cot):
    scaled = normed_cot * gain.astype(jnp.float32)[None, :]
    gain_grad = jnp.sum(normed_cot * values * inverse, axis=0)
    values_grad = inverse * scaled - values * (inverse * inverse * inverse) * jnp.mean(
        scaled * values, axis=-1, keepdims=True
    )
    return (gain_grad, values_grad)


def causal_scores(query_group, key_group):
    scale = query_group.shape[-1] ** (-0.5)
    scores = (
        jnp.einsum("qgd,kd->gqk", query_group, key_group, preferred_element_type=jnp.float32)
        * scale
    )
    length = key_group.shape[0]
    visible = lax.broadcasted_iota(jnp.int32, (length, length), 0) >= lax.broadcasted_iota(
        jnp.int32, (length, length), 1
    )
    return jnp.where(visible[None], scores, -jnp.inf)


def head_forward(parts):
    query_group, key_group, value_group = parts
    scores = causal_scores(query_group, key_group)
    top_score = jnp.max(scores, axis=-1, keepdims=True)
    log_norm = top_score + jnp.log(jnp.sum(jnp.exp(scores - top_score), axis=-1, keepdims=True))
    probs_b = jnp.exp(scores - log_norm).astype(jnp.bfloat16)
    attended = jnp.einsum(
        "gqk,kd->qgd", probs_b, value_group, preferred_element_type=jnp.float32
    ).astype(jnp.bfloat16)
    return (attended, log_norm[..., 0])


def head_backward(parts):
    query_group, key_group, value_group, attended, log_norm, attended_cot = parts
    scale = query_group.shape[-1] ** (-0.5)
    scores = causal_scores(query_group, key_group)
    probs = jnp.exp(scores - log_norm[..., None])
    probs_b = probs.astype(jnp.bfloat16)
    value_cot = jnp.einsum("gqk,qgd->kd", probs_b, attended_cot, preferred_element_type=jnp.float32)
    probs_cot = jnp.einsum(
        "qgd,kd->gqk", attended_cot, value_group, preferred_element_type=jnp.float32
    )
    delta = jnp.sum(attended_cot.astype(jnp.float32) * attended.astype(jnp.float32), axis=-1).T
    score_cot = (probs * (probs_cot - delta[:, :, None])).astype(jnp.bfloat16)
    query_cot = (
        jnp.einsum("gqk,kd->qgd", score_cot, key_group, preferred_element_type=jnp.float32) * scale
    )
    key_cot = (
        jnp.einsum("gqk,qgd->kd", score_cot, query_group, preferred_element_type=jnp.float32)
        * scale
    )
    return (query_cot, key_cot, value_cot)


def plain_shards(
    block_input,
    attn_gain,
    query_weight,
    key_weight,
    value_weight,
    output_weight,
    ffn_gain,
    gate_weight,
    up_weight,
    down_weight,
    output_cotangent,
):
    local_rows = block_input.shape[0]
    own_start = lax.axis_index("mp") * local_rows
    query_full, key_full, value_full, out_full, gain_one = (
        lax.all_gather(query_weight, "dp", axis=0, tiled=True),
        lax.all_gather(key_weight, "dp", axis=0, tiled=True),
        lax.all_gather(value_weight, "dp", axis=0, tiled=True),
        lax.all_gather(output_weight, "dp", axis=0, tiled=True),
        lax.all_gather(attn_gain, "dp", axis=0, tiled=True),
    )
    seq_input = lax.all_gather(block_input, "mp", axis=0, tiled=True)
    length = seq_input.shape[0]
    local_heads = query_full.shape[1] // HD
    local_groups = key_full.shape[1] // HD
    per_group = local_heads // local_groups
    cosine, sine = rope_tables(length, HD)
    input_f32 = seq_input.astype(jnp.float32)
    inv_one = norm_scale(input_f32)
    normed_one = (input_f32 * inv_one * gain_one.astype(jnp.float32)[None, :]).astype(jnp.bfloat16)
    query_raw = jnp.dot(normed_one, query_full, preferred_element_type=jnp.float32)
    key_raw = jnp.dot(normed_one, key_full, preferred_element_type=jnp.float32)
    value_raw = jnp.dot(normed_one, value_full, preferred_element_type=jnp.float32)
    query_rot = rotate(query_raw.reshape(length, local_heads, HD), cosine, sine).astype(
        jnp.bfloat16
    )
    key_rot = rotate(key_raw.reshape(length, local_groups, HD), cosine, sine).astype(jnp.bfloat16)
    value_b = value_raw.astype(jnp.bfloat16)
    query_groups = query_rot.reshape(length, local_groups, per_group, HD).transpose(1, 0, 2, 3)
    key_groups = key_rot.transpose(1, 0, 2)
    value_groups = value_b.reshape(length, local_groups, HD).transpose(1, 0, 2)
    attended, log_norm = lax.map(head_forward, (query_groups, key_groups, value_groups))
    attn_rows = attended.transpose(1, 0, 2, 3).reshape(length, local_heads * HD)
    attn_part = jnp.dot(attn_rows, out_full, preferred_element_type=jnp.float32)
    residual = input_f32 + lax.psum(attn_part, "mp")
    gate_full, up_full, down_full, gain_two = (
        lax.all_gather(gate_weight, "dp", axis=0, tiled=True),
        lax.all_gather(up_weight, "dp", axis=0, tiled=True),
        lax.all_gather(down_weight, "dp", axis=0, tiled=True),
        lax.all_gather(ffn_gain, "dp", axis=0, tiled=True),
    )
    inv_two = norm_scale(residual)
    normed_two = (residual * inv_two * gain_two.astype(jnp.float32)[None, :]).astype(jnp.bfloat16)
    gate_raw = jnp.dot(normed_two, gate_full, preferred_element_type=jnp.float32)
    up_raw = jnp.dot(normed_two, up_full, preferred_element_type=jnp.float32)
    sigma = jax.nn.sigmoid(gate_raw)
    hidden = (gate_raw * sigma * up_raw).astype(jnp.bfloat16)
    ffn_own = lax.psum_scatter(
        jnp.dot(hidden, down_full, preferred_element_type=jnp.float32),
        "mp",
        scatter_dimension=0,
        tiled=True,
    )
    residual_own = lax.dynamic_slice_in_dim(residual, own_start, local_rows, 0)
    block_output = (residual_own + ffn_own).astype(jnp.bfloat16)
    cot_seq = lax.all_gather(output_cotangent, "mp", axis=0, tiled=True)
    hidden_cot = jnp.einsum("td,fd->tf", cot_seq, down_full, preferred_element_type=jnp.float32)
    gate_cot = (hidden_cot * up_raw * sigma * (1.0 + gate_raw * (1.0 - sigma))).astype(jnp.bfloat16)
    up_cot = (hidden_cot * gate_raw * sigma).astype(jnp.bfloat16)
    normed_two_part = jnp.einsum(
        "tf,df->td", gate_cot, gate_full, preferred_element_type=jnp.float32
    )
    normed_two_part = normed_two_part + jnp.einsum(
        "tf,df->td", up_cot, up_full, preferred_element_type=jnp.float32
    )
    normed_two_cot = lax.psum(normed_two_part, "mp")
    ffn_gain_grad, residual_part = norm_backward(residual, inv_two, gain_two, normed_two_cot)
    residual_cot = cot_seq.astype(jnp.float32) + residual_part
    down_grad = jnp.einsum("tf,td->fd", hidden, cot_seq, preferred_element_type=jnp.float32)
    gate_grad = jnp.einsum("td,tf->df", normed_two, gate_cot, preferred_element_type=jnp.float32)
    up_grad = jnp.einsum("td,tf->df", normed_two, up_cot, preferred_element_type=jnp.float32)
    gate_share, up_share, down_share, ffn_gain_share = (
        lax.psum_scatter(gate_grad, "dp", scatter_dimension=0, tiled=True),
        lax.psum_scatter(up_grad, "dp", scatter_dimension=0, tiled=True),
        lax.psum_scatter(down_grad, "dp", scatter_dimension=0, tiled=True),
        lax.psum_scatter(ffn_gain_grad, "dp", scatter_dimension=0, tiled=True),
    )
    residual_cot_b = residual_cot.astype(jnp.bfloat16)
    output_weight_grad = jnp.einsum(
        "th,td->hd", attn_rows, residual_cot_b, preferred_element_type=jnp.float32
    )
    attended_cot = jnp.einsum(
        "td,hd->th", residual_cot_b, out_full, preferred_element_type=jnp.float32
    ).astype(jnp.bfloat16)
    cot_groups = attended_cot.reshape(length, local_groups, per_group, HD).transpose(1, 0, 2, 3)
    query_parts, key_parts, value_parts = lax.map(
        head_backward, (query_groups, key_groups, value_groups, attended, log_norm, cot_groups)
    )
    query_cot = (
        unrotate(query_parts.transpose(1, 0, 2, 3).reshape(length, local_heads, HD), cosine, sine)
        .reshape(length, local_heads * HD)
        .astype(jnp.bfloat16)
    )
    key_cot = (
        unrotate(key_parts.transpose(1, 0, 2), cosine, sine)
        .reshape(length, local_groups * HD)
        .astype(jnp.bfloat16)
    )
    value_cot = (
        value_parts.transpose(1, 0, 2).reshape(length, local_groups * HD).astype(jnp.bfloat16)
    )
    normed_one_part = jnp.einsum(
        "th,dh->td", query_cot, query_full, preferred_element_type=jnp.float32
    )
    normed_one_part = normed_one_part + jnp.einsum(
        "th,dh->td", key_cot, key_full, preferred_element_type=jnp.float32
    )
    normed_one_part = normed_one_part + jnp.einsum(
        "th,dh->td", value_cot, value_full, preferred_element_type=jnp.float32
    )
    normed_one_cot = lax.psum(normed_one_part, "mp")
    query_grad = jnp.einsum("td,th->dh", normed_one, query_cot, preferred_element_type=jnp.float32)
    key_grad = jnp.einsum("td,th->dh", normed_one, key_cot, preferred_element_type=jnp.float32)
    value_grad = jnp.einsum("td,th->dh", normed_one, value_cot, preferred_element_type=jnp.float32)
    attn_gain_grad, input_part = norm_backward(input_f32, inv_one, gain_one, normed_one_cot)
    input_cot = residual_cot + input_part
    input_grad = lax.dynamic_slice_in_dim(input_cot, own_start, local_rows, 0)
    attn_gain_share, query_share, key_share, value_share, output_share = (
        lax.psum_scatter(attn_gain_grad, "dp", scatter_dimension=0, tiled=True),
        lax.psum_scatter(query_grad, "dp", scatter_dimension=0, tiled=True),
        lax.psum_scatter(key_grad, "dp", scatter_dimension=0, tiled=True),
        lax.psum_scatter(value_grad, "dp", scatter_dimension=0, tiled=True),
        lax.psum_scatter(output_weight_grad, "dp", scatter_dimension=0, tiled=True),
    )
    return (
        block_output,
        input_grad,
        attn_gain_share,
        query_share,
        key_share,
        value_share,
        output_share,
        ffn_gain_share,
        gate_share,
        up_share,
        down_share,
    )


GROUP = 4
LANES = 128


def whole_up(size, step):
    return -(-size // step) * step


def partner(values, key):
    pairs = [(at, at ^ key) for at in range(lax.axis_size("dp"))]
    return lax.ppermute(values, "dp", pairs)


def twin(values):
    return lax.ppermute(values, "mp", [(0, 1), (1, 0)])


def along_line(values, sources, step):
    pairs = [
        (at * GROUP + place, (at + step) * GROUP + place)
        for at in sources
        for place in range(GROUP)
    ]
    return lax.ppermute(values, "dp", pairs)


def line_gather(values, own):
    lines = lax.axis_size("dp") // GROUP
    ups, downs = [values], [values]
    for hop in range(1, lines):
        ups.append(along_line(ups[-1], range(hop - 1, lines - 1), 1))
        downs.append(along_line(downs[-1], range(1, lines - hop + 1), -1))
    out = jnp.zeros((lines,) + values.shape, values.dtype)
    out = lax.dynamic_update_index_in_dim(out, values, own, 0)
    for hop in range(1, lines):
        block = jnp.where(own >= hop, ups[hop], downs[lines - hop])
        out = lax.dynamic_update_index_in_dim(out, block, lax.rem(own - hop + lines, lines), 0)
    return out


def line_scatter(blocks, own):
    lines = blocks.shape[0]
    total = lax.dynamic_index_in_dim(blocks, own, 0, keepdims=False)
    for step in (1, -1):
        moving = None
        for hop in range(1, lines):
            far = own + step * (lines - hop)
            part = lax.dynamic_index_in_dim(blocks, jnp.clip(far, 0, lines - 1), 0, keepdims=False)
            if moving is not None:
                part = part + moving
            sources = range(0, hop) if step == 1 else range(lines - hop, lines)
            moving = along_line(part, sources, step)
        total = total + moving
    return total


def pair_gather(blocks, bits):
    place = lax.rem(lax.axis_index("dp"), GROUP)
    for bit in bits:
        here = lax.rem(place // (bit + 1), 2)
        there = partner(blocks, bit + 1)
        axis = 1 if (bit == 1 or blocks.ndim == 3) else 2
        low = jnp.where(here == 0, blocks, there)
        high = jnp.where(here == 0, there, blocks)
        blocks = jnp.stack([low, high], axis=axis)
    return blocks


def pair_scatter(blocks, bits):
    place = lax.rem(lax.axis_index("dp"), GROUP)
    for bit in bits:
        here = lax.rem(place // (bit + 1), 2)
        axis = 1 if (bit == 1 or blocks.ndim == 4) else 2
        keep = lax.dynamic_index_in_dim(blocks, here, axis, keepdims=False)
        away = lax.dynamic_index_in_dim(blocks, 1 - here, axis, keepdims=False)
        blocks = keep + partner(away, bit + 1)
    return blocks


def group_rows(own):
    mine = jnp.stack([own] + [partner(own, key) for key in range(1, GROUP)])
    both = jnp.stack([mine, twin(mine)])
    return both.reshape(2 * GROUP * own.shape[0], own.shape[1])


def group_sum(near, far):
    blocks = near.reshape(GROUP, -1, near.shape[1])
    blocks = blocks + twin(far).reshape(blocks.shape)
    total = blocks[0]
    for key in range(1, GROUP):
        total = total + partner(blocks[key], key)
    return total


def ordered(own, core):
    there = twin(own)
    first = jnp.where(core == 0, own, there)
    second = jnp.where(core == 0, there, own)
    return jnp.concatenate([first, second], axis=0)


def twin_sum(part, core):
    halves = part.reshape(2, -1, part.shape[1])
    keep = lax.dynamic_index_in_dim(halves, core, 0, keepdims=False)
    away = lax.dynamic_index_in_dim(halves, 1 - core, 0, keepdims=False)
    return keep + twin(away)


def grouped_shards(
    block_input,
    attn_gain,
    query_weight,
    key_weight,
    value_weight,
    output_weight,
    ffn_gain,
    gate_weight,
    up_weight,
    down_weight,
    output_cotangent,
):
    f32, bf16 = jnp.float32, jnp.bfloat16
    members = lax.axis_size("dp")
    lines = members // GROUP
    index = lax.axis_index("dp")
    own, place = index // GROUP, lax.rem(index, GROUP)
    core = lax.axis_index("mp")
    rows, units = gate_weight.shape
    width = rows * members
    query_cols, key_cols = query_weight.shape[1], key_weight.shape[1]
    unit_rows = down_weight.shape[0]
    share = unit_rows * lines
    padded = whole_up(share, LANES)

    narrow = jnp.concatenate([query_weight, key_weight, value_weight], axis=1)
    cols = narrow.shape[1]
    gains = jnp.pad(jnp.stack([attn_gain, ffn_gain]), ((0, 6), (0, cols - rows)))
    narrow = jnp.concatenate([narrow, gains], axis=0)
    seq_input = ordered(block_input, core)
    narrow_all = pair_gather(line_gather(narrow, own), (0, 1))
    out_all = pair_gather(line_gather(output_weight, own), (1, 0))
    narrow_full = narrow_all[..., :rows, :].reshape(width, cols)
    gain_one = narrow_all[..., rows, :rows].reshape(width)
    gain_two = narrow_all[..., rows + 1, :rows].reshape(width)
    out_full = out_all.reshape(-1, width)

    def shares(weight):
        parts = weight.reshape(rows, lines, GROUP, unit_rows).transpose(2, 0, 1, 3)
        return jnp.pad(parts.reshape(GROUP, rows, share), ((0, 0), (0, 0), (0, padded - share)))

    pieces = jnp.concatenate([shares(gate_weight), shares(up_weight)], axis=2)
    mixed = jnp.zeros((GROUP, rows, 2 * padded), bf16)
    for key in range(GROUP):
        other = place ^ key
        piece = lax.dynamic_index_in_dim(pieces, other, 0, keepdims=False)
        if key:
            piece = partner(piece, key)
        mixed = lax.dynamic_update_index_in_dim(mixed, piece, other, 0)
    wide_full = line_gather(mixed.reshape(GROUP * rows, 2 * padded), own).reshape(width, 2 * padded)
    down_share = line_gather(down_weight, own).reshape(share, width)
    down_share = jnp.pad(down_share, ((0, padded - share), (0, 0)))
    cot_rows = group_rows(output_cotangent)

    length = seq_input.shape[0]
    local_heads = query_cols // HD
    local_groups = key_cols // HD
    per_group = local_heads // local_groups
    cosine, sine = rope_tables(length, HD)
    input_f32 = seq_input.astype(f32)
    normed_one = (input_f32 * norm_scale(input_f32) * gain_one.astype(f32)[None, :]).astype(bf16)
    raw = jnp.dot(normed_one, narrow_full, preferred_element_type=f32)
    query_raw = raw[:, :query_cols]
    key_raw = raw[:, query_cols : query_cols + key_cols]
    value_raw = raw[:, query_cols + key_cols :]
    query_rot = rotate(query_raw.reshape(length, local_heads, HD), cosine, sine).astype(bf16)
    key_rot = rotate(key_raw.reshape(length, local_groups, HD), cosine, sine).astype(bf16)
    value_b = value_raw.astype(bf16)
    query_groups = query_rot.reshape(length, local_groups, per_group, HD).transpose(1, 0, 2, 3)
    key_groups = key_rot.transpose(1, 0, 2)
    value_groups = value_b.reshape(length, local_groups, HD).transpose(1, 0, 2)
    attended, log_norm = lax.map(head_forward, (query_groups, key_groups, value_groups))
    attn_rows = attended.transpose(1, 0, 2, 3).reshape(length, local_heads * HD)
    attn_part = jnp.dot(attn_rows, out_full, preferred_element_type=f32)
    own_f32 = block_input.astype(f32)
    residual = own_f32 + twin_sum(attn_part, core)
    inv_two = norm_scale(residual)
    normed_two = (residual * inv_two * gain_two.astype(f32)[None, :]).astype(bf16)

    ffn_rows = group_rows(normed_two)
    both_raw = jnp.dot(ffn_rows, wide_full, preferred_element_type=f32)
    gate_raw, up_raw = both_raw[:, :padded], both_raw[:, padded:]
    sigma = jax.nn.sigmoid(gate_raw)
    hidden = (gate_raw * sigma * up_raw).astype(bf16)
    hidden_cot = jnp.einsum("td,fd->tf", cot_rows, down_share, preferred_element_type=f32)
    gate_cot = (hidden_cot * up_raw * sigma * (1.0 + gate_raw * (1.0 - sigma))).astype(bf16)
    up_cot = (hidden_cot * gate_raw * sigma).astype(bf16)
    both_cot = jnp.concatenate([gate_cot, up_cot], axis=1)
    half = ffn_rows.shape[0] // 2

    def back(part):
        return jnp.einsum("tf,df->td", part, wide_full, preferred_element_type=f32)

    normed_two_cot = group_sum(back(both_cot[:half]), back(both_cot[half:]))

    def forth(part):
        return jnp.dot(part, down_share, preferred_element_type=f32)

    ffn_out = group_sum(forth(hidden[:half]), forth(hidden[half:]))
    block_output = (residual + ffn_out).astype(bf16)
    wide_grad = jnp.einsum("td,tf->df", ffn_rows, both_cot, preferred_element_type=f32)
    down_grad = jnp.einsum("tf,td->fd", hidden, cot_rows, preferred_element_type=f32)

    down_own = line_scatter(down_grad[:share].reshape(lines, unit_rows, width), own)
    wide_own = line_scatter(wide_grad.reshape(lines, GROUP * rows, 2 * padded), own)
    wide_own = wide_own.reshape(GROUP, rows, 2 * padded)
    wide_mixed = jnp.zeros(wide_own.shape, f32)
    for key in range(GROUP):
        other = place ^ key
        piece = lax.dynamic_index_in_dim(wide_own, other, 0, keepdims=False)
        if key:
            piece = partner(piece, key)
        wide_mixed = lax.dynamic_update_index_in_dim(wide_mixed, piece, other, 0)

    def unshared(parts):
        parts = parts[:, :, :share].reshape(GROUP, rows, lines, unit_rows)
        return parts.transpose(1, 2, 0, 3).reshape(rows, units)

    gate_own = unshared(wide_mixed[:, :, :padded])
    up_own = unshared(wide_mixed[:, :, padded:])

    ffn_gain_part, residual_part = norm_backward(residual, inv_two, gain_two, normed_two_cot)
    residual_cot = output_cotangent.astype(f32) + residual_part
    residual_cot_b = ordered(residual_cot.astype(bf16), core)
    out_grad = jnp.einsum("th,td->hd", attn_rows, residual_cot_b, preferred_element_type=f32)
    out_own = line_scatter(
        pair_scatter(out_grad.reshape(lines, 2, 2, -1, width), (1, 0)), own
    )
    attended_cot = jnp.einsum(
        "td,hd->th", residual_cot_b, out_full, preferred_element_type=f32
    ).astype(bf16)
    cot_groups = attended_cot.reshape(length, local_groups, per_group, HD).transpose(1, 0, 2, 3)
    query_parts, key_parts, value_parts = lax.map(
        head_backward, (query_groups, key_groups, value_groups, attended, log_norm, cot_groups)
    )
    query_cot = unrotate(
        query_parts.transpose(1, 0, 2, 3).reshape(length, local_heads, HD), cosine, sine
    ).reshape(length, local_heads * HD)
    key_cot = unrotate(key_parts.transpose(1, 0, 2), cosine, sine).reshape(length, key_cols)
    value_cot = value_parts.transpose(1, 0, 2).reshape(length, key_cols)
    narrow_cot = jnp.concatenate(
        [query_cot.astype(bf16), key_cot.astype(bf16), value_cot.astype(bf16)], axis=1
    )
    normed_one_part = jnp.einsum("th,dh->td", narrow_cot, narrow_full, preferred_element_type=f32)
    normed_one_cot = twin_sum(normed_one_part, core)
    attn_gain_part, input_part = norm_backward(
        own_f32, norm_scale(own_f32), gain_one, normed_one_cot
    )
    input_grad = residual_cot + input_part
    narrow_grad = jnp.einsum("td,th->dh", normed_one, narrow_cot, preferred_element_type=f32)
    gain_parts = jnp.stack([attn_gain_part, ffn_gain_part])
    gain_parts = gain_parts + twin(gain_parts)
    gain_parts = gain_parts.reshape(2, members, rows).transpose(1, 0, 2)
    gain_parts = jnp.pad(gain_parts, ((0, 0), (0, 6), (0, cols - rows)))
    narrow_grad = jnp.concatenate([narrow_grad.reshape(members, rows, cols), gain_parts], axis=1)
    narrow_own = line_scatter(
        pair_scatter(narrow_grad.reshape(lines, 2, 2, -1, cols), (0, 1)), own
    )
    return (
        block_output,
        input_grad,
        narrow_own[rows, :rows],
        narrow_own[:rows, :query_cols],
        narrow_own[:rows, query_cols : query_cols + key_cols],
        narrow_own[:rows, query_cols + key_cols :],
        out_own,
        narrow_own[rows + 1, :rows],
        gate_own,
        up_own,
        down_own,
    )


def solution(mesh):
    placed = (
        P(("dp", "mp"), None),
        P("dp"),
        P("dp", "mp"),
        P("dp", "mp"),
        P("dp", "mp"),
        P(("mp", "dp"), None),
        P("dp"),
        P("dp", "mp"),
        P("dp", "mp"),
        P(("mp", "dp"), None),
        P(("dp", "mp"), None),
    )
    members = mesh.shape["dp"]
    fits = mesh.shape["mp"] == 2 and members % GROUP == 0 and members // GROUP <= GROUP
    return jax.shard_map(
        grouped_shards if fits else plain_shards,
        mesh=mesh,
        in_specs=placed,
        out_specs=(
            P(("dp", "mp"), None),
            P(("dp", "mp"), None),
            P("dp"),
            P("dp", "mp"),
            P("dp", "mp"),
            P("dp", "mp"),
            P(("mp", "dp"), None),
            P("dp"),
            P("dp", "mp"),
            P("dp", "mp"),
            P(("mp", "dp"), None),
        ),
        check_vma=False,
    )
```

```python
import functools

import jax
import jax.numpy as jnp
from jax import lax
from jax.experimental import pallas as pl
from jax.experimental.pallas import tpu as pltpu
from jax.sharding import PartitionSpec as P

HD = 64


EPSILON = 1e-05
ROPE_BASE = 10000.0


def rope_tables(length, head_dim):
    half_dim = head_dim // 2
    position = jnp.arange(length, dtype=jnp.float32)
    inverse = ROPE_BASE ** (-(jnp.arange(half_dim, dtype=jnp.float32) * (2.0 / head_dim)))
    angle = position[:, None] * inverse[None, :]
    return (jnp.cos(angle), jnp.sin(angle))


def rotate(values, cosine, sine):
    half_dim = values.shape[-1] // 2
    first_half = values[..., :half_dim]
    second_half = values[..., half_dim:]
    cos_part = cosine[:, None, :]
    sin_part = sine[:, None, :]
    return jnp.concatenate(
        [
            first_half * cos_part - second_half * sin_part,
            second_half * cos_part + first_half * sin_part,
        ],
        axis=-1,
    )


def unrotate(values, cosine, sine):
    half_dim = values.shape[-1] // 2
    first_half = values[..., :half_dim]
    second_half = values[..., half_dim:]
    cos_part = cosine[:, None, :]
    sin_part = sine[:, None, :]
    return jnp.concatenate(
        [
            first_half * cos_part + second_half * sin_part,
            second_half * cos_part - first_half * sin_part,
        ],
        axis=-1,
    )


def norm_scale(values):
    return lax.rsqrt(jnp.mean(values * values, axis=-1, keepdims=True) + EPSILON)


def norm_backward(values, inverse, gain, normed_cot):
    scaled = normed_cot * gain.astype(jnp.float32)[None, :]
    gain_grad = jnp.sum(normed_cot * values * inverse, axis=0)
    values_grad = inverse * scaled - values * (inverse * inverse * inverse) * jnp.mean(
        scaled * values, axis=-1, keepdims=True
    )
    return (gain_grad, values_grad)


def causal_scores(query_group, key_group):
    scale = query_group.shape[-1] ** (-0.5)
    scores = (
        jnp.einsum("qgd,kd->gqk", query_group, key_group, preferred_element_type=jnp.float32)
        * scale
    )
    length = key_group.shape[0]
    visible = lax.broadcasted_iota(jnp.int32, (length, length), 0) >= lax.broadcasted_iota(
        jnp.int32, (length, length), 1
    )
    return jnp.where(visible[None], scores, -jnp.inf)


def head_forward(parts):
    query_group, key_group, value_group = parts
    scores = causal_scores(query_group, key_group)
    top_score = jnp.max(scores, axis=-1, keepdims=True)
    log_norm = top_score + jnp.log(jnp.sum(jnp.exp(scores - top_score), axis=-1, keepdims=True))
    probs_b = jnp.exp(scores - log_norm).astype(jnp.bfloat16)
    attended = jnp.einsum(
        "gqk,kd->qgd", probs_b, value_group, preferred_element_type=jnp.float32
    ).astype(jnp.bfloat16)
    return (attended, log_norm[..., 0])


def head_backward(parts):
    query_group, key_group, value_group, attended, log_norm, attended_cot = parts
    scale = query_group.shape[-1] ** (-0.5)
    scores = causal_scores(query_group, key_group)
    probs = jnp.exp(scores - log_norm[..., None])
    probs_b = probs.astype(jnp.bfloat16)
    value_cot = jnp.einsum("gqk,qgd->kd", probs_b, attended_cot, preferred_element_type=jnp.float32)
    probs_cot = jnp.einsum(
        "qgd,kd->gqk", attended_cot, value_group, preferred_element_type=jnp.float32
    )
    delta = jnp.sum(attended_cot.astype(jnp.float32) * attended.astype(jnp.float32), axis=-1).T
    score_cot = (probs * (probs_cot - delta[:, :, None])).astype(jnp.bfloat16)
    query_cot = (
        jnp.einsum("gqk,kd->qgd", score_cot, key_group, preferred_element_type=jnp.float32) * scale
    )
    key_cot = (
        jnp.einsum("gqk,qgd->kd", score_cot, query_group, preferred_element_type=jnp.float32)
        * scale
    )
    return (query_cot, key_cot, value_cot)


def plain_shards(
    block_input,
    attn_gain,
    query_weight,
    key_weight,
    value_weight,
    output_weight,
    ffn_gain,
    gate_weight,
    up_weight,
    down_weight,
    output_cotangent,
):
    local_rows = block_input.shape[0]
    own_start = lax.axis_index("mp") * local_rows
    query_full, key_full, value_full, out_full, gain_one = (
        lax.all_gather(query_weight, "dp", axis=0, tiled=True),
        lax.all_gather(key_weight, "dp", axis=0, tiled=True),
        lax.all_gather(value_weight, "dp", axis=0, tiled=True),
        lax.all_gather(output_weight, "dp", axis=0, tiled=True),
        lax.all_gather(attn_gain, "dp", axis=0, tiled=True),
    )
    seq_input = lax.all_gather(block_input, "mp", axis=0, tiled=True)
    length = seq_input.shape[0]
    local_heads = query_full.shape[1] // HD
    local_groups = key_full.shape[1] // HD
    per_group = local_heads // local_groups
    cosine, sine = rope_tables(length, HD)
    input_f32 = seq_input.astype(jnp.float32)
    inv_one = norm_scale(input_f32)
    normed_one = (input_f32 * inv_one * gain_one.astype(jnp.float32)[None, :]).astype(jnp.bfloat16)
    query_raw = jnp.dot(normed_one, query_full, preferred_element_type=jnp.float32)
    key_raw = jnp.dot(normed_one, key_full, preferred_element_type=jnp.float32)
    value_raw = jnp.dot(normed_one, value_full, preferred_element_type=jnp.float32)
    query_rot = rotate(query_raw.reshape(length, local_heads, HD), cosine, sine).astype(
        jnp.bfloat16
    )
    key_rot = rotate(key_raw.reshape(length, local_groups, HD), cosine, sine).astype(jnp.bfloat16)
    value_b = value_raw.astype(jnp.bfloat16)
    query_groups = query_rot.reshape(length, local_groups, per_group, HD).transpose(1, 0, 2, 3)
    key_groups = key_rot.transpose(1, 0, 2)
    value_groups = value_b.reshape(length, local_groups, HD).transpose(1, 0, 2)
    attended, log_norm = lax.map(head_forward, (query_groups, key_groups, value_groups))
    attn_rows = attended.transpose(1, 0, 2, 3).reshape(length, local_heads * HD)
    attn_part = jnp.dot(attn_rows, out_full, preferred_element_type=jnp.float32)
    residual = input_f32 + lax.psum(attn_part, "mp")
    gate_full, up_full, down_full, gain_two = (
        lax.all_gather(gate_weight, "dp", axis=0, tiled=True),
        lax.all_gather(up_weight, "dp", axis=0, tiled=True),
        lax.all_gather(down_weight, "dp", axis=0, tiled=True),
        lax.all_gather(ffn_gain, "dp", axis=0, tiled=True),
    )
    inv_two = norm_scale(residual)
    normed_two = (residual * inv_two * gain_two.astype(jnp.float32)[None, :]).astype(jnp.bfloat16)
    gate_raw = jnp.dot(normed_two, gate_full, preferred_element_type=jnp.float32)
    up_raw = jnp.dot(normed_two, up_full, preferred_element_type=jnp.float32)
    sigma = jax.nn.sigmoid(gate_raw)
    hidden = (gate_raw * sigma * up_raw).astype(jnp.bfloat16)
    ffn_own = lax.psum_scatter(
        jnp.dot(hidden, down_full, preferred_element_type=jnp.float32),
        "mp",
        scatter_dimension=0,
        tiled=True,
    )
    residual_own = lax.dynamic_slice_in_dim(residual, own_start, local_rows, 0)
    block_output = (residual_own + ffn_own).astype(jnp.bfloat16)
    cot_seq = lax.all_gather(output_cotangent, "mp", axis=0, tiled=True)
    hidden_cot = jnp.einsum("td,fd->tf", cot_seq, down_full, preferred_element_type=jnp.float32)
    gate_cot = (hidden_cot * up_raw * sigma * (1.0 + gate_raw * (1.0 - sigma))).astype(jnp.bfloat16)
    up_cot = (hidden_cot * gate_raw * sigma).astype(jnp.bfloat16)
    normed_two_part = jnp.einsum(
        "tf,df->td", gate_cot, gate_full, preferred_element_type=jnp.float32
    )
    normed_two_part = normed_two_part + jnp.einsum(
        "tf,df->td", up_cot, up_full, preferred_element_type=jnp.float32
    )
    normed_two_cot = lax.psum(normed_two_part, "mp")
    ffn_gain_grad, residual_part = norm_backward(residual, inv_two, gain_two, normed_two_cot)
    residual_cot = cot_seq.astype(jnp.float32) + residual_part
    down_grad = jnp.einsum("tf,td->fd", hidden, cot_seq, preferred_element_type=jnp.float32)
    gate_grad = jnp.einsum("td,tf->df", normed_two, gate_cot, preferred_element_type=jnp.float32)
    up_grad = jnp.einsum("td,tf->df", normed_two, up_cot, preferred_element_type=jnp.float32)
    gate_share, up_share, down_share, ffn_gain_share = (
        lax.psum_scatter(gate_grad, "dp", scatter_dimension=0, tiled=True),
        lax.psum_scatter(up_grad, "dp", scatter_dimension=0, tiled=True),
        lax.psum_scatter(down_grad, "dp", scatter_dimension=0, tiled=True),
        lax.psum_scatter(ffn_gain_grad, "dp", scatter_dimension=0, tiled=True),
    )
    residual_cot_b = residual_cot.astype(jnp.bfloat16)
    output_weight_grad = jnp.einsum(
        "th,td->hd", attn_rows, residual_cot_b, preferred_element_type=jnp.float32
    )
    attended_cot = jnp.einsum(
        "td,hd->th", residual_cot_b, out_full, preferred_element_type=jnp.float32
    ).astype(jnp.bfloat16)
    cot_groups = attended_cot.reshape(length, local_groups, per_group, HD).transpose(1, 0, 2, 3)
    query_parts, key_parts, value_parts = lax.map(
        head_backward, (query_groups, key_groups, value_groups, attended, log_norm, cot_groups)
    )
    query_cot = (
        unrotate(query_parts.transpose(1, 0, 2, 3).reshape(length, local_heads, HD), cosine, sine)
        .reshape(length, local_heads * HD)
        .astype(jnp.bfloat16)
    )
    key_cot = (
        unrotate(key_parts.transpose(1, 0, 2), cosine, sine)
        .reshape(length, local_groups * HD)
        .astype(jnp.bfloat16)
    )
    value_cot = (
        value_parts.transpose(1, 0, 2).reshape(length, local_groups * HD).astype(jnp.bfloat16)
    )
    normed_one_part = jnp.einsum(
        "th,dh->td", query_cot, query_full, preferred_element_type=jnp.float32
    )
    normed_one_part = normed_one_part + jnp.einsum(
        "th,dh->td", key_cot, key_full, preferred_element_type=jnp.float32
    )
    normed_one_part = normed_one_part + jnp.einsum(
        "th,dh->td", value_cot, value_full, preferred_element_type=jnp.float32
    )
    normed_one_cot = lax.psum(normed_one_part, "mp")
    query_grad = jnp.einsum("td,th->dh", normed_one, query_cot, preferred_element_type=jnp.float32)
    key_grad = jnp.einsum("td,th->dh", normed_one, key_cot, preferred_element_type=jnp.float32)
    value_grad = jnp.einsum("td,th->dh", normed_one, value_cot, preferred_element_type=jnp.float32)
    attn_gain_grad, input_part = norm_backward(input_f32, inv_one, gain_one, normed_one_cot)
    input_cot = residual_cot + input_part
    input_grad = lax.dynamic_slice_in_dim(input_cot, own_start, local_rows, 0)
    attn_gain_share, query_share, key_share, value_share, output_share = (
        lax.psum_scatter(attn_gain_grad, "dp", scatter_dimension=0, tiled=True),
        lax.psum_scatter(query_grad, "dp", scatter_dimension=0, tiled=True),
        lax.psum_scatter(key_grad, "dp", scatter_dimension=0, tiled=True),
        lax.psum_scatter(value_grad, "dp", scatter_dimension=0, tiled=True),
        lax.psum_scatter(output_weight_grad, "dp", scatter_dimension=0, tiled=True),
    )
    return (
        block_output,
        input_grad,
        attn_gain_share,
        query_share,
        key_share,
        value_share,
        output_share,
        ffn_gain_share,
        gate_share,
        up_share,
        down_share,
    )


GROUP = 4
LANES = 128


def whole_up(size, step):
    return -(-size // step) * step


def partner(values, key):
    pairs = [(at, at ^ key) for at in range(lax.axis_size("dp"))]
    return lax.ppermute(values, "dp", pairs)


def twin(values):
    return lax.ppermute(values, "mp", [(0, 1), (1, 0)])


def across(values, key):
    pairs = [(at, at ^ (key * GROUP)) for at in range(lax.axis_size("dp"))]
    return lax.ppermute(values, "dp", pairs)


SPAN = 14.0


def exponent_of(values):
    top = jnp.max(jnp.abs(values))
    return jnp.clip(jnp.ceil(jnp.log2(jnp.maximum(top, 1e-33))), -108.0, 126.0)


def narrowed(values, exponent):
    scaled = (values * jnp.exp2(SPAN - exponent)).astype(jnp.float16)
    note = jnp.full((8, values.shape[1]), exponent, jnp.float32).astype(jnp.float16)
    return jnp.concatenate([scaled, note], axis=0)


def widened(message):
    exponent = message[-1, 0].astype(jnp.float32)
    return message[:-8].astype(jnp.float32) * jnp.exp2(exponent - SPAN)


def scattered(blocks, at, exchange):
    exponent = exponent_of(blocks)
    total = lax.dynamic_index_in_dim(blocks, at, 0, keepdims=False)
    for key in range(1, blocks.shape[0]):
        away = lax.dynamic_index_in_dim(blocks, at ^ key, 0, keepdims=False)
        total = total + widened(exchange(narrowed(away, exponent), key))
    return total


def group_scatter(blocks, place):
    lines, _, rows, cols = blocks.shape
    exponent = exponent_of(blocks)
    total = lax.dynamic_index_in_dim(blocks, place, 1, keepdims=False)
    for key in range(1, GROUP):
        away = lax.dynamic_index_in_dim(blocks, place ^ key, 1, keepdims=False)
        message = partner(narrowed(away.reshape(lines * rows, cols), exponent), key)
        total = total + widened(message).reshape(lines, rows, cols)
    return total


def group_sum(near, far):
    blocks = near.reshape(GROUP, -1, near.shape[1])
    blocks = blocks + twin(far).reshape(blocks.shape)
    exponent = exponent_of(blocks)
    total = blocks[0]
    for key in range(1, GROUP):
        total = total + widened(partner(narrowed(blocks[key], exponent), key))
    return total


def twin_sum(part, core):
    halves = part.reshape(2, -1, part.shape[1])
    keep = lax.dynamic_index_in_dim(halves, core, 0, keepdims=False)
    away = lax.dynamic_index_in_dim(halves, 1 - core, 0, keepdims=False)
    return keep + twin(away)


def ordered(own, core):
    there = twin(own)
    first = jnp.where(core == 0, own, there)
    second = jnp.where(core == 0, there, own)
    return jnp.concatenate([first, second], axis=0)


MESH = pl.DeviceIdType.MESH


def flipped(place, key):
    if key == 1:
        return place + 1 - 2 * lax.rem(place, 2)
    if key == 2:
        return place + 2 - 4 * lax.div(place, 2)
    return GROUP - 1 - place


class Wires:
    def __init__(self, send_sem):
        self.send_sem, self.used, self.open = send_sem, 0, []

    def send(self, source, target, arrival, device, when=None):
        copy = pltpu.make_async_remote_copy(
            src_ref=source,
            dst_ref=target,
            send_sem=self.send_sem.at[self.used],
            recv_sem=arrival,
            device_id=device,
            device_id_type=MESH,
        )
        self.used += 1
        self.open.append((copy, when))
        if when is None:
            copy.start()
        else:
            pl.when(when)(copy.start)

    def arrived(self, target, arrival, device, when=None):
        copy = pltpu.make_async_remote_copy(
            src_ref=target,
            dst_ref=target,
            send_sem=self.send_sem.at[0],
            recv_sem=arrival,
            device_id=device,
            device_id_type=MESH,
        )
        if when is None:
            copy.wait_recv()
        else:
            pl.when(when)(copy.wait_recv)

    def drain(self):
        for copy, when in self.open:
            if when is None:
                copy.wait_send()
            else:
                pl.when(when)(copy.wait_send)


class Seat:
    def __init__(self, lines):
        self.index = lax.axis_index("dp")
        self.core = lax.axis_index("mp")
        self.own, self.place = lax.div(self.index, GROUP), lax.rem(self.index, GROUP)
        self.lines = lines

    def mate(self, key):
        return (self.own * GROUP + flipped(self.place, key), self.core)

    def line(self, step):
        return ((self.own + step) * GROUP + self.place, self.core)

    def twin(self):
        return (self.index, 1 - self.core)

    def greet(self):
        barrier = pltpu.get_barrier_semaphore()
        for key in range(1, GROUP):
            pl.semaphore_signal(barrier, 1, device_id=self.mate(key), device_id_type=MESH)
        pl.semaphore_signal(barrier, 1, device_id=self.twin(), device_id_type=MESH)
        above, below = self.own < self.lines - 1, self.own > 0

        @pl.when(above)
        def _():
            pl.semaphore_signal(barrier, 1, device_id=self.line(1), device_id_type=MESH)

        @pl.when(below)
        def _():
            pl.semaphore_signal(barrier, 1, device_id=self.line(-1), device_id_type=MESH)

        ends = lax.div(self.own, self.lines - 1) + 1 - lax.div(self.own + self.lines - 1, self.lines)
        pl.semaphore_wait(barrier, GROUP + 2 - ends)


class Staged:
    def __init__(self, sems):
        self.sems, self.used, self.loads, self.stores = sems, 0, [], []

    def add(self, source, middle, target):
        load = pltpu.make_async_copy(source, middle, self.sems.at[self.used])
        store = pltpu.make_async_copy(middle, target, self.sems.at[self.used + 1])
        self.used += 2
        load.start()
        self.loads.append((load, store))

    def forward(self):
        for load, store in self.loads:
            load.wait()
            store.start()
            self.stores.append(store)
        self.loads = []

    def finish(self):
        for store in self.stores:
            store.wait()


def line_hop(wires, seat, arrays, hop):
    lines = seat.lines
    for blocks, arrivals in arrays:
        for step in (1, -1):
            from_block = seat.own - step * (hop - 1)
            into = seat.own + step
            ok = (from_block >= 0) & (from_block < lines) & (into >= 0) & (into < lines)
            block = blocks.at[lax.rem(from_block + lines, lines)]
            wires.send(
                block, block, arrivals.at[lax.rem(from_block + lines, lines)], seat.line(step), ok
            )


def line_landed(wires, seat, arrays, hop):
    lines = seat.lines
    for blocks, arrivals in arrays:
        for step in (1, -1):
            block = seat.own - step * hop
            ok = (block >= 0) & (block < lines)
            block = lax.rem(block + lines, lines)
            wires.arrived(blocks.at[block], arrivals.at[block], seat.twin(), ok)


def spread_own(wires, seat, own, rows, arrivals):
    for key in range(1, GROUP):
        wires.send(own, rows.at[0, key], arrivals.at[0, key], seat.mate(key))
    wires.send(own, rows.at[1, 0], arrivals.at[1, 0], seat.twin())


def spread_on(wires, seat, rows, arrivals):
    for key in range(1, GROUP):
        wires.arrived(rows.at[0, key], arrivals.at[0, key], seat.twin())
        wires.send(rows.at[0, key], rows.at[1, key], arrivals.at[1, key], seat.twin())


def spread_landed(wires, seat, rows, arrivals):
    for key in range(GROUP):
        wires.arrived(rows.at[1, key], arrivals.at[1, key], seat.twin())


def front_kernel(
    lines,
    gains,
    narrow,
    out,
    pieces,
    down,
    inputs,
    cots,
    gains_all,
    narrow_all,
    out_all,
    wide,
    downs,
    seq,
    cot_rows,
    gains_mid,
    narrow_mid,
    out_mid,
    piece_mid,
    down_mid,
    seq_mid,
    cot_mid,
    stage_sem,
    send_sem,
    block_sem,
    mix_sem,
    line_sem,
    cot_sem,
    seq_sem,
):
    seat = Seat(lines)
    wires, staged = Wires(send_sem), Staged(stage_sem)
    index, own, place = seat.index, seat.own, seat.place
    staged.add(pieces.at[place], piece_mid, wide.at[own, place])
    staged.add(down, down_mid, downs.at[own])
    staged.add(gains, gains_mid, gains_all.at[index])
    staged.add(narrow, narrow_mid, narrow_all.at[index])
    staged.add(out, out_mid, out_all.at[index])
    staged.add(inputs, seq_mid, seq.at[seat.core])
    staged.add(cots, cot_mid, cot_rows.at[0, 0])
    seat.greet()
    whole = (
        (gains, gains_all, 0, 1, 2),
        (narrow, narrow_all, 1, 1, 2),
        (out, out_all, 2, 2, 1),
    )

    def block_of(at, key=0):
        return lax.rem(at + lines, lines) * GROUP + (flipped(place, key) if key else place)

    for source, target, which, first, second in whole:
        for step in (1, -1):
            ok = (own + step >= 0) & (own + step < lines)
            wires.send(source, target.at[index], block_sem.at[which, index], seat.line(step), ok)
        for key in (first, second):
            wires.send(source, target.at[index], block_sem.at[which, index], seat.mate(key))
    for key in range(1, GROUP):
        wires.send(
            pieces.at[flipped(place, key)], wide.at[own, place], mix_sem.at[key], seat.mate(key)
        )
    wires.send(inputs, seq.at[seat.core], seq_sem.at[0], seat.twin())
    staged.forward()
    for hop in range(1, lines):
        for _, target, which, first, second in whole:
            for step in (1, -1):
                at = own - step * hop
                ok = (at >= 0) & (at < lines)
                block = block_of(at)
                wires.arrived(target.at[block], block_sem.at[which, block], seat.twin(), ok)
                onward = ok & (own + step >= 0) & (own + step < lines)
                wires.send(
                    target.at[block],
                    target.at[block],
                    block_sem.at[which, block],
                    seat.line(step),
                    onward,
                )
                for key in (first, second):
                    wires.send(
                        target.at[block],
                        target.at[block],
                        block_sem.at[which, block],
                        seat.mate(key),
                        ok,
                    )
        if hop == 1:
            for _, target, which, first, second in whole:
                block = block_of(own, first)
                wires.arrived(target.at[block], block_sem.at[which, block], seat.twin())
                wires.send(
                    target.at[block], target.at[block], block_sem.at[which, block], seat.mate(second)
                )
    staged.finish()
    for key in range(1, GROUP):
        wires.arrived(wide.at[own, flipped(place, key)], mix_sem.at[key], seat.twin())
    ffn = ((wide, line_sem.at[0]), (downs, line_sem.at[1]))
    line_hop(wires, seat, ffn, 1)
    for hop in range(1, lines):
        for _, target, which, first, second in whole:
            for step in (1, -1):
                at = own - step * hop
                ok = (at >= 0) & (at < lines)
                block = block_of(at, first)
                wires.arrived(target.at[block], block_sem.at[which, block], seat.twin(), ok)
                wires.send(
                    target.at[block],
                    target.at[block],
                    block_sem.at[which, block],
                    seat.mate(second),
                    ok,
                )
    spread_own(wires, seat, cots, cot_rows, cot_sem)
    line_landed(wires, seat, ffn, 1)
    line_hop(wires, seat, ffn, 2)
    for _, target, which, first, second in whole:
        for at in range(lines):
            for key in (second, GROUP - 1):
                block = block_of(at, key)
                wires.arrived(target.at[block], block_sem.at[which, block], seat.twin())
    wires.arrived(seq.at[1 - seat.core], seq_sem.at[0], seat.twin())
    spread_on(wires, seat, cot_rows, cot_sem)
    spread_landed(wires, seat, cot_rows, cot_sem)
    line_landed(wires, seat, ffn, 2)
    wires.drain()


ANY = pl.BlockSpec(memory_space=pl.ANY)


def front(gains, narrow, out, pieces, down, inputs, cots):
    members = lax.axis_size("dp")
    lines = members // GROUP
    bf16 = gains.dtype
    sources = (gains, narrow, out, pieces, down, inputs, cots)
    shapes = [(members,) + part.shape for part in (gains, narrow, out)]
    shapes += [
        (lines,) + pieces.shape,
        (lines,) + down.shape,
        (2,) + inputs.shape,
        (2, GROUP) + cots.shape,
    ]
    middles = [part.shape[1:] if part is pieces else part.shape for part in sources]
    whole = 3
    sends = whole * (4 + (lines - 1) * 2 * 3 + 1 + (lines - 1) * 2) + 3 + 1 + 8 + 7
    dma = pltpu.SemaphoreType.DMA
    return pl.pallas_call(
        functools.partial(front_kernel, lines),
        out_shape=[jax.ShapeDtypeStruct(shape, bf16) for shape in shapes],
        in_specs=[ANY] * len(sources),
        out_specs=[ANY] * len(shapes),
        scratch_shapes=[pltpu.VMEM(shape, bf16) for shape in middles]
        + [
            dma((2 * len(sources),)),
            dma((sends,)),
            dma((whole, members)),
            dma((GROUP,)),
            dma((2, lines)),
            dma((2, GROUP)),
            dma((1,)),
        ],
        compiler_params=pltpu.CompilerParams(collective_id=0, has_side_effects=True),
        name="front",
    )(*sources)


def middle_kernel(
    lines,
    normed,
    wide_in,
    downs_in,
    rows,
    wide,
    downs,
    normed_mid,
    stage_sem,
    send_sem,
    row_sem,
    line_sem,
):
    seat = Seat(lines)
    wires, staged = Wires(send_sem), Staged(stage_sem)
    staged.add(normed, normed_mid, rows.at[0, 0])
    seat.greet()
    spread_own(wires, seat, normed, rows, row_sem)
    ffn = ((wide, line_sem.at[0]), (downs, line_sem.at[1]))
    for hop in range(3, lines):
        line_hop(wires, seat, ffn, hop)
    staged.forward()
    spread_on(wires, seat, rows, row_sem)
    spread_landed(wires, seat, rows, row_sem)
    for hop in range(3, lines):
        line_landed(wires, seat, ffn, hop)
    staged.finish()
    wires.drain()


def middle(normed, wide, downs):
    lines = wide.shape[0]
    dma = pltpu.SemaphoreType.DMA
    return pl.pallas_call(
        functools.partial(middle_kernel, lines),
        out_shape=[
            jax.ShapeDtypeStruct((2, GROUP) + normed.shape, normed.dtype),
            jax.ShapeDtypeStruct(wide.shape, wide.dtype),
            jax.ShapeDtypeStruct(downs.shape, downs.dtype),
        ],
        in_specs=[ANY] * 3,
        out_specs=[ANY] * 3,
        scratch_shapes=[
            pltpu.VMEM(normed.shape, normed.dtype),
            dma((2,)),
            dma((7 + 4,)),
            dma((2, GROUP)),
            dma((2, lines)),
        ],
        input_output_aliases={1: 1, 2: 2},
        compiler_params=pltpu.CompilerParams(collective_id=1, has_side_effects=True),
        name="middle",
    )(normed, wide, downs)


def grouped_shards(
    block_input,
    attn_gain,
    query_weight,
    key_weight,
    value_weight,
    output_weight,
    ffn_gain,
    gate_weight,
    up_weight,
    down_weight,
    output_cotangent,
):
    f32, bf16 = jnp.float32, jnp.bfloat16
    members = lax.axis_size("dp")
    lines = members // GROUP
    index = lax.axis_index("dp")
    own, place = index // GROUP, lax.rem(index, GROUP)
    core = lax.axis_index("mp")
    rows, units = gate_weight.shape
    width = rows * members
    query_cols, key_cols = query_weight.shape[1], key_weight.shape[1]
    unit_rows = down_weight.shape[0]
    share = unit_rows * lines
    padded = whole_up(share, LANES)

    narrow = jnp.concatenate([query_weight, key_weight, value_weight], axis=1)
    cols = narrow.shape[1]
    gains = jnp.stack([attn_gain, ffn_gain])
    gains = jnp.pad(gains, ((0, 6), (0, whole_up(rows, LANES) - rows)))

    def shares(weight):
        parts = weight.reshape(rows, lines, GROUP, unit_rows).transpose(2, 0, 1, 3)
        return jnp.pad(parts.reshape(GROUP, rows, share), ((0, 0), (0, 0), (0, padded - share)))

    pieces = jnp.concatenate([shares(gate_weight), shares(up_weight)], axis=2)
    gains_all, narrow_all, out_all, wide, downs, seq_input, cot_rows = front(
        gains, narrow, output_weight, pieces, down_weight, block_input, output_cotangent
    )
    narrow_full = narrow_all.reshape(width, cols)
    gain_one = gains_all[:, 0, :rows].reshape(width)
    gain_two = gains_all[:, 1, :rows].reshape(width)
    out_full = out_all.reshape(-1, width)
    seq_input = seq_input.reshape(-1, width)
    cot_rows = cot_rows.reshape(-1, width)

    length = seq_input.shape[0]
    local_heads = query_cols // HD
    local_groups = key_cols // HD
    per_group = local_heads // local_groups
    cosine, sine = rope_tables(length, HD)
    input_f32 = seq_input.astype(f32)
    normed_one = (input_f32 * norm_scale(input_f32) * gain_one.astype(f32)[None, :]).astype(bf16)
    raw = jnp.dot(normed_one, narrow_full, preferred_element_type=f32)
    query_raw = raw[:, :query_cols]
    key_raw = raw[:, query_cols : query_cols + key_cols]
    value_raw = raw[:, query_cols + key_cols :]
    query_rot = rotate(query_raw.reshape(length, local_heads, HD), cosine, sine).astype(bf16)
    key_rot = rotate(key_raw.reshape(length, local_groups, HD), cosine, sine).astype(bf16)
    value_b = value_raw.astype(bf16)
    query_groups = query_rot.reshape(length, local_groups, per_group, HD).transpose(1, 0, 2, 3)
    key_groups = key_rot.transpose(1, 0, 2)
    value_groups = value_b.reshape(length, local_groups, HD).transpose(1, 0, 2)
    attended, log_norm = lax.map(head_forward, (query_groups, key_groups, value_groups))
    attn_rows = attended.transpose(1, 0, 2, 3).reshape(length, local_heads * HD)
    attn_part = jnp.dot(attn_rows, out_full, preferred_element_type=f32)
    own_f32 = block_input.astype(f32)
    residual = own_f32 + twin_sum(attn_part, core)
    inv_two = norm_scale(residual)
    normed_two = (residual * inv_two * gain_two.astype(f32)[None, :]).astype(bf16)

    ffn_rows, wide, downs = middle(normed_two, wide, downs)
    ffn_rows = ffn_rows.reshape(-1, width)
    wide_full = wide.reshape(width, 2 * padded)
    down_share = jnp.pad(downs.reshape(share, width), ((0, padded - share), (0, 0)))
    both_raw = jnp.dot(ffn_rows, wide_full, preferred_element_type=f32)
    gate_raw, up_raw = both_raw[:, :padded], both_raw[:, padded:]
    sigma = jax.nn.sigmoid(gate_raw)
    hidden = (gate_raw * sigma * up_raw).astype(bf16)
    hidden_cot = jnp.einsum("td,fd->tf", cot_rows, down_share, preferred_element_type=f32)
    gate_cot = (hidden_cot * up_raw * sigma * (1.0 + gate_raw * (1.0 - sigma))).astype(bf16)
    up_cot = (hidden_cot * gate_raw * sigma).astype(bf16)
    both_cot = jnp.concatenate([gate_cot, up_cot], axis=1)
    half = ffn_rows.shape[0] // 2

    def back(part):
        return jnp.einsum("tf,df->td", part, wide_full, preferred_element_type=f32)

    normed_two_cot = group_sum(back(both_cot[:half]), back(both_cot[half:]))

    def forth(part):
        return jnp.dot(part, down_share, preferred_element_type=f32)

    ffn_out = group_sum(forth(hidden[:half]), forth(hidden[half:]))
    block_output = (residual + ffn_out).astype(bf16)
    wide_grad = jnp.einsum("td,tf->df", ffn_rows, both_cot, preferred_element_type=f32)
    down_grad = jnp.einsum("tf,td->fd", hidden, cot_rows, preferred_element_type=f32)

    down_own = scattered(down_grad[:share].reshape(lines, unit_rows, width), own, across)
    wide_own = scattered(wide_grad.reshape(lines, GROUP * rows, 2 * padded), own, across)
    wide_own = wide_own.reshape(GROUP, rows, 2 * padded)
    exponent = exponent_of(wide_own)
    wide_mixed = jnp.zeros(wide_own.shape, f32)
    for key in range(GROUP):
        other = place ^ key
        piece = lax.dynamic_index_in_dim(wide_own, other, 0, keepdims=False)
        if key:
            piece = widened(partner(narrowed(piece, exponent), key))
        wide_mixed = lax.dynamic_update_index_in_dim(wide_mixed, piece, other, 0)

    def unshared(parts):
        parts = parts[:, :, :share].reshape(GROUP, rows, lines, unit_rows)
        return parts.transpose(1, 2, 0, 3).reshape(rows, units)

    gate_own = unshared(wide_mixed[:, :, :padded])
    up_own = unshared(wide_mixed[:, :, padded:])

    ffn_gain_part, residual_part = norm_backward(residual, inv_two, gain_two, normed_two_cot)
    residual_cot = output_cotangent.astype(f32) + residual_part
    residual_cot_b = ordered(residual_cot.astype(bf16), core)
    out_grad = jnp.einsum("th,td->hd", attn_rows, residual_cot_b, preferred_element_type=f32)
    out_own = scattered(group_scatter(out_grad.reshape(lines, GROUP, -1, width), place), own, across)
    attended_cot = jnp.einsum(
        "td,hd->th", residual_cot_b, out_full, preferred_element_type=f32
    ).astype(bf16)
    cot_groups = attended_cot.reshape(length, local_groups, per_group, HD).transpose(1, 0, 2, 3)
    query_parts, key_parts, value_parts = lax.map(
        head_backward, (query_groups, key_groups, value_groups, attended, log_norm, cot_groups)
    )
    query_cot = unrotate(
        query_parts.transpose(1, 0, 2, 3).reshape(length, local_heads, HD), cosine, sine
    ).reshape(length, local_heads * HD)
    key_cot = unrotate(key_parts.transpose(1, 0, 2), cosine, sine).reshape(length, key_cols)
    value_cot = value_parts.transpose(1, 0, 2).reshape(length, key_cols)
    narrow_cot = jnp.concatenate(
        [query_cot.astype(bf16), key_cot.astype(bf16), value_cot.astype(bf16)], axis=1
    )
    normed_one_part = jnp.einsum("th,dh->td", narrow_cot, narrow_full, preferred_element_type=f32)
    normed_one_cot = twin_sum(normed_one_part, core)
    attn_gain_part, input_part = norm_backward(
        own_f32, norm_scale(own_f32), gain_one, normed_one_cot
    )
    input_grad = residual_cot + input_part
    narrow_grad = jnp.einsum("td,th->dh", normed_one, narrow_cot, preferred_element_type=f32)
    gain_parts = jnp.stack([attn_gain_part, ffn_gain_part])
    gain_parts = gain_parts + twin(gain_parts)
    gain_parts = gain_parts.reshape(2, members, rows).transpose(1, 0, 2)
    gain_parts = jnp.pad(gain_parts, ((0, 0), (0, 6), (0, cols - rows)))
    narrow_grad = jnp.concatenate([narrow_grad.reshape(members, rows, cols), gain_parts], axis=1)
    narrow_own = scattered(
        group_scatter(narrow_grad.reshape(lines, GROUP, -1, cols), place), own, across
    )
    return (
        block_output,
        input_grad,
        narrow_own[rows, :rows],
        narrow_own[:rows, :query_cols],
        narrow_own[:rows, query_cols : query_cols + key_cols],
        narrow_own[:rows, query_cols + key_cols :],
        out_own,
        narrow_own[rows + 1, :rows],
        gate_own,
        up_own,
        down_own,
    )


def solution(mesh):
    placed = (
        P(("dp", "mp"), None),
        P("dp"),
        P("dp", "mp"),
        P("dp", "mp"),
        P("dp", "mp"),
        P(("mp", "dp"), None),
        P("dp"),
        P("dp", "mp"),
        P("dp", "mp"),
        P(("mp", "dp"), None),
        P(("dp", "mp"), None),
    )
    members = mesh.shape["dp"]
    fits = mesh.shape["mp"] == 2 and members in (2 * GROUP, 4 * GROUP)
    return jax.shard_map(
        grouped_shards if fits else plain_shards,
        mesh=mesh,
        in_specs=placed,
        out_specs=(
            P(("dp", "mp"), None),
            P(("dp", "mp"), None),
            P("dp"),
            P("dp", "mp"),
            P("dp", "mp"),
            P("dp", "mp"),
            P(("mp", "dp"), None),
            P("dp"),
            P("dp", "mp"),
            P("dp", "mp"),
            P(("mp", "dp"), None),
        ),
        check_vma=False,
    )
```

```python
import functools

import jax
import jax.numpy as jnp
from jax import lax
from jax.experimental import pallas as pl
from jax.experimental.pallas import tpu as pltpu
from jax.sharding import PartitionSpec as P

HD = 64


EPSILON = 1e-05
ROPE_BASE = 10000.0


def rope_tables(length, head_dim):
    half_dim = head_dim // 2
    position = jnp.arange(length, dtype=jnp.float32)
    inverse = ROPE_BASE ** (-(jnp.arange(half_dim, dtype=jnp.float32) * (2.0 / head_dim)))
    angle = position[:, None] * inverse[None, :]
    return (jnp.cos(angle), jnp.sin(angle))


def rotate(values, cosine, sine):
    half_dim = values.shape[-1] // 2
    first_half = values[..., :half_dim]
    second_half = values[..., half_dim:]
    cos_part = cosine[:, None, :]
    sin_part = sine[:, None, :]
    return jnp.concatenate(
        [
            first_half * cos_part - second_half * sin_part,
            second_half * cos_part + first_half * sin_part,
        ],
        axis=-1,
    )


def unrotate(values, cosine, sine):
    half_dim = values.shape[-1] // 2
    first_half = values[..., :half_dim]
    second_half = values[..., half_dim:]
    cos_part = cosine[:, None, :]
    sin_part = sine[:, None, :]
    return jnp.concatenate(
        [
            first_half * cos_part + second_half * sin_part,
            second_half * cos_part - first_half * sin_part,
        ],
        axis=-1,
    )


def norm_scale(values):
    return lax.rsqrt(jnp.mean(values * values, axis=-1, keepdims=True) + EPSILON)


def norm_backward(values, inverse, gain, normed_cot):
    scaled = normed_cot * gain.astype(jnp.float32)[None, :]
    gain_grad = jnp.sum(normed_cot * values * inverse, axis=0)
    values_grad = inverse * scaled - values * (inverse * inverse * inverse) * jnp.mean(
        scaled * values, axis=-1, keepdims=True
    )
    return (gain_grad, values_grad)


def causal_scores(query_group, key_group):
    scale = query_group.shape[-1] ** (-0.5)
    scores = (
        jnp.einsum("qgd,kd->gqk", query_group, key_group, preferred_element_type=jnp.float32)
        * scale
    )
    length = key_group.shape[0]
    visible = lax.broadcasted_iota(jnp.int32, (length, length), 0) >= lax.broadcasted_iota(
        jnp.int32, (length, length), 1
    )
    return jnp.where(visible[None], scores, -jnp.inf)


def head_forward(parts):
    query_group, key_group, value_group = parts
    scores = causal_scores(query_group, key_group)
    top_score = jnp.max(scores, axis=-1, keepdims=True)
    log_norm = top_score + jnp.log(jnp.sum(jnp.exp(scores - top_score), axis=-1, keepdims=True))
    probs_b = jnp.exp(scores - log_norm).astype(jnp.bfloat16)
    attended = jnp.einsum(
        "gqk,kd->qgd", probs_b, value_group, preferred_element_type=jnp.float32
    ).astype(jnp.bfloat16)
    return (attended, log_norm[..., 0])


def head_backward(parts):
    query_group, key_group, value_group, attended, log_norm, attended_cot = parts
    scale = query_group.shape[-1] ** (-0.5)
    scores = causal_scores(query_group, key_group)
    probs = jnp.exp(scores - log_norm[..., None])
    probs_b = probs.astype(jnp.bfloat16)
    value_cot = jnp.einsum("gqk,qgd->kd", probs_b, attended_cot, preferred_element_type=jnp.float32)
    probs_cot = jnp.einsum(
        "qgd,kd->gqk", attended_cot, value_group, preferred_element_type=jnp.float32
    )
    delta = jnp.sum(attended_cot.astype(jnp.float32) * attended.astype(jnp.float32), axis=-1).T
    score_cot = (probs * (probs_cot - delta[:, :, None])).astype(jnp.bfloat16)
    query_cot = (
        jnp.einsum("gqk,kd->qgd", score_cot, key_group, preferred_element_type=jnp.float32) * scale
    )
    key_cot = (
        jnp.einsum("gqk,qgd->kd", score_cot, query_group, preferred_element_type=jnp.float32)
        * scale
    )
    return (query_cot, key_cot, value_cot)


def plain_shards(
    block_input,
    attn_gain,
    query_weight,
    key_weight,
    value_weight,
    output_weight,
    ffn_gain,
    gate_weight,
    up_weight,
    down_weight,
    output_cotangent,
):
    local_rows = block_input.shape[0]
    own_start = lax.axis_index("mp") * local_rows
    query_full, key_full, value_full, out_full, gain_one = (
        lax.all_gather(query_weight, "dp", axis=0, tiled=True),
        lax.all_gather(key_weight, "dp", axis=0, tiled=True),
        lax.all_gather(value_weight, "dp", axis=0, tiled=True),
        lax.all_gather(output_weight, "dp", axis=0, tiled=True),
        lax.all_gather(attn_gain, "dp", axis=0, tiled=True),
    )
    seq_input = lax.all_gather(block_input, "mp", axis=0, tiled=True)
    length = seq_input.shape[0]
    local_heads = query_full.shape[1] // HD
    local_groups = key_full.shape[1] // HD
    per_group = local_heads // local_groups
    cosine, sine = rope_tables(length, HD)
    input_f32 = seq_input.astype(jnp.float32)
    inv_one = norm_scale(input_f32)
    normed_one = (input_f32 * inv_one * gain_one.astype(jnp.float32)[None, :]).astype(jnp.bfloat16)
    query_raw = jnp.dot(normed_one, query_full, preferred_element_type=jnp.float32)
    key_raw = jnp.dot(normed_one, key_full, preferred_element_type=jnp.float32)
    value_raw = jnp.dot(normed_one, value_full, preferred_element_type=jnp.float32)
    query_rot = rotate(query_raw.reshape(length, local_heads, HD), cosine, sine).astype(
        jnp.bfloat16
    )
    key_rot = rotate(key_raw.reshape(length, local_groups, HD), cosine, sine).astype(jnp.bfloat16)
    value_b = value_raw.astype(jnp.bfloat16)
    query_groups = query_rot.reshape(length, local_groups, per_group, HD).transpose(1, 0, 2, 3)
    key_groups = key_rot.transpose(1, 0, 2)
    value_groups = value_b.reshape(length, local_groups, HD).transpose(1, 0, 2)
    attended, log_norm = lax.map(head_forward, (query_groups, key_groups, value_groups))
    attn_rows = attended.transpose(1, 0, 2, 3).reshape(length, local_heads * HD)
    attn_part = jnp.dot(attn_rows, out_full, preferred_element_type=jnp.float32)
    residual = input_f32 + lax.psum(attn_part, "mp")
    gate_full, up_full, down_full, gain_two = (
        lax.all_gather(gate_weight, "dp", axis=0, tiled=True),
        lax.all_gather(up_weight, "dp", axis=0, tiled=True),
        lax.all_gather(down_weight, "dp", axis=0, tiled=True),
        lax.all_gather(ffn_gain, "dp", axis=0, tiled=True),
    )
    inv_two = norm_scale(residual)
    normed_two = (residual * inv_two * gain_two.astype(jnp.float32)[None, :]).astype(jnp.bfloat16)
    gate_raw = jnp.dot(normed_two, gate_full, preferred_element_type=jnp.float32)
    up_raw = jnp.dot(normed_two, up_full, preferred_element_type=jnp.float32)
    sigma = jax.nn.sigmoid(gate_raw)
    hidden = (gate_raw * sigma * up_raw).astype(jnp.bfloat16)
    ffn_own = lax.psum_scatter(
        jnp.dot(hidden, down_full, preferred_element_type=jnp.float32),
        "mp",
        scatter_dimension=0,
        tiled=True,
    )
    residual_own = lax.dynamic_slice_in_dim(residual, own_start, local_rows, 0)
    block_output = (residual_own + ffn_own).astype(jnp.bfloat16)
    cot_seq = lax.all_gather(output_cotangent, "mp", axis=0, tiled=True)
    hidden_cot = jnp.einsum("td,fd->tf", cot_seq, down_full, preferred_element_type=jnp.float32)
    gate_cot = (hidden_cot * up_raw * sigma * (1.0 + gate_raw * (1.0 - sigma))).astype(jnp.bfloat16)
    up_cot = (hidden_cot * gate_raw * sigma).astype(jnp.bfloat16)
    normed_two_part = jnp.einsum(
        "tf,df->td", gate_cot, gate_full, preferred_element_type=jnp.float32
    )
    normed_two_part = normed_two_part + jnp.einsum(
        "tf,df->td", up_cot, up_full, preferred_element_type=jnp.float32
    )
    normed_two_cot = lax.psum(normed_two_part, "mp")
    ffn_gain_grad, residual_part = norm_backward(residual, inv_two, gain_two, normed_two_cot)
    residual_cot = cot_seq.astype(jnp.float32) + residual_part
    down_grad = jnp.einsum("tf,td->fd", hidden, cot_seq, preferred_element_type=jnp.float32)
    gate_grad = jnp.einsum("td,tf->df", normed_two, gate_cot, preferred_element_type=jnp.float32)
    up_grad = jnp.einsum("td,tf->df", normed_two, up_cot, preferred_element_type=jnp.float32)
    gate_share, up_share, down_share, ffn_gain_share = (
        lax.psum_scatter(gate_grad, "dp", scatter_dimension=0, tiled=True),
        lax.psum_scatter(up_grad, "dp", scatter_dimension=0, tiled=True),
        lax.psum_scatter(down_grad, "dp", scatter_dimension=0, tiled=True),
        lax.psum_scatter(ffn_gain_grad, "dp", scatter_dimension=0, tiled=True),
    )
    residual_cot_b = residual_cot.astype(jnp.bfloat16)
    output_weight_grad = jnp.einsum(
        "th,td->hd", attn_rows, residual_cot_b, preferred_element_type=jnp.float32
    )
    attended_cot = jnp.einsum(
        "td,hd->th", residual_cot_b, out_full, preferred_element_type=jnp.float32
    ).astype(jnp.bfloat16)
    cot_groups = attended_cot.reshape(length, local_groups, per_group, HD).transpose(1, 0, 2, 3)
    query_parts, key_parts, value_parts = lax.map(
        head_backward, (query_groups, key_groups, value_groups, attended, log_norm, cot_groups)
    )
    query_cot = (
        unrotate(query_parts.transpose(1, 0, 2, 3).reshape(length, local_heads, HD), cosine, sine)
        .reshape(length, local_heads * HD)
        .astype(jnp.bfloat16)
    )
    key_cot = (
        unrotate(key_parts.transpose(1, 0, 2), cosine, sine)
        .reshape(length, local_groups * HD)
        .astype(jnp.bfloat16)
    )
    value_cot = (
        value_parts.transpose(1, 0, 2).reshape(length, local_groups * HD).astype(jnp.bfloat16)
    )
    normed_one_part = jnp.einsum(
        "th,dh->td", query_cot, query_full, preferred_element_type=jnp.float32
    )
    normed_one_part = normed_one_part + jnp.einsum(
        "th,dh->td", key_cot, key_full, preferred_element_type=jnp.float32
    )
    normed_one_part = normed_one_part + jnp.einsum(
        "th,dh->td", value_cot, value_full, preferred_element_type=jnp.float32
    )
    normed_one_cot = lax.psum(normed_one_part, "mp")
    query_grad = jnp.einsum("td,th->dh", normed_one, query_cot, preferred_element_type=jnp.float32)
    key_grad = jnp.einsum("td,th->dh", normed_one, key_cot, preferred_element_type=jnp.float32)
    value_grad = jnp.einsum("td,th->dh", normed_one, value_cot, preferred_element_type=jnp.float32)
    attn_gain_grad, input_part = norm_backward(input_f32, inv_one, gain_one, normed_one_cot)
    input_cot = residual_cot + input_part
    input_grad = lax.dynamic_slice_in_dim(input_cot, own_start, local_rows, 0)
    attn_gain_share, query_share, key_share, value_share, output_share = (
        lax.psum_scatter(attn_gain_grad, "dp", scatter_dimension=0, tiled=True),
        lax.psum_scatter(query_grad, "dp", scatter_dimension=0, tiled=True),
        lax.psum_scatter(key_grad, "dp", scatter_dimension=0, tiled=True),
        lax.psum_scatter(value_grad, "dp", scatter_dimension=0, tiled=True),
        lax.psum_scatter(output_weight_grad, "dp", scatter_dimension=0, tiled=True),
    )
    return (
        block_output,
        input_grad,
        attn_gain_share,
        query_share,
        key_share,
        value_share,
        output_share,
        ffn_gain_share,
        gate_share,
        up_share,
        down_share,
    )


GROUP = 4
LANES = 128


def whole_up(size, step):
    return -(-size // step) * step


def partner(values, key):
    pairs = [(at, at ^ key) for at in range(lax.axis_size("dp"))]
    return lax.ppermute(values, "dp", pairs)


def twin(values):
    return lax.ppermute(values, "mp", [(0, 1), (1, 0)])


def across(values, key):
    pairs = [(at, at ^ (key * GROUP)) for at in range(lax.axis_size("dp"))]
    return lax.ppermute(values, "dp", pairs)


SPAN = 14.0


def after(value, *marks):
    return lax.optimization_barrier((value,) + marks)[0]


def scales_of(values):
    top = jnp.max(jnp.abs(values), axis=tuple(range(values.ndim - 1)))
    power = jnp.clip(jnp.ceil(jnp.log2(jnp.maximum(top, 1e-33))), -100.0, 126.0) - SPAN
    eighth = jnp.round(power * 0.125)
    rest = power - 8.0 * eighth
    row = lax.broadcasted_iota(jnp.int32, (8, power.shape[0]), 0)
    return lax.optimization_barrier(
        (jnp.exp2(-power), jnp.exp2(jnp.where(row < 4, eighth[None, :], rest[None, :])))
    )


def narrowed(values, scales):
    scale, notes = scales
    return jnp.concatenate([values * scale, notes], axis=0).astype(jnp.float16)


def widened(message):
    root = message[-8:-7].astype(jnp.float32)
    values = message[:-8].astype(jnp.float32) * message[-1:].astype(jnp.float32)
    for _ in range(8):
        values = values * root
    return values


def messages_of(blocks, scales, at):
    return [
        narrowed(lax.dynamic_index_in_dim(blocks, at ^ key, 0, keepdims=False), scales)
        for key in range(1, blocks.shape[0])
    ]


def exchanged(messages, exchange):
    return [exchange(message, key + 1) for key, message in enumerate(messages)]


def added(total, messages):
    for message in messages:
        total = total + widened(message).reshape(total.shape)
    return total


def group_messages(blocks, place):
    lines, _, rows, cols = blocks.shape
    scales = scales_of(blocks)
    return [
        narrowed(
            lax.dynamic_index_in_dim(blocks, place ^ key, 1, keepdims=False).reshape(-1, cols),
            scales,
        )
        for key in range(1, GROUP)
    ]


def by_place(pieces, place):
    for bit in (1, 2):
        swap = (place & bit) != 0
        pieces = [jnp.where(swap, pieces[key ^ bit], pieces[key]) for key in range(GROUP)]
    return pieces


def twin_sum(part, core):
    halves = part.reshape(2, -1, part.shape[1])
    keep = lax.dynamic_index_in_dim(halves, core, 0, keepdims=False)
    away = lax.dynamic_index_in_dim(halves, 1 - core, 0, keepdims=False)
    return keep + twin(away)


def ordered(own, core):
    there = twin(own)
    first = jnp.where(core == 0, own, there)
    second = jnp.where(core == 0, there, own)
    return jnp.concatenate([first, second], axis=0)


MESH = pl.DeviceIdType.MESH


def flipped(place, key):
    if key == 1:
        return place + 1 - 2 * lax.rem(place, 2)
    if key == 2:
        return place + 2 - 4 * lax.div(place, 2)
    return GROUP - 1 - place


class Wires:
    def __init__(self, send_sem):
        self.send_sem, self.used, self.open = send_sem, 0, []

    def send(self, source, target, arrival, device, when=None):
        copy = pltpu.make_async_remote_copy(
            src_ref=source,
            dst_ref=target,
            send_sem=self.send_sem.at[self.used],
            recv_sem=arrival,
            device_id=device,
            device_id_type=MESH,
        )
        self.used += 1
        self.open.append((copy, when))
        if when is None:
            copy.start()
        else:
            pl.when(when)(copy.start)

    def arrived(self, target, arrival, device, when=None):
        copy = pltpu.make_async_remote_copy(
            src_ref=target,
            dst_ref=target,
            send_sem=self.send_sem.at[0],
            recv_sem=arrival,
            device_id=device,
            device_id_type=MESH,
        )
        if when is None:
            copy.wait_recv()
        else:
            pl.when(when)(copy.wait_recv)

    def drain(self):
        for copy, when in self.open:
            if when is None:
                copy.wait_send()
            else:
                pl.when(when)(copy.wait_send)


class Seat:
    def __init__(self, lines):
        self.index = lax.axis_index("dp")
        self.core = lax.axis_index("mp")
        self.own, self.place = lax.div(self.index, GROUP), lax.rem(self.index, GROUP)
        self.lines = lines

    def mate(self, key):
        return (self.own * GROUP + flipped(self.place, key), self.core)

    def line(self, step):
        return ((self.own + step) * GROUP + self.place, self.core)

    def twin(self):
        return (self.index, 1 - self.core)

    def greet(self):
        barrier = pltpu.get_barrier_semaphore()
        for key in range(1, GROUP):
            pl.semaphore_signal(barrier, 1, device_id=self.mate(key), device_id_type=MESH)
        pl.semaphore_signal(barrier, 1, device_id=self.twin(), device_id_type=MESH)
        above, below = self.own < self.lines - 1, self.own > 0

        @pl.when(above)
        def _():
            pl.semaphore_signal(barrier, 1, device_id=self.line(1), device_id_type=MESH)

        @pl.when(below)
        def _():
            pl.semaphore_signal(barrier, 1, device_id=self.line(-1), device_id_type=MESH)

        ends = lax.div(self.own, self.lines - 1) + 1 - lax.div(self.own + self.lines - 1, self.lines)
        pl.semaphore_wait(barrier, GROUP + 2 - ends)


class Staged:
    def __init__(self, sems):
        self.sems, self.used, self.loads, self.stores = sems, 0, [], []

    def add(self, source, middle, target):
        load = pltpu.make_async_copy(source, middle, self.sems.at[self.used])
        store = pltpu.make_async_copy(middle, target, self.sems.at[self.used + 1])
        self.used += 2
        load.start()
        self.loads.append((load, store))

    def forward(self):
        for load, store in self.loads:
            load.wait()
            store.start()
            self.stores.append(store)
        self.loads = []

    def finish(self):
        for store in self.stores:
            store.wait()


def line_hop(wires, seat, arrays, hop):
    lines = seat.lines
    for blocks, arrivals in arrays:
        for step in (1, -1):
            from_block = seat.own - step * (hop - 1)
            into = seat.own + step
            ok = (from_block >= 0) & (from_block < lines) & (into >= 0) & (into < lines)
            block = blocks.at[lax.rem(from_block + lines, lines)]
            wires.send(
                block, block, arrivals.at[lax.rem(from_block + lines, lines)], seat.line(step), ok
            )


def line_landed(wires, seat, arrays, hop):
    lines = seat.lines
    for blocks, arrivals in arrays:
        for step in (1, -1):
            block = seat.own - step * hop
            ok = (block >= 0) & (block < lines)
            block = lax.rem(block + lines, lines)
            wires.arrived(blocks.at[block], arrivals.at[block], seat.twin(), ok)


def spread_own(wires, seat, own, rows, arrivals):
    for key in range(1, GROUP):
        wires.send(own, rows.at[0, key], arrivals.at[0, key], seat.mate(key))
    wires.send(own, rows.at[1, 0], arrivals.at[1, 0], seat.twin())


def spread_on(wires, seat, rows, arrivals):
    for key in range(1, GROUP):
        wires.arrived(rows.at[0, key], arrivals.at[0, key], seat.twin())
        wires.send(rows.at[0, key], rows.at[1, key], arrivals.at[1, key], seat.twin())


def spread_landed(wires, seat, rows, arrivals):
    for key in range(GROUP):
        wires.arrived(rows.at[1, key], arrivals.at[1, key], seat.twin())


def front_kernel(
    lines,
    gains,
    narrow,
    out,
    pieces,
    down,
    inputs,
    cots,
    gains_all,
    narrow_all,
    out_all,
    wide,
    downs,
    seq,
    cot_rows,
    gains_mid,
    narrow_mid,
    out_mid,
    piece_mid,
    down_mid,
    seq_mid,
    cot_mid,
    stage_sem,
    send_sem,
    block_sem,
    mix_sem,
    line_sem,
    cot_sem,
    seq_sem,
):
    seat = Seat(lines)
    wires, staged = Wires(send_sem), Staged(stage_sem)
    index, own, place = seat.index, seat.own, seat.place
    staged.add(pieces.at[place], piece_mid, wide.at[own, place])
    staged.add(down, down_mid, downs.at[own])
    staged.add(gains, gains_mid, gains_all.at[index])
    staged.add(narrow, narrow_mid, narrow_all.at[index])
    staged.add(out, out_mid, out_all.at[index])
    staged.add(inputs, seq_mid, seq.at[seat.core])
    staged.add(cots, cot_mid, cot_rows.at[0, 0])
    seat.greet()
    whole = (
        (gains, gains_all, 0, 1, 2),
        (narrow, narrow_all, 1, 1, 2),
        (out, out_all, 2, 2, 1),
    )

    def block_of(at, key=0):
        return lax.rem(at + lines, lines) * GROUP + (flipped(place, key) if key else place)

    for source, target, which, first, second in whole:
        for step in (1, -1):
            ok = (own + step >= 0) & (own + step < lines)
            wires.send(source, target.at[index], block_sem.at[which, index], seat.line(step), ok)
        for key in (first, second):
            wires.send(source, target.at[index], block_sem.at[which, index], seat.mate(key))
    for key in range(1, GROUP):
        wires.send(
            pieces.at[flipped(place, key)], wide.at[own, place], mix_sem.at[key], seat.mate(key)
        )
    wires.send(inputs, seq.at[seat.core], seq_sem.at[0], seat.twin())
    staged.forward()
    for hop in range(1, lines):
        for _, target, which, first, second in whole:
            for step in (1, -1):
                at = own - step * hop
                ok = (at >= 0) & (at < lines)
                block = block_of(at)
                wires.arrived(target.at[block], block_sem.at[which, block], seat.twin(), ok)
                onward = ok & (own + step >= 0) & (own + step < lines)
                wires.send(
                    target.at[block],
                    target.at[block],
                    block_sem.at[which, block],
                    seat.line(step),
                    onward,
                )
                for key in (first, second):
                    wires.send(
                        target.at[block],
                        target.at[block],
                        block_sem.at[which, block],
                        seat.mate(key),
                        ok,
                    )
        if hop == 1:
            for _, target, which, first, second in whole:
                block = block_of(own, first)
                wires.arrived(target.at[block], block_sem.at[which, block], seat.twin())
                wires.send(
                    target.at[block], target.at[block], block_sem.at[which, block], seat.mate(second)
                )
    staged.finish()
    for key in range(1, GROUP):
        wires.arrived(wide.at[own, flipped(place, key)], mix_sem.at[key], seat.twin())
    ffn = ((wide, line_sem.at[0]), (downs, line_sem.at[1]))
    line_hop(wires, seat, ffn, 1)
    for hop in range(1, lines):
        for _, target, which, first, second in whole:
            for step in (1, -1):
                at = own - step * hop
                ok = (at >= 0) & (at < lines)
                block = block_of(at, first)
                wires.arrived(target.at[block], block_sem.at[which, block], seat.twin(), ok)
                wires.send(
                    target.at[block],
                    target.at[block],
                    block_sem.at[which, block],
                    seat.mate(second),
                    ok,
                )
    spread_own(wires, seat, cots, cot_rows, cot_sem)
    line_landed(wires, seat, ffn, 1)
    line_hop(wires, seat, ffn, 2)
    for _, target, which, first, second in whole:
        for at in range(lines):
            for key in (second, GROUP - 1):
                block = block_of(at, key)
                wires.arrived(target.at[block], block_sem.at[which, block], seat.twin())
    wires.arrived(seq.at[1 - seat.core], seq_sem.at[0], seat.twin())
    spread_on(wires, seat, cot_rows, cot_sem)
    spread_landed(wires, seat, cot_rows, cot_sem)
    line_landed(wires, seat, ffn, 2)
    wires.drain()


ANY = pl.BlockSpec(memory_space=pl.ANY)


def front(gains, narrow, out, pieces, down, inputs, cots):
    members = lax.axis_size("dp")
    lines = members // GROUP
    bf16 = gains.dtype
    sources = (gains, narrow, out, pieces, down, inputs, cots)
    shapes = [(members,) + part.shape for part in (gains, narrow, out)]
    shapes += [
        (lines,) + pieces.shape,
        (lines,) + down.shape,
        (2,) + inputs.shape,
        (2, GROUP) + cots.shape,
    ]
    middles = [part.shape[1:] if part is pieces else part.shape for part in sources]
    whole = 3
    sends = whole * (4 + (lines - 1) * 2 * 3 + 1 + (lines - 1) * 2) + 3 + 1 + 8 + 7
    dma = pltpu.SemaphoreType.DMA
    return pl.pallas_call(
        functools.partial(front_kernel, lines),
        out_shape=[jax.ShapeDtypeStruct(shape, bf16) for shape in shapes],
        in_specs=[ANY] * len(sources),
        out_specs=[ANY] * len(shapes),
        scratch_shapes=[pltpu.VMEM(shape, bf16) for shape in middles]
        + [
            dma((2 * len(sources),)),
            dma((sends,)),
            dma((whole, members)),
            dma((GROUP,)),
            dma((2, lines)),
            dma((2, GROUP)),
            dma((1,)),
        ],
        compiler_params=pltpu.CompilerParams(collective_id=0, has_side_effects=True),
        name="front",
    )(*sources)


def middle_kernel(
    lines,
    normed,
    wide_in,
    downs_in,
    rows,
    wide,
    downs,
    normed_mid,
    stage_sem,
    send_sem,
    row_sem,
    line_sem,
):
    seat = Seat(lines)
    wires, staged = Wires(send_sem), Staged(stage_sem)
    staged.add(normed, normed_mid, rows.at[0, 0])
    seat.greet()
    spread_own(wires, seat, normed, rows, row_sem)
    ffn = ((wide, line_sem.at[0]), (downs, line_sem.at[1]))
    for hop in range(3, lines):
        line_hop(wires, seat, ffn, hop)
    staged.forward()
    spread_on(wires, seat, rows, row_sem)
    spread_landed(wires, seat, rows, row_sem)
    for hop in range(3, lines):
        line_landed(wires, seat, ffn, hop)
    staged.finish()
    wires.drain()


def middle(normed, wide, downs):
    lines = wide.shape[0]
    dma = pltpu.SemaphoreType.DMA
    return pl.pallas_call(
        functools.partial(middle_kernel, lines),
        out_shape=[
            jax.ShapeDtypeStruct((2, GROUP) + normed.shape, normed.dtype),
            jax.ShapeDtypeStruct(wide.shape, wide.dtype),
            jax.ShapeDtypeStruct(downs.shape, downs.dtype),
        ],
        in_specs=[ANY] * 3,
        out_specs=[ANY] * 3,
        scratch_shapes=[
            pltpu.VMEM(normed.shape, normed.dtype),
            dma((2,)),
            dma((7 + 4,)),
            dma((2, GROUP)),
            dma((2, lines)),
        ],
        input_output_aliases={1: 1, 2: 2},
        compiler_params=pltpu.CompilerParams(collective_id=1, has_side_effects=True),
        name="middle",
    )(normed, wide, downs)


def grouped_shards(
    block_input,
    attn_gain,
    query_weight,
    key_weight,
    value_weight,
    output_weight,
    ffn_gain,
    gate_weight,
    up_weight,
    down_weight,
    output_cotangent,
):
    f32, bf16 = jnp.float32, jnp.bfloat16
    members = lax.axis_size("dp")
    lines = members // GROUP
    index = lax.axis_index("dp")
    own, place = index // GROUP, lax.rem(index, GROUP)
    core = lax.axis_index("mp")
    rows, units = gate_weight.shape
    width = rows * members
    query_cols, key_cols = query_weight.shape[1], key_weight.shape[1]
    unit_rows = down_weight.shape[0]
    share = unit_rows * lines
    padded = whole_up(share, LANES)

    narrow = jnp.concatenate([query_weight, key_weight, value_weight], axis=1)
    cols = narrow.shape[1]
    gains = jnp.stack([attn_gain, ffn_gain])
    gains = jnp.pad(gains, ((0, 6), (0, whole_up(rows, LANES) - rows)))

    def shares(weight):
        parts = weight.reshape(rows, lines, GROUP, unit_rows).transpose(2, 0, 1, 3)
        return jnp.pad(parts.reshape(GROUP, rows, share), ((0, 0), (0, 0), (0, padded - share)))

    pieces = jnp.concatenate([shares(gate_weight), shares(up_weight)], axis=2)
    gains_all, narrow_all, out_all, wide, downs, seq_input, cot_rows = front(
        gains, narrow, output_weight, pieces, down_weight, block_input, output_cotangent
    )
    narrow_full = narrow_all.reshape(width, cols)
    gain_one = gains_all[:, 0, :rows].reshape(width)
    gain_two = gains_all[:, 1, :rows].reshape(width)
    out_full = out_all.reshape(-1, width)
    seq_input = seq_input.reshape(-1, width)
    cot_rows = cot_rows.reshape(-1, width)

    length = seq_input.shape[0]
    local_heads = query_cols // HD
    local_groups = key_cols // HD
    per_group = local_heads // local_groups
    cosine, sine = rope_tables(length, HD)
    input_f32 = seq_input.astype(f32)
    normed_one = (input_f32 * norm_scale(input_f32) * gain_one.astype(f32)[None, :]).astype(bf16)
    raw = jnp.dot(normed_one, narrow_full, preferred_element_type=f32)
    query_raw = raw[:, :query_cols]
    key_raw = raw[:, query_cols : query_cols + key_cols]
    value_raw = raw[:, query_cols + key_cols :]
    query_rot = rotate(query_raw.reshape(length, local_heads, HD), cosine, sine).astype(bf16)
    key_rot = rotate(key_raw.reshape(length, local_groups, HD), cosine, sine).astype(bf16)
    value_b = value_raw.astype(bf16)
    query_groups = query_rot.reshape(length, local_groups, per_group, HD).transpose(1, 0, 2, 3)
    key_groups = key_rot.transpose(1, 0, 2)
    value_groups = value_b.reshape(length, local_groups, HD).transpose(1, 0, 2)
    attended, log_norm = lax.map(head_forward, (query_groups, key_groups, value_groups))
    attn_rows = attended.transpose(1, 0, 2, 3).reshape(length, local_heads * HD)
    attn_part = jnp.dot(attn_rows, out_full, preferred_element_type=f32)
    own_f32 = block_input.astype(f32)
    residual = own_f32 + twin_sum(attn_part, core)
    inv_two = norm_scale(residual)
    normed_two = (residual * inv_two * gain_two.astype(f32)[None, :]).astype(bf16)

    ffn_rows, wide, downs = middle(normed_two, wide, downs)
    ffn_rows = ffn_rows.reshape(-1, width)
    wide_full = wide.reshape(width, 2 * padded)
    down_share = jnp.pad(downs.reshape(share, width), ((0, padded - share), (0, 0)))
    both_raw = jnp.dot(ffn_rows, wide_full, preferred_element_type=f32)
    gate_raw, up_raw = both_raw[:, :padded], both_raw[:, padded:]
    sigma = jax.nn.sigmoid(gate_raw)
    hidden = (gate_raw * sigma * up_raw).astype(bf16)
    hidden_cot = jnp.einsum("td,fd->tf", cot_rows, down_share, preferred_element_type=f32)
    gate_cot = (hidden_cot * up_raw * sigma * (1.0 + gate_raw * (1.0 - sigma))).astype(bf16)
    up_cot = (hidden_cot * gate_raw * sigma).astype(bf16)
    both_cot = jnp.concatenate([gate_cot, up_cot], axis=1)
    half = ffn_rows.shape[0] // 2

    def back(part):
        return jnp.einsum("tf,df->td", part, wide_full, preferred_element_type=f32)

    def forth(part):
        return jnp.dot(part, down_share, preferred_element_type=f32)

    back_far = twin(back(both_cot[half:]))
    back_sum = (back(both_cot[:half]) + back_far).reshape(GROUP, -1, width)
    back_scales = scales_of(back_sum)
    back_out = [narrowed(back_sum[key], back_scales) for key in range(1, GROUP)]
    back_in = exchanged(back_out, partner)

    ffn_rows, both_cot = after((ffn_rows, both_cot), *back_out)
    wide_grad = jnp.einsum("td,tf->df", ffn_rows, both_cot, preferred_element_type=f32)
    wide_grad = wide_grad.reshape(lines, GROUP * rows, 2 * padded)
    wide_out = messages_of(wide_grad, scales_of(wide_grad), own)
    wide_in = exchanged(wide_out, across)
    hidden, cot_rows = after((hidden, cot_rows), *wide_out)
    down_grad = jnp.einsum("tf,td->fd", hidden, cot_rows, preferred_element_type=f32)
    down_grad = down_grad[:share].reshape(lines, unit_rows, width)
    down_out = messages_of(down_grad, scales_of(down_grad), own)
    down_in = exchanged(down_out, across)

    hidden = after(hidden, *down_out)
    forth_far = twin(forth(hidden[half:]))
    forth_sum = (forth(hidden[:half]) + forth_far).reshape(GROUP, -1, width)

    back_in = after(back_in, forth_sum)
    normed_two_cot = added(back_sum[0], back_in)
    ffn_gain_part, residual_part = norm_backward(residual, inv_two, gain_two, normed_two_cot)
    residual_cot = output_cotangent.astype(f32) + residual_part
    residual_cot_b = ordered(residual_cot.astype(bf16), core)
    forth_sum = after(forth_sum, residual_cot)
    forth_scales = scales_of(forth_sum)
    forth_out = [narrowed(forth_sum[key], forth_scales) for key in range(1, GROUP)]
    forth_in = exchanged(forth_out, partner)
    out_grad = jnp.einsum("th,td->hd", attn_rows, residual_cot_b, preferred_element_type=f32)
    out_grad = out_grad.reshape(lines, GROUP, -1, width)
    attended_cot = jnp.einsum(
        "td,hd->th", residual_cot_b, out_full, preferred_element_type=f32
    ).astype(bf16)
    cot_groups = attended_cot.reshape(length, local_groups, per_group, HD).transpose(1, 0, 2, 3)
    query_parts, key_parts, value_parts = lax.map(
        head_backward, (query_groups, key_groups, value_groups, attended, log_norm, cot_groups)
    )
    query_cot = unrotate(
        query_parts.transpose(1, 0, 2, 3).reshape(length, local_heads, HD), cosine, sine
    ).reshape(length, local_heads * HD)
    key_cot = unrotate(key_parts.transpose(1, 0, 2), cosine, sine).reshape(length, key_cols)
    value_cot = value_parts.transpose(1, 0, 2).reshape(length, key_cols)
    narrow_cot = jnp.concatenate(
        [query_cot.astype(bf16), key_cot.astype(bf16), value_cot.astype(bf16)], axis=1
    )
    normed_one_part = jnp.einsum("th,dh->td", narrow_cot, narrow_full, preferred_element_type=f32)
    normed_one_cot = twin_sum(normed_one_part, core)
    out_grad = after(out_grad, normed_one_part)
    out_out = group_messages(out_grad, place)
    out_in = exchanged(out_out, partner)
    attn_gain_part, input_part = norm_backward(
        own_f32, norm_scale(own_f32), gain_one, normed_one_cot
    )
    input_grad = residual_cot + input_part
    narrow_grad = jnp.einsum("td,th->dh", normed_one, narrow_cot, preferred_element_type=f32)
    gain_parts = jnp.stack([attn_gain_part, ffn_gain_part])
    gain_parts = gain_parts + twin(gain_parts)
    gain_parts = gain_parts.reshape(2, members, rows).transpose(1, 0, 2)
    gain_parts = jnp.pad(gain_parts, ((0, 0), (0, 6), (0, cols - rows)))
    narrow_grad = jnp.concatenate([narrow_grad.reshape(members, rows, cols), gain_parts], axis=1)
    narrow_grad = narrow_grad.reshape(lines, GROUP, -1, cols)
    narrow_out = group_messages(narrow_grad, place)
    narrow_in = exchanged(narrow_out, partner)

    forth_in = after(forth_in, *narrow_out)
    block_output = (residual + added(forth_sum[0], forth_in)).astype(bf16)
    out_in = after(out_in, *narrow_out)
    out_sum = added(lax.dynamic_index_in_dim(out_grad, place, 1, keepdims=False), out_in)
    out_line = messages_of(out_sum, scales_of(out_sum), own)
    out_line_in = exchanged(out_line, across)
    wide_in = after(wide_in, *out_line)
    wide_own = added(lax.dynamic_index_in_dim(wide_grad, own, 0, keepdims=False), wide_in)
    wide_own = wide_own.reshape(GROUP, rows, 2 * padded)
    share_out = messages_of(wide_own, scales_of(wide_own), place)
    share_in = exchanged(share_out, partner)
    narrow_in = after(narrow_in, *share_out)
    narrow_sum = added(lax.dynamic_index_in_dim(narrow_grad, place, 1, keepdims=False), narrow_in)
    narrow_line = messages_of(narrow_sum, scales_of(narrow_sum), own)
    narrow_line_in = exchanged(narrow_line, across)
    share_in = after(share_in, *narrow_line)
    shares_in = [lax.dynamic_index_in_dim(wide_own, place, 0, keepdims=False)]
    shares_in = by_place(shares_in + [widened(message) for message in share_in], place)

    def unshared(start):
        parts = [part[:, start : start + share].reshape(rows, lines, unit_rows) for part in shares_in]
        return jnp.stack(parts, axis=2).reshape(rows, units)

    gate_own, up_own = unshared(0), unshared(padded)
    down_in = after(down_in, gate_own, up_own)
    down_own = added(lax.dynamic_index_in_dim(down_grad, own, 0, keepdims=False), down_in)
    out_line_in = after(out_line_in, down_own)
    out_own = added(lax.dynamic_index_in_dim(out_sum, own, 0, keepdims=False), out_line_in)
    narrow_line_in = after(narrow_line_in, out_own)
    narrow_own = added(lax.dynamic_index_in_dim(narrow_sum, own, 0, keepdims=False), narrow_line_in)
    return (
        block_output,
        input_grad,
        narrow_own[rows, :rows],
        narrow_own[:rows, :query_cols],
        narrow_own[:rows, query_cols : query_cols + key_cols],
        narrow_own[:rows, query_cols + key_cols :],
        out_own,
        narrow_own[rows + 1, :rows],
        gate_own,
        up_own,
        down_own,
    )


def solution(mesh):
    placed = (
        P(("dp", "mp"), None),
        P("dp"),
        P("dp", "mp"),
        P("dp", "mp"),
        P("dp", "mp"),
        P(("mp", "dp"), None),
        P("dp"),
        P("dp", "mp"),
        P("dp", "mp"),
        P(("mp", "dp"), None),
        P(("dp", "mp"), None),
    )
    members = mesh.shape["dp"]
    fits = mesh.shape["mp"] == 2 and members in (2 * GROUP, 4 * GROUP)
    return jax.shard_map(
        grouped_shards if fits else plain_shards,
        mesh=mesh,
        in_specs=placed,
        out_specs=(
            P(("dp", "mp"), None),
            P(("dp", "mp"), None),
            P("dp"),
            P("dp", "mp"),
            P("dp", "mp"),
            P("dp", "mp"),
            P(("mp", "dp"), None),
            P("dp"),
            P("dp", "mp"),
            P("dp", "mp"),
            P(("mp", "dp"), None),
        ),
        check_vma=False,
    )
```

```python
import functools

import jax
import jax.numpy as jnp
from jax import lax
from jax.experimental import pallas as pl
from jax.experimental.pallas import tpu as pltpu
from jax.sharding import PartitionSpec as P


HD = 64


EPSILON = 1e-05
ROPE_BASE = 10000.0


def rope_tables(length, head_dim):
    half_dim = head_dim // 2
    position = jnp.arange(length, dtype=jnp.float32)
    inverse = ROPE_BASE ** (-(jnp.arange(half_dim, dtype=jnp.float32) * (2.0 / head_dim)))
    angle = position[:, None] * inverse[None, :]
    return (jnp.cos(angle), jnp.sin(angle))


def rotate(values, cosine, sine):
    half_dim = values.shape[-1] // 2
    first_half = values[..., :half_dim]
    second_half = values[..., half_dim:]
    cos_part = cosine[:, None, :]
    sin_part = sine[:, None, :]
    return jnp.concatenate(
        [
            first_half * cos_part - second_half * sin_part,
            second_half * cos_part + first_half * sin_part,
        ],
        axis=-1,
    )


def unrotate(values, cosine, sine):
    half_dim = values.shape[-1] // 2
    first_half = values[..., :half_dim]
    second_half = values[..., half_dim:]
    cos_part = cosine[:, None, :]
    sin_part = sine[:, None, :]
    return jnp.concatenate(
        [
            first_half * cos_part + second_half * sin_part,
            second_half * cos_part - first_half * sin_part,
        ],
        axis=-1,
    )


def norm_scale(values):
    return lax.rsqrt(jnp.mean(values * values, axis=-1, keepdims=True) + EPSILON)


def norm_backward(values, inverse, gain, normed_cot):
    scaled = normed_cot * gain.astype(jnp.float32)[None, :]
    gain_grad = jnp.sum(normed_cot * values * inverse, axis=0)
    values_grad = inverse * scaled - values * (inverse * inverse * inverse) * jnp.mean(
        scaled * values, axis=-1, keepdims=True
    )
    return (gain_grad, values_grad)


def causal_scores(query_group, key_group):
    scale = query_group.shape[-1] ** (-0.5)
    scores = (
        jnp.einsum("qgd,kd->gqk", query_group, key_group, preferred_element_type=jnp.float32)
        * scale
    )
    length = key_group.shape[0]
    visible = lax.broadcasted_iota(jnp.int32, (length, length), 0) >= lax.broadcasted_iota(
        jnp.int32, (length, length), 1
    )
    return jnp.where(visible[None], scores, -jnp.inf)


def head_forward(parts):
    query_group, key_group, value_group = parts
    scores = causal_scores(query_group, key_group)
    top_score = jnp.max(scores, axis=-1, keepdims=True)
    log_norm = top_score + jnp.log(jnp.sum(jnp.exp(scores - top_score), axis=-1, keepdims=True))
    probs_b = jnp.exp(scores - log_norm).astype(jnp.bfloat16)
    attended = jnp.einsum(
        "gqk,kd->qgd", probs_b, value_group, preferred_element_type=jnp.float32
    ).astype(jnp.bfloat16)
    return (attended, log_norm[..., 0])


def head_backward(parts):
    query_group, key_group, value_group, attended, log_norm, attended_cot = parts
    scale = query_group.shape[-1] ** (-0.5)
    scores = causal_scores(query_group, key_group)
    probs = jnp.exp(scores - log_norm[..., None])
    probs_b = probs.astype(jnp.bfloat16)
    value_cot = jnp.einsum("gqk,qgd->kd", probs_b, attended_cot, preferred_element_type=jnp.float32)
    probs_cot = jnp.einsum(
        "qgd,kd->gqk", attended_cot, value_group, preferred_element_type=jnp.float32
    )
    delta = jnp.sum(attended_cot.astype(jnp.float32) * attended.astype(jnp.float32), axis=-1).T
    score_cot = (probs * (probs_cot - delta[:, :, None])).astype(jnp.bfloat16)
    query_cot = (
        jnp.einsum("gqk,kd->qgd", score_cot, key_group, preferred_element_type=jnp.float32) * scale
    )
    key_cot = (
        jnp.einsum("gqk,qgd->kd", score_cot, query_group, preferred_element_type=jnp.float32)
        * scale
    )
    return (query_cot, key_cot, value_cot)


def plain_shards(
    block_input,
    attn_gain,
    query_weight,
    key_weight,
    value_weight,
    output_weight,
    ffn_gain,
    gate_weight,
    up_weight,
    down_weight,
    output_cotangent,
):
    local_rows = block_input.shape[0]
    own_start = lax.axis_index("mp") * local_rows
    query_full, key_full, value_full, out_full, gain_one = (
        lax.all_gather(query_weight, "dp", axis=0, tiled=True),
        lax.all_gather(key_weight, "dp", axis=0, tiled=True),
        lax.all_gather(value_weight, "dp", axis=0, tiled=True),
        lax.all_gather(output_weight, "dp", axis=0, tiled=True),
        lax.all_gather(attn_gain, "dp", axis=0, tiled=True),
    )
    seq_input = lax.all_gather(block_input, "mp", axis=0, tiled=True)
    length = seq_input.shape[0]
    local_heads = query_full.shape[1] // HD
    local_groups = key_full.shape[1] // HD
    per_group = local_heads // local_groups
    cosine, sine = rope_tables(length, HD)
    input_f32 = seq_input.astype(jnp.float32)
    inv_one = norm_scale(input_f32)
    normed_one = (input_f32 * inv_one * gain_one.astype(jnp.float32)[None, :]).astype(jnp.bfloat16)
    query_raw = jnp.dot(normed_one, query_full, preferred_element_type=jnp.float32)
    key_raw = jnp.dot(normed_one, key_full, preferred_element_type=jnp.float32)
    value_raw = jnp.dot(normed_one, value_full, preferred_element_type=jnp.float32)
    query_rot = rotate(query_raw.reshape(length, local_heads, HD), cosine, sine).astype(
        jnp.bfloat16
    )
    key_rot = rotate(key_raw.reshape(length, local_groups, HD), cosine, sine).astype(jnp.bfloat16)
    value_b = value_raw.astype(jnp.bfloat16)
    query_groups = query_rot.reshape(length, local_groups, per_group, HD).transpose(1, 0, 2, 3)
    key_groups = key_rot.transpose(1, 0, 2)
    value_groups = value_b.reshape(length, local_groups, HD).transpose(1, 0, 2)
    attended, log_norm = lax.map(head_forward, (query_groups, key_groups, value_groups))
    attn_rows = attended.transpose(1, 0, 2, 3).reshape(length, local_heads * HD)
    attn_part = jnp.dot(attn_rows, out_full, preferred_element_type=jnp.float32)
    residual = input_f32 + lax.psum(attn_part, "mp")
    gate_full, up_full, down_full, gain_two = (
        lax.all_gather(gate_weight, "dp", axis=0, tiled=True),
        lax.all_gather(up_weight, "dp", axis=0, tiled=True),
        lax.all_gather(down_weight, "dp", axis=0, tiled=True),
        lax.all_gather(ffn_gain, "dp", axis=0, tiled=True),
    )
    inv_two = norm_scale(residual)
    normed_two = (residual * inv_two * gain_two.astype(jnp.float32)[None, :]).astype(jnp.bfloat16)
    gate_raw = jnp.dot(normed_two, gate_full, preferred_element_type=jnp.float32)
    up_raw = jnp.dot(normed_two, up_full, preferred_element_type=jnp.float32)
    sigma = jax.nn.sigmoid(gate_raw)
    hidden = (gate_raw * sigma * up_raw).astype(jnp.bfloat16)
    ffn_own = lax.psum_scatter(
        jnp.dot(hidden, down_full, preferred_element_type=jnp.float32),
        "mp",
        scatter_dimension=0,
        tiled=True,
    )
    residual_own = lax.dynamic_slice_in_dim(residual, own_start, local_rows, 0)
    block_output = (residual_own + ffn_own).astype(jnp.bfloat16)
    cot_seq = lax.all_gather(output_cotangent, "mp", axis=0, tiled=True)
    hidden_cot = jnp.einsum("td,fd->tf", cot_seq, down_full, preferred_element_type=jnp.float32)
    gate_cot = (hidden_cot * up_raw * sigma * (1.0 + gate_raw * (1.0 - sigma))).astype(jnp.bfloat16)
    up_cot = (hidden_cot * gate_raw * sigma).astype(jnp.bfloat16)
    normed_two_part = jnp.einsum(
        "tf,df->td", gate_cot, gate_full, preferred_element_type=jnp.float32
    )
    normed_two_part = normed_two_part + jnp.einsum(
        "tf,df->td", up_cot, up_full, preferred_element_type=jnp.float32
    )
    normed_two_cot = lax.psum(normed_two_part, "mp")
    ffn_gain_grad, residual_part = norm_backward(residual, inv_two, gain_two, normed_two_cot)
    residual_cot = cot_seq.astype(jnp.float32) + residual_part
    down_grad = jnp.einsum("tf,td->fd", hidden, cot_seq, preferred_element_type=jnp.float32)
    gate_grad = jnp.einsum("td,tf->df", normed_two, gate_cot, preferred_element_type=jnp.float32)
    up_grad = jnp.einsum("td,tf->df", normed_two, up_cot, preferred_element_type=jnp.float32)
    gate_share, up_share, down_share, ffn_gain_share = (
        lax.psum_scatter(gate_grad, "dp", scatter_dimension=0, tiled=True),
        lax.psum_scatter(up_grad, "dp", scatter_dimension=0, tiled=True),
        lax.psum_scatter(down_grad, "dp", scatter_dimension=0, tiled=True),
        lax.psum_scatter(ffn_gain_grad, "dp", scatter_dimension=0, tiled=True),
    )
    residual_cot_b = residual_cot.astype(jnp.bfloat16)
    output_weight_grad = jnp.einsum(
        "th,td->hd", attn_rows, residual_cot_b, preferred_element_type=jnp.float32
    )
    attended_cot = jnp.einsum(
        "td,hd->th", residual_cot_b, out_full, preferred_element_type=jnp.float32
    ).astype(jnp.bfloat16)
    cot_groups = attended_cot.reshape(length, local_groups, per_group, HD).transpose(1, 0, 2, 3)
    query_parts, key_parts, value_parts = lax.map(
        head_backward, (query_groups, key_groups, value_groups, attended, log_norm, cot_groups)
    )
    query_cot = (
        unrotate(query_parts.transpose(1, 0, 2, 3).reshape(length, local_heads, HD), cosine, sine)
        .reshape(length, local_heads * HD)
        .astype(jnp.bfloat16)
    )
    key_cot = (
        unrotate(key_parts.transpose(1, 0, 2), cosine, sine)
        .reshape(length, local_groups * HD)
        .astype(jnp.bfloat16)
    )
    value_cot = (
        value_parts.transpose(1, 0, 2).reshape(length, local_groups * HD).astype(jnp.bfloat16)
    )
    normed_one_part = jnp.einsum(
        "th,dh->td", query_cot, query_full, preferred_element_type=jnp.float32
    )
    normed_one_part = normed_one_part + jnp.einsum(
        "th,dh->td", key_cot, key_full, preferred_element_type=jnp.float32
    )
    normed_one_part = normed_one_part + jnp.einsum(
        "th,dh->td", value_cot, value_full, preferred_element_type=jnp.float32
    )
    normed_one_cot = lax.psum(normed_one_part, "mp")
    query_grad = jnp.einsum("td,th->dh", normed_one, query_cot, preferred_element_type=jnp.float32)
    key_grad = jnp.einsum("td,th->dh", normed_one, key_cot, preferred_element_type=jnp.float32)
    value_grad = jnp.einsum("td,th->dh", normed_one, value_cot, preferred_element_type=jnp.float32)
    attn_gain_grad, input_part = norm_backward(input_f32, inv_one, gain_one, normed_one_cot)
    input_cot = residual_cot + input_part
    input_grad = lax.dynamic_slice_in_dim(input_cot, own_start, local_rows, 0)
    attn_gain_share, query_share, key_share, value_share, output_share = (
        lax.psum_scatter(attn_gain_grad, "dp", scatter_dimension=0, tiled=True),
        lax.psum_scatter(query_grad, "dp", scatter_dimension=0, tiled=True),
        lax.psum_scatter(key_grad, "dp", scatter_dimension=0, tiled=True),
        lax.psum_scatter(value_grad, "dp", scatter_dimension=0, tiled=True),
        lax.psum_scatter(output_weight_grad, "dp", scatter_dimension=0, tiled=True),
    )
    return (
        block_output,
        input_grad,
        attn_gain_share,
        query_share,
        key_share,
        value_share,
        output_share,
        ffn_gain_share,
        gate_share,
        up_share,
        down_share,
    )


GROUP = 4
LANES = 128


def whole_up(size, step):
    return -(-size // step) * step


def partner(values, key):
    pairs = [(at, at ^ key) for at in range(lax.axis_size("dp"))]
    return lax.ppermute(values, "dp", pairs)


def across(values, key):
    pairs = [(at, at ^ (key * GROUP)) for at in range(lax.axis_size("dp"))]
    return lax.ppermute(values, "dp", pairs)


def after(value, *marks):
    return lax.optimization_barrier((value,) + marks)[0]


def narrowed(values, scale):
    return (values * scale).astype(jnp.float16)


def added(total, messages, undo):
    come = sum(message.astype(jnp.float32) for message in messages)
    return total + (come * undo).reshape(total.shape)


def messages_of(blocks, scale, at):
    return [
        narrowed(lax.dynamic_index_in_dim(blocks, at ^ key, 0, keepdims=False), scale)
        for key in range(1, blocks.shape[0])
    ]


def noted(values, scale, notes):
    return jnp.concatenate([values * scale, notes], axis=0).astype(jnp.float16)


def undo_of(message):
    return jnp.prod(message[-8:].astype(jnp.float32), axis=0, keepdims=True)


def group_messages(blocks, place, scale, notes):
    cols = blocks.shape[3]
    return [
        noted(
            lax.dynamic_index_in_dim(blocks, place ^ key, 1, keepdims=False).reshape(-1, cols),
            scale,
            notes,
        )
        for key in range(1, GROUP)
    ]


def line_messages(blocks, undo, at):
    power = jnp.log2(undo)
    row = lax.broadcasted_iota(jnp.float32, (8, undo.shape[1]), 0)
    notes = jnp.exp2(jnp.floor((jnp.round(power) + row) * 0.125))
    scale, notes = lax.optimization_barrier((1.0 / undo, notes))
    return [
        noted(lax.dynamic_index_in_dim(blocks, at ^ key, 0, keepdims=False), scale, notes)
        for key in range(1, blocks.shape[0])
    ]


def added_noted(total, messages, undos):
    for message, undo in zip(messages, undos):
        total = total + (message[:-8].astype(jnp.float32) * undo).reshape(total.shape)
    return total


def raised(undo, undos):
    for other in undos:
        undo = jnp.maximum(undo, other)
    return 4.0 * undo


def exchanged(messages, exchange):
    return [exchange(message, key + 1) for key, message in enumerate(messages)]


MESH = pl.DeviceIdType.MESH


def flipped(place, key):
    if key == 1:
        return place + 1 - 2 * lax.rem(place, 2)
    if key == 2:
        return place + 2 - 4 * lax.div(place, 2)
    return GROUP - 1 - place


class Wires:
    def __init__(self, send_sem):
        self.send_sem, self.used, self.open = send_sem, 0, []

    def send(self, source, target, arrival, device, when=None):
        copy = pltpu.make_async_remote_copy(
            src_ref=source,
            dst_ref=target,
            send_sem=self.send_sem.at[self.used],
            recv_sem=arrival,
            device_id=device,
            device_id_type=MESH,
        )
        self.used += 1
        self.open.append((copy, when))
        if when is None:
            copy.start()
        else:
            pl.when(when)(copy.start)

    def arrived(self, target, arrival, device, when=None):
        copy = pltpu.make_async_remote_copy(
            src_ref=target,
            dst_ref=target,
            send_sem=self.send_sem.at[0],
            recv_sem=arrival,
            device_id=device,
            device_id_type=MESH,
        )
        if when is None:
            copy.wait_recv()
        else:
            pl.when(when)(copy.wait_recv)

    def drain(self):
        for copy, when in self.open:
            if when is None:
                copy.wait_send()
            else:
                pl.when(when)(copy.wait_send)


class Seat:
    def __init__(self, lines):
        self.index = lax.axis_index("dp")
        self.core = lax.axis_index("mp")
        self.own, self.place = lax.div(self.index, GROUP), lax.rem(self.index, GROUP)
        self.lines = lines

    def mate(self, key):
        return (self.own * GROUP + flipped(self.place, key), self.core)

    def line(self, step):
        return ((self.own + step) * GROUP + self.place, self.core)

    def peer(self, key):
        return (flipped(self.own, key) * GROUP + self.place, self.core)

    def twin(self):
        return (self.index, 1 - self.core)

    def greet(self):
        barrier = pltpu.get_barrier_semaphore()
        for key in range(1, GROUP):
            pl.semaphore_signal(barrier, 1, device_id=self.mate(key), device_id_type=MESH)
        pl.semaphore_signal(barrier, 1, device_id=self.twin(), device_id_type=MESH)
        above, below = self.own < self.lines - 1, self.own > 0

        @pl.when(above)
        def _():
            pl.semaphore_signal(barrier, 1, device_id=self.line(1), device_id_type=MESH)

        @pl.when(below)
        def _():
            pl.semaphore_signal(barrier, 1, device_id=self.line(-1), device_id_type=MESH)

        ends = lax.div(self.own, self.lines - 1) + 1 - lax.div(self.own + self.lines - 1, self.lines)
        pl.semaphore_wait(barrier, GROUP + 2 - ends)


class Staged:
    def __init__(self, sems):
        self.sems, self.used, self.loads, self.stores = sems, 0, [], []

    def add(self, source, middle, target):
        load = pltpu.make_async_copy(source, middle, self.sems.at[self.used])
        store = pltpu.make_async_copy(middle, target, self.sems.at[self.used + 1])
        self.used += 2
        load.start()
        self.loads.append((load, store))

    def forward(self):
        for load, store in self.loads:
            load.wait()
            store.start()
            self.stores.append(store)
        self.loads = []

    def finish(self):
        for store in self.stores:
            store.wait()


def line_hop(wires, seat, arrays, hop):
    lines = seat.lines
    for blocks, arrivals in arrays:
        for step in (1, -1):
            from_block = seat.own - step * (hop - 1)
            into = seat.own + step
            ok = (from_block >= 0) & (from_block < lines) & (into >= 0) & (into < lines)
            block = blocks.at[lax.rem(from_block + lines, lines)]
            wires.send(
                block, block, arrivals.at[lax.rem(from_block + lines, lines)], seat.line(step), ok
            )


def line_landed(wires, seat, arrays, hop):
    lines = seat.lines
    for blocks, arrivals in arrays:
        for step in (1, -1):
            block = seat.own - step * hop
            ok = (block >= 0) & (block < lines)
            block = lax.rem(block + lines, lines)
            wires.arrived(blocks.at[block], arrivals.at[block], seat.twin(), ok)


def spread_own(wires, seat, own, rows, arrivals):
    for key in range(1, GROUP):
        wires.send(own, rows.at[0, key], arrivals.at[0, key], seat.mate(key))
    wires.send(own, rows.at[1, 0], arrivals.at[1, 0], seat.twin())


def spread_on(wires, seat, rows, arrivals):
    for key in range(1, GROUP):
        wires.arrived(rows.at[0, key], arrivals.at[0, key], seat.twin())
        wires.send(rows.at[0, key], rows.at[1, key], arrivals.at[1, key], seat.twin())


def spread_landed(wires, seat, rows, arrivals):
    for key in range(GROUP):
        wires.arrived(rows.at[1, key], arrivals.at[1, key], seat.twin())


def whole_gain(gains, which, rows):
    members = gains.shape[0]
    width = members * rows
    lane = lax.broadcasted_iota(jnp.int32, (1, LANES), 1)
    chunks = []
    for start in range(0, width, LANES):
        block = start // rows
        shift = block * rows - start
        chunk = gains[block, which : which + 1, :].astype(jnp.float32)
        chunk = pltpu.roll(chunk, shift % LANES, 1) if shift else chunk
        edge = rows + shift
        while edge < LANES and block + 1 < members:
            block += 1
            more = gains[block, which : which + 1, :].astype(jnp.float32)
            more = pltpu.roll(more, edge, 1) if edge % LANES else more
            chunk = jnp.where(lane < edge, chunk, more)
            edge += rows
        chunks.append(chunk)
    return jnp.concatenate(chunks, axis=1)


def turned(values, cosine, sine):
    half = HD // 2
    lane = lax.broadcasted_iota(jnp.int32, values.shape, 1)
    ahead = pltpu.roll(values, LANES - half, 1)
    behind = pltpu.roll(values, half, 1)
    other = jnp.where(lax.rem(lane, HD) < half, ahead, behind)
    return values * cosine + other * sine


def masked_scores(query, key):
    scores = lax.dot_general(
        query, key, (((1,), (1,)), ((), ())), preferred_element_type=jnp.float32
    ) * (HD**-0.5)
    row = lax.broadcasted_iota(jnp.int32, scores.shape, 0)
    column = lax.broadcasted_iota(jnp.int32, scores.shape, 1)
    return jnp.where(row >= column, scores, -jnp.inf)


def probabilities(query, key):
    scores = masked_scores(query, key)
    top = jnp.max(scores, axis=1, keepdims=True)
    log_norm = top + jnp.log(jnp.sum(jnp.exp(scores - top), axis=1, keepdims=True))
    return jnp.exp(scores - log_norm)


def norm_rows(source, start, count):
    values = source[pl.ds(start, count), :].astype(jnp.float32)
    inverse = lax.rsqrt(jnp.mean(values * values, axis=1, keepdims=True) + EPSILON)
    return values, inverse


STEP = 32


def attend_forward(normed, narrow, raw, heads, attended, tables):
    pairs = attended.shape[1] // LANES
    raw[...] = jnp.dot(normed[...], narrow[...], preferred_element_type=jnp.float32)
    last = pairs * LANES
    heads[:, last:] = turned(raw[:, last:], tables[2], tables[3]).astype(jnp.bfloat16)

    def pair(at, carry):
        lanes = pl.ds(pl.multiple_of(at * LANES, LANES), LANES)
        query = turned(raw[:, lanes], tables[0], tables[1]).astype(jnp.bfloat16)
        heads[:, lanes] = query
        key, value = heads[:, last : last + HD], heads[:, last + HD : last + 2 * HD]
        parts = []
        for head in range(LANES // HD):
            probs = probabilities(query[:, head * HD : (head + 1) * HD], key)
            parts.append(
                jnp.dot(probs.astype(jnp.bfloat16), value, preferred_element_type=jnp.float32)
            )
        attended[:, lanes] = jnp.concatenate(parts, axis=1).astype(jnp.bfloat16)
        return carry

    lax.fori_loop(0, pairs, pair, 0)


def front_kernel(
    lines,
    gains,
    narrow,
    out,
    pieces,
    down,
    inputs,
    cots,
    tables,
    gains_rows,
    narrow_full,
    out_full,
    wide,
    downs,
    cot_rows,
    rows,
    normed_one,
    heads_out,
    attended_out,
    residual_out,
    gains_v,
    narrow_v,
    out_v,
    piece_v,
    down_v,
    seq_v,
    cot_v,
    gain_v,
    tables_v,
    normed_v,
    raw_v,
    heads_v,
    attended_v,
    away_v,
    come_v,
    residual_v,
    second_v,
    stage_sem,
    load_sem,
    store_sem,
    send_sem,
    block_sem,
    mix_sem,
    line_sem,
    cot_sem,
    row_sem,
    seq_sem,
):
    seat = Seat(lines)
    wires, staged = Wires(send_sem), Staged(stage_sem)
    index, own, place, core = seat.index, seat.own, seat.place, seat.core
    count, half = narrow.shape[0], inputs.shape[0]
    out_count = out.shape[0]

    def slot(target, block):
        if target is gains_v:
            return gains_v.at[block]
        size = count if target is narrow_v else out_count
        return target.at[pl.ds(pl.multiple_of(block * size, 16), size)]

    def half_of(target, which):
        return target.at[pl.ds(pl.multiple_of(which * half, half), half)]

    loads = [
        pltpu.make_async_copy(source, target, load_sem.at[at])
        for at, (source, target) in enumerate(
            (
                (gains, slot(gains_v, index)),
                (narrow, slot(narrow_v, index)),
                (out, slot(out_v, index)),
                (inputs, half_of(seq_v, core)),
                (tables, tables_v),
            )
        )
    ]
    for load in loads:
        load.start()
    staged.add(pieces.at[place], piece_v, wide.at[own, place])
    staged.add(down, down_v, downs.at[own])
    staged.add(cots, cot_v, cot_rows.at[0, 0])
    seat.greet()
    whole = ((gains, gains_v, 0, 1, 2), (narrow, narrow_v, 1, 1, 2), (out, out_v, 2, 2, 1))

    def block_of(at, key=0):
        return lax.rem(at + lines, lines) * GROUP + (flipped(place, key) if key else place)

    def pass_on(target, which, block, device, ok=None):
        wires.send(slot(target, block), slot(target, block), block_sem.at[which, block], device, ok)

    def landed(target, which, block, ok=None):
        wires.arrived(slot(target, block), block_sem.at[which, block], seat.twin(), ok)

    for source, target, which, first, second in whole:
        for step in (1, -1):
            ok = (own + step >= 0) & (own + step < lines)
            wires.send(
                source, slot(target, index), block_sem.at[which, index], seat.line(step), ok
            )
        for key in (first, second):
            wires.send(source, slot(target, index), block_sem.at[which, index], seat.mate(key))
    for key in range(1, GROUP):
        wires.send(
            pieces.at[flipped(place, key)], wide.at[own, place], mix_sem.at[key], seat.mate(key)
        )
    wires.send(inputs, half_of(seq_v, core), seq_sem.at[0], seat.twin())
    staged.forward()
    for hop in range(1, lines):
        for _, target, which, first, second in whole:
            for step in (1, -1):
                at = own - step * hop
                ok = (at >= 0) & (at < lines)
                block = block_of(at)
                landed(target, which, block, ok)
                onward = ok & (own + step >= 0) & (own + step < lines)
                pass_on(target, which, block, seat.line(step), onward)
                for key in (first, second):
                    pass_on(target, which, block, seat.mate(key), ok)
        if hop == 1:
            for _, target, which, first, second in whole:
                block = block_of(own, first)
                landed(target, which, block)
                pass_on(target, which, block, seat.mate(second))
    staged.finish()
    for key in range(1, GROUP):
        wires.arrived(wide.at[own, flipped(place, key)], mix_sem.at[key], seat.twin())
    ffn = ((wide, line_sem.at[0]), (downs, line_sem.at[1]))
    line_hop(wires, seat, ffn, 1)
    for hop in range(1, lines):
        for _, target, which, first, second in whole:
            for step in (1, -1):
                at = own - step * hop
                ok = (at >= 0) & (at < lines)
                block = block_of(at, first)
                landed(target, which, block, ok)
                pass_on(target, which, block, seat.mate(second), ok)
    spread_own(wires, seat, cots, cot_rows, cot_sem)
    for load in loads:
        load.wait()
    wires.arrived(half_of(seq_v, 1 - core), seq_sem.at[0], seat.twin())
    for _, target, which, first, second in whole:
        for at in range(lines):
            for key in (second, GROUP - 1):
                landed(target, which, block_of(at, key))
    stores = []

    def put(source, target):
        store = pltpu.make_async_copy(source, target, store_sem.at[len(stores)])
        store.start()
        stores.append(store)

    put(narrow_v, narrow_full)
    put(out_v, out_full)
    for which in range(2):
        gain = whole_gain(gains_v, which, count)
        gain_v[pl.ds(which * 8, 8), :] = jnp.broadcast_to(gain, (8, gain.shape[1]))
    put(gain_v, gains_rows)

    def norm_one(at, carry):
        start = pl.multiple_of(at * STEP, STEP)
        values, inverse = norm_rows(seq_v, start, STEP)
        normed_v[pl.ds(start, STEP), :] = (values * inverse * gain_v[0:1, :]).astype(jnp.bfloat16)
        return carry

    lax.fori_loop(0, 2 * half // STEP, norm_one, 0)
    put(normed_v, normed_one)
    line_landed(wires, seat, ffn, 1)
    line_hop(wires, seat, ffn, 2)
    attend_forward(normed_v, narrow_v, raw_v, heads_v, attended_v, tables_v)
    put(heads_v, heads_out)
    put(attended_v, attended_out)

    def part_of(which):
        rows_of = attended_v[pl.ds(pl.multiple_of(which * half, half), half), :]
        return jnp.dot(rows_of, out_v[...], preferred_element_type=jnp.float32)

    away_v[...] = part_of(1 - core)
    wires.send(away_v, come_v, seq_sem.at[1], seat.twin())
    residual_v[...] = part_of(core)
    wires.arrived(come_v, seq_sem.at[1], seat.twin())

    def norm_two(at, carry):
        start = pl.multiple_of(at * STEP, STEP)
        span = pl.ds(start, STEP)
        values = seq_v[pl.ds(pl.multiple_of(core * half + start, STEP), STEP), :]
        residual_v[span, :] = values.astype(jnp.float32) + (residual_v[span, :] + come_v[span, :])
        values, inverse = norm_rows(residual_v, start, STEP)
        second_v[span, :] = (values * inverse * gain_v[8:9, :]).astype(jnp.bfloat16)
        return carry

    lax.fori_loop(0, half // STEP, norm_two, 0)
    spread_own(wires, seat, second_v, rows, row_sem)
    put(residual_v, residual_out)
    put(second_v, rows.at[0, 0])
    spread_on(wires, seat, cot_rows, cot_sem)
    line_landed(wires, seat, ffn, 2)
    for hop in range(3, lines):
        line_hop(wires, seat, ffn, hop)
    spread_on(wires, seat, rows, row_sem)
    spread_landed(wires, seat, cot_rows, cot_sem)
    spread_landed(wires, seat, rows, row_sem)
    for hop in range(3, lines):
        line_landed(wires, seat, ffn, hop)
    for store in stores:
        store.wait()
    wires.drain()


ANY = pl.BlockSpec(memory_space=pl.ANY)


def front(gains, narrow, out, pieces, down, inputs, cots, tables):
    members = lax.axis_size("dp")
    lines = members // GROUP
    bf16, f32 = gains.dtype, jnp.float32
    sources = (gains, narrow, out, pieces, down, inputs, cots, tables)
    _, cols = narrow.shape
    half, width = inputs.shape
    depth = members * out.shape[0]
    shape = jax.ShapeDtypeStruct
    results = [
        shape((16, width), f32),
        shape((width, cols), bf16),
        shape((depth, width), bf16),
        shape((lines,) + pieces.shape, bf16),
        shape((lines,) + down.shape, bf16),
        shape((2, GROUP, half, width), bf16),
        shape((2, GROUP, half, width), bf16),
        shape((2 * half, width), bf16),
        shape((2 * half, cols), bf16),
        shape((2 * half, depth), bf16),
        shape((half, width), f32),
    ]
    whole = 3
    sends = whole * (4 + (lines - 1) * 2 * 3 + 1 + (lines - 1) * 2) + 3 + 2 + 4 * (lines - 1) + 2 * 7
    dma = pltpu.SemaphoreType.DMA
    vmem = pltpu.VMEM
    return pl.pallas_call(
        functools.partial(front_kernel, lines),
        out_shape=results,
        in_specs=[ANY] * len(sources),
        out_specs=[ANY] * len(results),
        scratch_shapes=[
            vmem((members,) + gains.shape, bf16),
            vmem((width, cols), bf16),
            vmem((depth, width), bf16),
            vmem(pieces.shape[1:], bf16),
            vmem(down.shape, bf16),
            vmem((2 * half, width), bf16),
            vmem(cots.shape, bf16),
            vmem((16, width), f32),
            vmem(tables.shape, f32),
            vmem((2 * half, width), bf16),
            vmem((2 * half, cols), f32),
            vmem((2 * half, cols), bf16),
            vmem((2 * half, depth), bf16),
            vmem((half, width), f32),
            vmem((half, width), f32),
            vmem((half, width), f32),
            vmem((half, width), bf16),
            dma((6,)),
            dma((5,)),
            dma((8,)),
            dma((sends,)),
            dma((whole, members)),
            dma((GROUP,)),
            dma((2, lines)),
            dma((2, GROUP)),
            dma((2, GROUP)),
            dma((2,)),
        ],
        compiler_params=pltpu.CompilerParams(
            collective_id=0, has_side_effects=True, vmem_limit_bytes=40 << 20
        ),
        name="front",
    )(*sources)


SPAN = 14.0


def put_scales(tops, rows):
    power = jnp.clip(jnp.ceil(jnp.log2(jnp.maximum(tops, 1e-33))), -98.0, 126.0) - SPAN
    shape = rows.shape[1:]
    row = lax.broadcasted_iota(jnp.int32, shape, 0).astype(jnp.float32)
    rows[0] = jnp.broadcast_to(jnp.exp2(-power), shape)
    rows[1] = jnp.broadcast_to(jnp.exp2(power), shape)
    rows[2] = jnp.exp2(jnp.floor((power + row) * 0.125))


def tops_of(values):
    return jnp.max(jnp.abs(values), axis=0, keepdims=True)


def meet(seat):
    barrier = pltpu.get_barrier_semaphore()
    others = [seat.mate(key) for key in range(1, GROUP)]
    others += [seat.peer(key) for key in range(1, seat.lines)] + [seat.twin()]
    for other in others:
        pl.semaphore_signal(barrier, 1, device_id=other, device_id_type=MESH)
    pl.semaphore_wait(barrier, len(others))


def meet_twin(seat):
    barrier = pltpu.get_barrier_semaphore()
    pl.semaphore_signal(barrier, 1, device_id=seat.twin(), device_id_type=MESH)
    pl.semaphore_wait(barrier, 1)


def send_bounds(wires, mine, come, sems, devices, first):
    for at, device in enumerate(devices):
        wires.send(mine, come.at[first + at], sems.at[first + at], device)


def take_bounds(wires, seat, mine, come, sems, devices, first):
    bounds = mine[...]
    for at in range(len(devices)):
        wires.arrived(come.at[first + at], sems.at[first + at], seat.twin())
        bounds = jnp.maximum(bounds, come[first + at])
    return bounds


class Moves:
    def __init__(self, sems):
        self.sems, self.used, self.open = sems, 0, []

    def start(self, source, target):
        copy = pltpu.make_async_copy(source, target, self.sems.at[self.used])
        copy.start()
        self.used += 1
        return copy

    def put(self, source, target):
        self.open.append(self.start(source, target))

    def finish(self):
        for copy in self.open:
            copy.wait()


def dot_rows(left, right):
    return jnp.dot(left, right, preferred_element_type=jnp.float32)


def dot_across(left, right):
    return lax.dot_general(left, right, (((1,), (1,)), ((), ())), preferred_element_type=jnp.float32)


def dot_down(left, right):
    return lax.dot_general(left, right, (((0,), (0,)), ((), ())), preferred_element_type=jnp.float32)


CHUNK = 256


def sum_up(near, come):
    def step(at, carry):
        span = pl.ds(pl.multiple_of(at * STEP, STEP), STEP)
        near[span, :] = near[span, :] + come[span, :]
        return carry

    lax.fori_loop(0, near.shape[0] // STEP, step, 0)


def units_kernel(
    lines,
    share,
    rows,
    cots,
    wide,
    down,
    gains,
    hidden_out,
    back_out,
    wide_out,
    factors,
    wide_factors,
    rows_v,
    cots_v,
    wide_v,
    down_v,
    gains_v,
    hidden_v,
    both_v,
    far_v,
    near_v,
    come_v,
    wide_grad_v,
    mine_v,
    bounds_v,
    factors_v,
    wide_factors_v,
    move_sem,
    send_sem,
    come_sem,
    bound_sem,
):
    seat = Seat(lines)
    moves = Moves(move_sem)
    count, width = rows.shape
    half = count // 2
    padded = hidden_v.shape[1]
    chunks = half // CHUNK
    loads = []
    for source, target in ((wide, wide_v), (down, down_v.at[pl.ds(0, share)]), (gains, gains_v)):
        loads.append(moves.start(source, target))
    for at in range(2 * chunks):
        span = pl.ds((at * CHUNK + half) % count, CHUNK)
        loads.append(moves.start(rows.at[span], rows_v.at[span]))
        loads.append(moves.start(cots.at[span], cots_v.at[span]))
    down_v[share:, :] = jnp.zeros((padded - share, width), down_v.dtype)
    meet(seat)
    for load in loads[:3]:
        load.wait()
    wires = Wires(send_sem)
    back_top = jnp.zeros((1, width), jnp.float32)
    cot_top = jnp.zeros((1, width), jnp.bfloat16)
    hidden_sum = jnp.zeros((1, padded), jnp.float32)
    hidden_top = jnp.zeros((1, 1), jnp.float32)
    both_sum = jnp.zeros((1, 2 * padded), jnp.float32)
    for at in range(2 * chunks):
        loads[3 + 2 * at].wait()
        loads[4 + 2 * at].wait()
        start = (at * CHUNK + half) % count
        span = pl.ds(start, CHUNK)
        raw = dot_rows(rows_v[span, :], wide_v[...])
        hidden_cot = dot_across(cots_v[span, :], down_v[...])
        gate, up = raw[:, :padded], raw[:, padded:]
        sigma = jax.nn.sigmoid(gate)
        hidden = (gate * sigma * up).astype(jnp.bfloat16)
        hidden_v[span, :] = hidden
        both_v[span, :padded] = (
            hidden_cot * up * sigma * (1.0 + gate * (1.0 - sigma))
        ).astype(jnp.bfloat16)
        both_v[span, padded:] = (hidden_cot * gate * sigma).astype(jnp.bfloat16)
        part = dot_across(both_v[span, :], wide_v[...])
        back_top = jnp.maximum(back_top, tops_of(part))
        if start >= half:
            piece = pl.ds(start - half, CHUNK)
            far_v[piece, :] = part
            wires.send(far_v.at[piece], come_v.at[piece], come_sem.at[at], seat.twin())
        else:
            near_v[span, :] = part
        hidden_size = jnp.abs(hidden.astype(jnp.float32))
        hidden_sum += jnp.sum(hidden_size, axis=0, keepdims=True)
        across = jnp.sum(hidden_size, axis=1, keepdims=True)
        hidden_top = jnp.maximum(hidden_top, jnp.max(across, axis=0, keepdims=True))
        both_sum += jnp.sum(jnp.abs(both_v[span, :].astype(jnp.float32)), axis=0, keepdims=True)
        cot_top = jnp.maximum(cot_top, jnp.max(jnp.abs(cots_v[span, :]), axis=0, keepdims=True))
    gain_top = jnp.max(jnp.abs(gains_v[8:9, :]), axis=1, keepdims=True)
    down_top = jnp.max(jnp.abs(down_v[...]), axis=0, keepdims=True).astype(jnp.float32)
    mine_v[0:1, :] = 2.0 * back_top
    mine_v[1:2, :] = (
        1.1 * jnp.max(hidden_sum, axis=1, keepdims=True) * cot_top.astype(jnp.float32)
    )
    mine_v[2:3, :] = 2.2 * hidden_top * down_top
    mine_v[3:4, :] = jnp.zeros((1, width), jnp.float32)
    mine_v[3:4, : 2 * padded] = (1.1 * width**0.5) * gain_top * both_sum
    mine_v[4:8, :] = jnp.zeros((4, width), jnp.float32)
    mates = [seat.mate(key) for key in range(1, GROUP)]
    others = [seat.peer(key) for key in range(1, lines)] + [seat.twin()]
    send_bounds(wires, mine_v.at[pl.ds(0, 8)], bounds_v, bound_sem, mates, 0)
    moves.put(hidden_v, hidden_out)

    def wide_step(at, carry):
        span = pl.ds(pl.multiple_of(at * CHUNK, CHUNK), CHUNK)
        wide_grad_v[span, :] = dot_down(rows_v[:, span], both_v[...])
        return carry

    lax.fori_loop(0, width // CHUNK // 2, wide_step, 0)
    mine_v[8:, :] = take_bounds(
        wires, seat, mine_v.at[pl.ds(0, 8)], bounds_v, bound_sem, mates, 0
    )
    send_bounds(wires, mine_v.at[pl.ds(8, 8)], bounds_v, bound_sem, others, len(mates))
    lax.fori_loop(width // CHUNK // 2, width // CHUNK, wide_step, 0)
    moves.put(wide_grad_v, wide_out)
    for at in range(chunks):
        wires.arrived(come_v.at[pl.ds(at * CHUNK, CHUNK)], come_sem.at[at], seat.twin())
    sum_up(near_v, come_v)
    moves.put(near_v, back_out)
    bounds = take_bounds(
        wires, seat, mine_v.at[pl.ds(8, 8)], bounds_v, bound_sem, others[:-1], len(mates)
    )
    last = len(mates) + len(others) - 1
    wires.arrived(bounds_v.at[last], bound_sem.at[last], seat.twin())
    for at in range(3):
        bound = bounds[at : at + 1]
        if at != 1:
            bound = jnp.maximum(bound, bounds_v[last, at : at + 1, :])
        put_scales(bound, factors_v.at[at])
    put_scales(bounds[3:4, : 2 * padded], wide_factors_v)
    moves.put(factors_v, factors)
    moves.put(wide_factors_v, wide_factors)
    moves.finish()
    wires.drain()


HBM = pl.BlockSpec(memory_space=pltpu.HBM)


def units(rows, cots, wide, down, gains, padded):
    count, width = rows.shape
    half = count // 2
    share = down.shape[0]
    lines = lax.axis_size("dp") // GROUP
    f32, bf16 = jnp.float32, rows.dtype
    shape, vmem, dma = jax.ShapeDtypeStruct, pltpu.VMEM, pltpu.SemaphoreType.DMA
    chunks = half // CHUNK
    rounds = GROUP - 1 + lines
    return pl.pallas_call(
        functools.partial(units_kernel, lines, share),
        out_shape=[
            shape((count, padded), bf16),
            shape((half, width), f32),
            shape((width, 2 * padded), f32),
            shape((3, 3, 8, width), f32),
            shape((3, 8, 2 * padded), f32),
        ],
        in_specs=[HBM] * 5,
        out_specs=[HBM] * 5,
        scratch_shapes=[
            vmem((count, width), bf16),
            vmem((count, width), bf16),
            vmem(wide.shape, bf16),
            vmem((padded, width), bf16),
            vmem(gains.shape, f32),
            vmem((count, padded), bf16),
            vmem((count, 2 * padded), bf16),
            vmem((half, width), f32),
            vmem((half, width), f32),
            vmem((half, width), f32),
            vmem((width, 2 * padded), f32),
            vmem((16, width), f32),
            vmem((rounds, 8, width), f32),
            vmem((3, 3, 8, width), f32),
            vmem((3, 8, 2 * padded), f32),
            dma((3 + 4 * chunks + 5,)),
            dma((chunks + rounds,)),
            dma((chunks,)),
            dma((rounds,)),
        ],
        compiler_params=pltpu.CompilerParams(
            collective_id=1, has_side_effects=True, vmem_limit_bytes=48 << 20
        ),
        cost_estimate=pl.CostEstimate(flops=10**10, bytes_accessed=2 * 10**7, transcendentals=0),
        name="units",
    )(rows, cots, wide, down, gains)


def grads_kernel(
    lines,
    share,
    cots,
    hidden,
    down,
    down_out,
    forth_out,
    cots_v,
    hidden_v,
    down_v,
    down_grad_v,
    far_v,
    near_v,
    come_v,
    move_sem,
    send_sem,
    come_sem,
):
    seat = Seat(lines)
    moves = Moves(move_sem)
    count, width = cots.shape
    half = count // 2
    padded = hidden_v.shape[1]
    pairs = ((hidden, hidden_v), (down, down_v.at[pl.ds(0, share)]), (cots, cots_v))
    loads = [moves.start(source, target) for source, target in pairs]
    down_v[share:, :] = jnp.zeros((padded - share, width), down_v.dtype)
    meet_twin(seat)
    wires = Wires(send_sem)
    for load in loads[:2]:
        load.wait()
    far_v[...] = dot_rows(hidden_v[half:, :], down_v[...])
    wires.send(far_v, come_v, come_sem.at[0], seat.twin())
    loads[2].wait()

    def down_step(at, carry):
        span = pl.ds(pl.multiple_of(at * LANES, LANES), LANES)
        down_grad_v[span, :] = dot_down(hidden_v[:, span], cots_v[...])
        return carry

    lax.fori_loop(0, padded // LANES, down_step, 0)
    moves.put(down_grad_v.at[pl.ds(0, share)], down_out)
    near_v[...] = dot_rows(hidden_v[:half, :], down_v[...])
    wires.arrived(come_v, come_sem.at[0], seat.twin())
    sum_up(near_v, come_v)
    moves.put(near_v, forth_out)
    moves.finish()
    wires.drain()


def grads(cots, hidden, down):
    count, width = cots.shape
    half = count // 2
    padded = hidden.shape[1]
    share = down.shape[0]
    lines = lax.axis_size("dp") // GROUP
    f32, bf16 = jnp.float32, cots.dtype
    shape, vmem, dma = jax.ShapeDtypeStruct, pltpu.VMEM, pltpu.SemaphoreType.DMA
    return pl.pallas_call(
        functools.partial(grads_kernel, lines, share),
        out_shape=[shape((share, width), f32), shape((half, width), f32)],
        in_specs=[HBM] * 3,
        out_specs=[HBM] * 2,
        scratch_shapes=[
            vmem((count, width), bf16),
            vmem((count, padded), bf16),
            vmem((padded, width), bf16),
            vmem((padded, width), f32),
            vmem((half, width), f32),
            vmem((half, width), f32),
            vmem((half, width), f32),
            dma((3 + 2,)),
            dma((1,)),
            dma((1,)),
        ],
        compiler_params=pltpu.CompilerParams(
            collective_id=2, has_side_effects=True, vmem_limit_bytes=40 << 20
        ),
        cost_estimate=pl.CostEstimate(flops=10**10, bytes_accessed=2 * 10**7, transcendentals=0),
        name="grads",
    )(cots, hidden, down)


def split_gain(flat, block, rows):
    start = block * rows
    chunk, offset = start // LANES, start % LANES
    lane = lax.broadcasted_iota(jnp.int32, (1, LANES), 1)
    piece = flat[:, chunk * LANES : (chunk + 1) * LANES]
    piece = pltpu.roll(piece, LANES - offset, 1) if offset else piece
    if offset + rows > LANES:
        more = flat[:, (chunk + 1) * LANES : (chunk + 2) * LANES]
        piece = jnp.where(lane < LANES - offset, piece, pltpu.roll(more, LANES - offset, 1))
    return jnp.where(lane < rows, piece, 0.0)


def norm_back(values, inverse, gain, cot):
    scaled = cot * gain
    share = jnp.mean(scaled * values, axis=1, keepdims=True)
    return inverse * scaled - values * (inverse * inverse * inverse) * share


def folded(values):
    return jnp.sum(values.reshape(-1, 8, values.shape[1]), axis=0)


def step_rows(start, which, half):
    return pl.ds(pl.multiple_of(which * half + start, STEP), STEP)


def half_of(target, which):
    half = target.shape[0] // 2
    return target.at[pl.ds(pl.multiple_of(which * half, half), half)]


def turn_kernel(
    lines,
    second_cot,
    residual,
    gains,
    cots,
    attended,
    out_full,
    residual_cot,
    mix_out,
    out_grad,
    sums_out,
    out_factors,
    second_v,
    residual_v,
    gains_v,
    cots_v,
    attended_v,
    out_v,
    seq_v,
    mix_v,
    out_grad_v,
    sums_v,
    out_rows,
    move_sem,
    send_sem,
    come_sem,
):
    seat = Seat(lines)
    core = seat.core
    moves = Moves(move_sem)
    half, width = residual.shape
    depth = attended.shape[1]
    bf16 = attended_v.dtype
    pairs = (
        (second_cot, second_v),
        (residual, residual_v),
        (gains, gains_v),
        (cots, cots_v),
        (attended, attended_v),
        (out_full, out_v),
    )
    loads = [moves.start(source, target) for source, target in pairs]
    meet_twin(seat)
    wires = Wires(send_sem)
    for load in loads[:4]:
        load.wait()
    sums_v[...] = jnp.zeros_like(sums_v)

    def norm_two(at, carry):
        start = pl.multiple_of(at * STEP, STEP)
        span = pl.ds(start, STEP)
        values, inverse = norm_rows(residual_v, start, STEP)
        cot = second_v[span, :]
        sums_v[...] += folded(cot * values * inverse)
        total = cots_v[span, :].astype(jnp.float32) + norm_back(
            values, inverse, gains_v[8:9, :], cot
        )
        residual_v[span, :] = total
        seq_v[step_rows(start, core, half), :] = total.astype(bf16)
        return carry

    lax.fori_loop(0, half // STEP, norm_two, 0)
    wires.send(half_of(seq_v, core), half_of(seq_v, core), come_sem.at[0], seat.twin())
    moves.put(residual_v, residual_cot)
    moves.put(sums_v, sums_out)
    for load in loads[4:]:
        load.wait()
    wires.arrived(half_of(seq_v, 1 - core), come_sem.at[0], seat.twin())

    def out_step(at, top):
        span = pl.ds(pl.multiple_of(at * LANES, LANES), LANES)
        part = dot_down(attended_v[:, span], seq_v[...])
        out_grad_v[span, :] = part
        return jnp.maximum(top, tops_of(part))

    top = lax.fori_loop(0, depth // LANES, out_step, jnp.zeros((1, width), jnp.float32))
    moves.put(out_grad_v, out_grad)
    put_scales(top, out_rows)
    moves.put(out_rows, out_factors)
    mix_v[...] = dot_across(seq_v[...], out_v[...]).astype(bf16)
    moves.put(mix_v, mix_out)
    moves.finish()
    wires.drain()


def turn(second_cot, residual, gains, cots, attended, out_full):
    lines = lax.axis_size("dp") // GROUP
    half, width = residual.shape
    depth = attended.shape[1]
    f32, bf16 = jnp.float32, attended.dtype
    shape, vmem, dma = jax.ShapeDtypeStruct, pltpu.VMEM, pltpu.SemaphoreType.DMA
    sources = (second_cot, residual, gains, cots, attended, out_full)
    return pl.pallas_call(
        functools.partial(turn_kernel, lines),
        out_shape=[
            shape((half, width), f32),
            shape((2 * half, depth), bf16),
            shape((depth, width), f32),
            shape((8, width), f32),
            shape((3, 8, width), f32),
        ],
        in_specs=[HBM] * len(sources),
        out_specs=[HBM] * 5,
        scratch_shapes=[vmem(part.shape, part.dtype) for part in sources]
        + [
            vmem((2 * half, width), bf16),
            vmem((2 * half, depth), bf16),
            vmem((depth, width), f32),
            vmem((8, width), f32),
            vmem((3, 8, width), f32),
            dma((len(sources) + 5,)),
            dma((1,)),
            dma((1,)),
        ],
        compiler_params=pltpu.CompilerParams(
            collective_id=3, has_side_effects=True, vmem_limit_bytes=24 << 20
        ),
        cost_estimate=pl.CostEstimate(flops=10**10, bytes_accessed=2 * 10**7, transcendentals=0),
        name="turn",
    )(*sources)


def rear_kernel(
    lines,
    members,
    residual_cot,
    mix,
    sums,
    gains,
    inputs,
    heads,
    attended,
    narrow_full,
    normed,
    tables,
    input_grad,
    narrow_grad,
    narrow_factors,
    residual_v,
    mix_v,
    sums_in_v,
    gains_v,
    inputs_v,
    heads_v,
    attended_v,
    narrow_v,
    normed_v,
    tables_v,
    cot_v,
    pair_v,
    far_v,
    near_v,
    come_v,
    narrow_grad_v,
    sums_v,
    sums_come_v,
    gain_grad_v,
    narrow_rows,
    move_sem,
    send_sem,
    come_sem,
):
    seat = Seat(lines)
    core = seat.core
    moves = Moves(move_sem)
    half, width = inputs.shape
    depth = attended.shape[1]
    cols = heads.shape[1]
    count = width // members
    bf16 = heads_v.dtype
    pairs = (
        (mix, mix_v),
        (heads, heads_v),
        (attended, attended_v),
        (tables, tables_v),
        (narrow_full, narrow_v),
        (normed, normed_v),
        (residual_cot, residual_v),
        (sums, sums_in_v),
        (gains, gains_v),
        (inputs, inputs_v),
    )
    loads = [moves.start(source, target) for source, target in pairs]
    meet_twin(seat)
    wires = Wires(send_sem)
    for load in loads[:4]:
        load.wait()
    pair_v[...] = jnp.zeros_like(pair_v)

    def pair(at, carry):
        lanes = pl.ds(pl.multiple_of(at * LANES, LANES), LANES)
        key, value = heads_v[:, depth : depth + HD], heads_v[:, depth + HD : depth + 2 * HD]
        query_both, mix_both = heads_v[:, lanes], mix_v[:, lanes]
        delta_both = mix_both.astype(jnp.float32) * attended_v[:, lanes].astype(jnp.float32)
        parts = []
        for head in range(LANES // HD):
            own = slice(head * HD, (head + 1) * HD)
            query, mix_own = query_both[:, own], mix_both[:, own]
            probs = probabilities(query, key)
            value_part = dot_down(probs.astype(bf16), mix_own)
            delta = jnp.sum(delta_both[:, own], axis=1, keepdims=True)
            score_cot = (probs * (dot_across(mix_own, value) - delta)).astype(bf16)
            parts.append(dot_rows(score_cot, key) * (HD**-0.5))
            key_part = dot_down(score_cot, query) * (HD**-0.5)
            pair_v[...] += jnp.concatenate([key_part, value_part], axis=1)
        query_cot = turned(jnp.concatenate(parts, axis=1), tables_v[0], -tables_v[1])
        cot_v[:, lanes] = query_cot.astype(bf16)
        return carry

    lax.fori_loop(0, depth // LANES, pair, 0)
    cot_v[:, depth:] = turned(pair_v[...], tables_v[2], -tables_v[3]).astype(bf16)
    for load in loads[4:]:
        load.wait()

    def part_of(which):
        rows_of = cot_v[pl.ds(pl.multiple_of(which * half, half), half), :]
        return dot_across(rows_of, narrow_v[...])

    far_v[...] = part_of(1 - core)
    wires.send(far_v, come_v, come_sem.at[0], seat.twin())
    near_v[...] = part_of(core)

    def narrow_step(at, top):
        span = pl.ds(pl.multiple_of(at * CHUNK, CHUNK), CHUNK)
        part = dot_down(normed_v[:, span], cot_v[...])
        narrow_grad_v[span, :] = part
        return jnp.maximum(top, tops_of(part))

    top = lax.fori_loop(0, width // CHUNK, narrow_step, jnp.zeros((1, cols), jnp.float32))
    for block in range(members):
        moves.put(
            narrow_grad_v.at[pl.ds(block * count, count)], narrow_grad.at[block, pl.ds(0, count)]
        )
    wires.arrived(come_v, come_sem.at[0], seat.twin())
    sums_v[8:, :] = sums_in_v[...]
    sums_v[:8, :] = jnp.zeros_like(sums_in_v)

    def norm_one(at, carry):
        start = pl.multiple_of(at * STEP, STEP)
        span = pl.ds(start, STEP)
        values, inverse = norm_rows(inputs_v, start, STEP)
        cot = near_v[span, :] + come_v[span, :]
        sums_v[:8, :] += folded(cot * values * inverse)
        near_v[span, :] = residual_v[span, :] + norm_back(values, inverse, gains_v[0:1, :], cot)
        return carry

    lax.fori_loop(0, half // STEP, norm_one, 0)
    wires.send(sums_v, sums_come_v, come_sem.at[1], seat.twin())
    moves.put(near_v, input_grad)
    wires.arrived(sums_come_v, come_sem.at[1], seat.twin())
    both = sums_v[...] + sums_come_v[...]
    flat = [jnp.sum(both[8 * at : 8 * at + 8, :], axis=0, keepdims=True) for at in range(2)]
    gain_grad_v[...] = jnp.zeros_like(gain_grad_v)
    for block in range(members):
        for at in range(2):
            piece = split_gain(flat[at], block, count)
            gain_grad_v[block, 0:1, at * LANES : (at + 1) * LANES] = piece
            lanes = slice(at * LANES, (at + 1) * LANES)
            raised = jnp.maximum(top[:, lanes], jnp.abs(piece))
            top = jnp.concatenate(
                [part for part in (top[:, : at * LANES], raised, top[:, (at + 1) * LANES :]) if part.size],
                axis=1,
            )
    moves.put(gain_grad_v, narrow_grad.at[:, pl.ds(count, 8), :])
    put_scales(top, narrow_rows)
    moves.put(narrow_rows, narrow_factors)
    moves.finish()
    wires.drain()


def rear(residual_cot, mix, sums, gains, inputs, heads, attended, narrow_full, normed, tables):
    members = lax.axis_size("dp")
    lines = members // GROUP
    half, width = inputs.shape
    cols = heads.shape[1]
    count = width // members
    f32, bf16 = jnp.float32, heads.dtype
    shape, vmem, dma = jax.ShapeDtypeStruct, pltpu.VMEM, pltpu.SemaphoreType.DMA
    sources = (
        residual_cot,
        mix,
        sums,
        gains,
        inputs,
        heads,
        attended,
        narrow_full,
        normed,
        tables,
    )
    return pl.pallas_call(
        functools.partial(rear_kernel, lines, members),
        out_shape=[
            shape((half, width), f32),
            shape((members, count + 8, cols), f32),
            shape((3, 8, cols), f32),
        ],
        in_specs=[HBM] * len(sources),
        out_specs=[HBM] * 3,
        scratch_shapes=[vmem(part.shape, part.dtype) for part in sources]
        + [
            vmem((2 * half, cols), bf16),
            vmem((2 * half, LANES), f32),
            vmem((half, width), f32),
            vmem((half, width), f32),
            vmem((half, width), f32),
            vmem((width, cols), f32),
            vmem((16, width), f32),
            vmem((16, width), f32),
            vmem((members, 8, cols), f32),
            vmem((3, 8, cols), f32),
            dma((len(sources) + members + 3,)),
            dma((2,)),
            dma((2,)),
        ],
        compiler_params=pltpu.CompilerParams(
            collective_id=4, has_side_effects=True, vmem_limit_bytes=32 << 20
        ),
        cost_estimate=pl.CostEstimate(flops=10**10, bytes_accessed=2 * 10**7, transcendentals=0),
        name="rear",
    )(*sources)


def unshare_kernel(share, lines, pieces, gate, up):
    place = lax.rem(lax.axis_index("dp"), GROUP)
    unit_rows = share // lines
    padded = pieces.shape[2] // 2
    for start, target in ((0, gate), (padded, up)):
        parts = []
        for at in range(lines):
            for other in range(GROUP):
                piece = pieces[flipped(place, other) if other else place]
                first = start + at * unit_rows
                parts.append(piece[:, first : first + unit_rows])
        target[...] = jnp.concatenate(parts, axis=1)


def unshare(pieces, share, lines):
    rows = pieces.shape[1]
    result = jax.ShapeDtypeStruct((rows, GROUP * share), pieces.dtype)
    return pl.pallas_call(
        functools.partial(unshare_kernel, share, lines), out_shape=[result] * 2, name="unshare"
    )(pieces)


def grouped_shards(
    block_input,
    attn_gain,
    query_weight,
    key_weight,
    value_weight,
    output_weight,
    ffn_gain,
    gate_weight,
    up_weight,
    down_weight,
    output_cotangent,
):
    f32, bf16 = jnp.float32, jnp.bfloat16
    members = lax.axis_size("dp")
    lines = members // GROUP
    index = lax.axis_index("dp")
    own, place = index // GROUP, lax.rem(index, GROUP)
    rows, _ = gate_weight.shape
    width = rows * members
    query_cols, key_cols = query_weight.shape[1], key_weight.shape[1]
    unit_rows = down_weight.shape[0]
    share = unit_rows * lines
    padded = whole_up(share, LANES)

    narrow = jnp.concatenate([query_weight, key_weight, value_weight], axis=1)
    cols = narrow.shape[1]
    gains = jnp.stack([attn_gain, ffn_gain])
    gains = jnp.pad(gains, ((0, 6), (0, whole_up(rows, LANES) - rows)))

    def shares(weight):
        parts = weight.reshape(rows, lines, GROUP, unit_rows).transpose(2, 0, 1, 3)
        return jnp.pad(parts.reshape(GROUP, rows, share), ((0, 0), (0, 0), (0, padded - share)))

    pieces = jnp.concatenate([shares(gate_weight), shares(up_weight)], axis=2)
    length = 2 * block_input.shape[0]
    cosine, sine = rope_tables(length, HD)
    still, none = jnp.ones((length, HD), f32), jnp.zeros((length, HD), f32)
    twice = jnp.concatenate([cosine] * 4, axis=1)
    signed = jnp.concatenate([-sine, sine] * 2, axis=1)
    tables = jnp.stack(
        [
            twice,
            signed,
            jnp.concatenate([twice[:, :HD], still], axis=1),
            jnp.concatenate([signed[:, :HD], none], axis=1),
        ]
    )
    (
        gains_rows,
        narrow_full,
        out_full,
        wide,
        downs,
        cot_rows,
        ffn_rows,
        normed_one,
        heads,
        attn_rows,
        residual,
    ) = front(
        gains, narrow, output_weight, pieces, down_weight, block_input, output_cotangent, tables
    )
    cot_rows = cot_rows.reshape(-1, width)
    ffn_rows = ffn_rows.reshape(-1, width)
    wide_full = wide.reshape(width, 2 * padded)
    down_share = downs.reshape(share, width)
    half = block_input.shape[0]

    hidden, back_sum, wide_grad, factors, wide_factors = units(
        ffn_rows, cot_rows, wide_full, down_share, gains_rows, padded
    )
    back_sum = back_sum.reshape(GROUP, half, width)
    back_out = [narrowed(back_sum[key], factors[0, 0, :1]) for key in range(1, GROUP)]
    back_in = exchanged(back_out, partner)

    wide_grad = after(wide_grad.reshape(lines, GROUP * rows, 2 * padded), *back_out)
    wide_out = messages_of(wide_grad, wide_factors[0, :1], own)
    wide_in = exchanged(wide_out, across)
    hidden = after(hidden, *wide_out)
    down_grad, forth_sum = grads(cot_rows, hidden, down_share)
    down_grad = down_grad.reshape(lines, unit_rows, width)
    down_out = messages_of(down_grad, factors[1, 0, :1], own)
    down_in = exchanged(down_out, across)

    back_in = after(back_in, *down_out)
    second_cot = added(back_sum[0], back_in, factors[0, 1, :1])
    residual_cot, mix, out_grad, sums, out_factors = turn(
        second_cot, residual, gains_rows, output_cotangent, attn_rows, out_full
    )
    out_grad = out_grad.reshape(lines, GROUP, -1, width)
    out_out = group_messages(out_grad, place, out_factors[0, :1], out_factors[2])
    out_in = exchanged(out_out, partner)
    residual_cot = after(residual_cot, *out_out)
    input_grad, narrow_grad, narrow_factors = rear(
        residual_cot,
        mix,
        sums,
        gains_rows,
        block_input,
        heads,
        attn_rows,
        narrow_full,
        normed_one,
        tables,
    )
    narrow_grad = narrow_grad.reshape(lines, GROUP, -1, cols)
    narrow_out = group_messages(narrow_grad, place, narrow_factors[0, :1], narrow_factors[2])
    narrow_in = exchanged(narrow_out, partner)

    forth_sum = after(forth_sum.reshape(GROUP, half, width), *narrow_out)
    forth_out = [narrowed(forth_sum[key], factors[2, 0, :1]) for key in range(1, GROUP)]
    forth_in = exchanged(forth_out, partner)
    out_in = after(out_in, *forth_out)
    out_undos = [undo_of(message) for message in out_in]
    out_sum = lax.dynamic_index_in_dim(out_grad, place, 1, keepdims=False)
    out_sum = added_noted(out_sum, out_in, out_undos)
    out_line = line_messages(out_sum, raised(out_factors[1, :1], out_undos), own)
    out_line_in = exchanged(out_line, across)
    wide_in = after(wide_in, *out_line)
    wide_undo = wide_factors[1, :1]
    wide_own = added(lax.dynamic_index_in_dim(wide_grad, own, 0, keepdims=False), wide_in, wide_undo)
    wide_own = wide_own.reshape(GROUP, rows, 2 * padded)
    share_out = messages_of(wide_own, 0.25 * wide_factors[0, :1], place)
    share_in = exchanged(share_out, partner)
    narrow_in = after(narrow_in, *share_out)
    narrow_undos = [undo_of(message) for message in narrow_in]
    narrow_sum = lax.dynamic_index_in_dim(narrow_grad, place, 1, keepdims=False)
    narrow_sum = added_noted(narrow_sum, narrow_in, narrow_undos)
    narrow_line = line_messages(narrow_sum, raised(narrow_factors[1, :1], narrow_undos), own)
    narrow_line_in = exchanged(narrow_line, across)
    forth_in = after(forth_in, *narrow_line)
    block_output = (residual + added(forth_sum[0], forth_in, factors[2, 1, :1])).astype(bf16)
    share_in = after(share_in, block_output)
    pieces = [lax.dynamic_index_in_dim(wide_own, place, 0, keepdims=False)]
    pieces += [message.astype(f32) * (4.0 * wide_undo) for message in share_in]
    gate_own, up_own = unshare(jnp.stack(pieces), share, lines)
    down_in = after(down_in, gate_own, up_own)
    down_own = lax.dynamic_index_in_dim(down_grad, own, 0, keepdims=False)
    down_own = added(down_own, down_in, factors[1, 1, :1])
    out_line_in = after(out_line_in, down_own)
    out_own = added_noted(
        lax.dynamic_index_in_dim(out_sum, own, 0, keepdims=False),
        out_line_in,
        [undo_of(message) for message in out_line_in],
    )
    narrow_line_in = after(narrow_line_in, out_own)
    narrow_own = added_noted(
        lax.dynamic_index_in_dim(narrow_sum, own, 0, keepdims=False),
        narrow_line_in,
        [undo_of(message) for message in narrow_line_in],
    )
    return (
        block_output,
        input_grad,
        narrow_own[rows, :rows],
        narrow_own[:rows, :query_cols],
        narrow_own[:rows, query_cols : query_cols + key_cols],
        narrow_own[:rows, query_cols + key_cols :],
        out_own,
        narrow_own[rows, LANES : LANES + rows],
        gate_own,
        up_own,
        down_own,
    )


def solution(mesh):
    placed = (
        P(("dp", "mp"), None),
        P("dp"),
        P("dp", "mp"),
        P("dp", "mp"),
        P("dp", "mp"),
        P(("mp", "dp"), None),
        P("dp"),
        P("dp", "mp"),
        P("dp", "mp"),
        P(("mp", "dp"), None),
        P(("dp", "mp"), None),
    )
    members = mesh.shape["dp"]
    fits = mesh.shape["mp"] == 2 and members in (2 * GROUP, 4 * GROUP)
    return jax.shard_map(
        grouped_shards if fits else plain_shards,
        mesh=mesh,
        in_specs=placed,
        out_specs=(
            P(("dp", "mp"), None),
            P(("dp", "mp"), None),
            P("dp"),
            P("dp", "mp"),
            P("dp", "mp"),
            P("dp", "mp"),
            P(("mp", "dp"), None),
            P("dp"),
            P("dp", "mp"),
            P("dp", "mp"),
            P(("mp", "dp"), None),
        ),
        check_vma=False,
    )
```

```python
import functools

import jax
import jax.numpy as jnp
from jax import lax
from jax.experimental import pallas as pl
from jax.experimental.pallas import tpu as pltpu
from jax.sharding import PartitionSpec as P


HD = 64


EPSILON = 1e-05
ROPE_BASE = 10000.0


def rope_tables(length, head_dim):
    half_dim = head_dim // 2
    position = jnp.arange(length, dtype=jnp.float32)
    inverse = ROPE_BASE ** (-(jnp.arange(half_dim, dtype=jnp.float32) * (2.0 / head_dim)))
    angle = position[:, None] * inverse[None, :]
    return (jnp.cos(angle), jnp.sin(angle))


def rotate(values, cosine, sine):
    half_dim = values.shape[-1] // 2
    first_half = values[..., :half_dim]
    second_half = values[..., half_dim:]
    cos_part = cosine[:, None, :]
    sin_part = sine[:, None, :]
    return jnp.concatenate(
        [
            first_half * cos_part - second_half * sin_part,
            second_half * cos_part + first_half * sin_part,
        ],
        axis=-1,
    )


def unrotate(values, cosine, sine):
    half_dim = values.shape[-1] // 2
    first_half = values[..., :half_dim]
    second_half = values[..., half_dim:]
    cos_part = cosine[:, None, :]
    sin_part = sine[:, None, :]
    return jnp.concatenate(
        [
            first_half * cos_part + second_half * sin_part,
            second_half * cos_part - first_half * sin_part,
        ],
        axis=-1,
    )


def norm_scale(values):
    return lax.rsqrt(jnp.mean(values * values, axis=-1, keepdims=True) + EPSILON)


def norm_backward(values, inverse, gain, normed_cot):
    scaled = normed_cot * gain.astype(jnp.float32)[None, :]
    gain_grad = jnp.sum(normed_cot * values * inverse, axis=0)
    values_grad = inverse * scaled - values * (inverse * inverse * inverse) * jnp.mean(
        scaled * values, axis=-1, keepdims=True
    )
    return (gain_grad, values_grad)


def causal_scores(query_group, key_group):
    scale = query_group.shape[-1] ** (-0.5)
    scores = (
        jnp.einsum("qgd,kd->gqk", query_group, key_group, preferred_element_type=jnp.float32)
        * scale
    )
    length = key_group.shape[0]
    visible = lax.broadcasted_iota(jnp.int32, (length, length), 0) >= lax.broadcasted_iota(
        jnp.int32, (length, length), 1
    )
    return jnp.where(visible[None], scores, -jnp.inf)


def head_forward(parts):
    query_group, key_group, value_group = parts
    scores = causal_scores(query_group, key_group)
    top_score = jnp.max(scores, axis=-1, keepdims=True)
    log_norm = top_score + jnp.log(jnp.sum(jnp.exp(scores - top_score), axis=-1, keepdims=True))
    probs_b = jnp.exp(scores - log_norm).astype(jnp.bfloat16)
    attended = jnp.einsum(
        "gqk,kd->qgd", probs_b, value_group, preferred_element_type=jnp.float32
    ).astype(jnp.bfloat16)
    return (attended, log_norm[..., 0])


def head_backward(parts):
    query_group, key_group, value_group, attended, log_norm, attended_cot = parts
    scale = query_group.shape[-1] ** (-0.5)
    scores = causal_scores(query_group, key_group)
    probs = jnp.exp(scores - log_norm[..., None])
    probs_b = probs.astype(jnp.bfloat16)
    value_cot = jnp.einsum("gqk,qgd->kd", probs_b, attended_cot, preferred_element_type=jnp.float32)
    probs_cot = jnp.einsum(
        "qgd,kd->gqk", attended_cot, value_group, preferred_element_type=jnp.float32
    )
    delta = jnp.sum(attended_cot.astype(jnp.float32) * attended.astype(jnp.float32), axis=-1).T
    score_cot = (probs * (probs_cot - delta[:, :, None])).astype(jnp.bfloat16)
    query_cot = (
        jnp.einsum("gqk,kd->qgd", score_cot, key_group, preferred_element_type=jnp.float32) * scale
    )
    key_cot = (
        jnp.einsum("gqk,qgd->kd", score_cot, query_group, preferred_element_type=jnp.float32)
        * scale
    )
    return (query_cot, key_cot, value_cot)


def plain_shards(
    block_input,
    attn_gain,
    query_weight,
    key_weight,
    value_weight,
    output_weight,
    ffn_gain,
    gate_weight,
    up_weight,
    down_weight,
    output_cotangent,
):
    local_rows = block_input.shape[0]
    own_start = lax.axis_index("mp") * local_rows
    query_full, key_full, value_full, out_full, gain_one = (
        lax.all_gather(query_weight, "dp", axis=0, tiled=True),
        lax.all_gather(key_weight, "dp", axis=0, tiled=True),
        lax.all_gather(value_weight, "dp", axis=0, tiled=True),
        lax.all_gather(output_weight, "dp", axis=0, tiled=True),
        lax.all_gather(attn_gain, "dp", axis=0, tiled=True),
    )
    seq_input = lax.all_gather(block_input, "mp", axis=0, tiled=True)
    length = seq_input.shape[0]
    local_heads = query_full.shape[1] // HD
    local_groups = key_full.shape[1] // HD
    per_group = local_heads // local_groups
    cosine, sine = rope_tables(length, HD)
    input_f32 = seq_input.astype(jnp.float32)
    inv_one = norm_scale(input_f32)
    normed_one = (input_f32 * inv_one * gain_one.astype(jnp.float32)[None, :]).astype(jnp.bfloat16)
    query_raw = jnp.dot(normed_one, query_full, preferred_element_type=jnp.float32)
    key_raw = jnp.dot(normed_one, key_full, preferred_element_type=jnp.float32)
    value_raw = jnp.dot(normed_one, value_full, preferred_element_type=jnp.float32)
    query_rot = rotate(query_raw.reshape(length, local_heads, HD), cosine, sine).astype(
        jnp.bfloat16
    )
    key_rot = rotate(key_raw.reshape(length, local_groups, HD), cosine, sine).astype(jnp.bfloat16)
    value_b = value_raw.astype(jnp.bfloat16)
    query_groups = query_rot.reshape(length, local_groups, per_group, HD).transpose(1, 0, 2, 3)
    key_groups = key_rot.transpose(1, 0, 2)
    value_groups = value_b.reshape(length, local_groups, HD).transpose(1, 0, 2)
    attended, log_norm = lax.map(head_forward, (query_groups, key_groups, value_groups))
    attn_rows = attended.transpose(1, 0, 2, 3).reshape(length, local_heads * HD)
    attn_part = jnp.dot(attn_rows, out_full, preferred_element_type=jnp.float32)
    residual = input_f32 + lax.psum(attn_part, "mp")
    gate_full, up_full, down_full, gain_two = (
        lax.all_gather(gate_weight, "dp", axis=0, tiled=True),
        lax.all_gather(up_weight, "dp", axis=0, tiled=True),
        lax.all_gather(down_weight, "dp", axis=0, tiled=True),
        lax.all_gather(ffn_gain, "dp", axis=0, tiled=True),
    )
    inv_two = norm_scale(residual)
    normed_two = (residual * inv_two * gain_two.astype(jnp.float32)[None, :]).astype(jnp.bfloat16)
    gate_raw = jnp.dot(normed_two, gate_full, preferred_element_type=jnp.float32)
    up_raw = jnp.dot(normed_two, up_full, preferred_element_type=jnp.float32)
    sigma = jax.nn.sigmoid(gate_raw)
    hidden = (gate_raw * sigma * up_raw).astype(jnp.bfloat16)
    ffn_own = lax.psum_scatter(
        jnp.dot(hidden, down_full, preferred_element_type=jnp.float32),
        "mp",
        scatter_dimension=0,
        tiled=True,
    )
    residual_own = lax.dynamic_slice_in_dim(residual, own_start, local_rows, 0)
    block_output = (residual_own + ffn_own).astype(jnp.bfloat16)
    cot_seq = lax.all_gather(output_cotangent, "mp", axis=0, tiled=True)
    hidden_cot = jnp.einsum("td,fd->tf", cot_seq, down_full, preferred_element_type=jnp.float32)
    gate_cot = (hidden_cot * up_raw * sigma * (1.0 + gate_raw * (1.0 - sigma))).astype(jnp.bfloat16)
    up_cot = (hidden_cot * gate_raw * sigma).astype(jnp.bfloat16)
    normed_two_part = jnp.einsum(
        "tf,df->td", gate_cot, gate_full, preferred_element_type=jnp.float32
    )
    normed_two_part = normed_two_part + jnp.einsum(
        "tf,df->td", up_cot, up_full, preferred_element_type=jnp.float32
    )
    normed_two_cot = lax.psum(normed_two_part, "mp")
    ffn_gain_grad, residual_part = norm_backward(residual, inv_two, gain_two, normed_two_cot)
    residual_cot = cot_seq.astype(jnp.float32) + residual_part
    down_grad = jnp.einsum("tf,td->fd", hidden, cot_seq, preferred_element_type=jnp.float32)
    gate_grad = jnp.einsum("td,tf->df", normed_two, gate_cot, preferred_element_type=jnp.float32)
    up_grad = jnp.einsum("td,tf->df", normed_two, up_cot, preferred_element_type=jnp.float32)
    gate_share, up_share, down_share, ffn_gain_share = (
        lax.psum_scatter(gate_grad, "dp", scatter_dimension=0, tiled=True),
        lax.psum_scatter(up_grad, "dp", scatter_dimension=0, tiled=True),
        lax.psum_scatter(down_grad, "dp", scatter_dimension=0, tiled=True),
        lax.psum_scatter(ffn_gain_grad, "dp", scatter_dimension=0, tiled=True),
    )
    residual_cot_b = residual_cot.astype(jnp.bfloat16)
    output_weight_grad = jnp.einsum(
        "th,td->hd", attn_rows, residual_cot_b, preferred_element_type=jnp.float32
    )
    attended_cot = jnp.einsum(
        "td,hd->th", residual_cot_b, out_full, preferred_element_type=jnp.float32
    ).astype(jnp.bfloat16)
    cot_groups = attended_cot.reshape(length, local_groups, per_group, HD).transpose(1, 0, 2, 3)
    query_parts, key_parts, value_parts = lax.map(
        head_backward, (query_groups, key_groups, value_groups, attended, log_norm, cot_groups)
    )
    query_cot = (
        unrotate(query_parts.transpose(1, 0, 2, 3).reshape(length, local_heads, HD), cosine, sine)
        .reshape(length, local_heads * HD)
        .astype(jnp.bfloat16)
    )
    key_cot = (
        unrotate(key_parts.transpose(1, 0, 2), cosine, sine)
        .reshape(length, local_groups * HD)
        .astype(jnp.bfloat16)
    )
    value_cot = (
        value_parts.transpose(1, 0, 2).reshape(length, local_groups * HD).astype(jnp.bfloat16)
    )
    normed_one_part = jnp.einsum(
        "th,dh->td", query_cot, query_full, preferred_element_type=jnp.float32
    )
    normed_one_part = normed_one_part + jnp.einsum(
        "th,dh->td", key_cot, key_full, preferred_element_type=jnp.float32
    )
    normed_one_part = normed_one_part + jnp.einsum(
        "th,dh->td", value_cot, value_full, preferred_element_type=jnp.float32
    )
    normed_one_cot = lax.psum(normed_one_part, "mp")
    query_grad = jnp.einsum("td,th->dh", normed_one, query_cot, preferred_element_type=jnp.float32)
    key_grad = jnp.einsum("td,th->dh", normed_one, key_cot, preferred_element_type=jnp.float32)
    value_grad = jnp.einsum("td,th->dh", normed_one, value_cot, preferred_element_type=jnp.float32)
    attn_gain_grad, input_part = norm_backward(input_f32, inv_one, gain_one, normed_one_cot)
    input_cot = residual_cot + input_part
    input_grad = lax.dynamic_slice_in_dim(input_cot, own_start, local_rows, 0)
    attn_gain_share, query_share, key_share, value_share, output_share = (
        lax.psum_scatter(attn_gain_grad, "dp", scatter_dimension=0, tiled=True),
        lax.psum_scatter(query_grad, "dp", scatter_dimension=0, tiled=True),
        lax.psum_scatter(key_grad, "dp", scatter_dimension=0, tiled=True),
        lax.psum_scatter(value_grad, "dp", scatter_dimension=0, tiled=True),
        lax.psum_scatter(output_weight_grad, "dp", scatter_dimension=0, tiled=True),
    )
    return (
        block_output,
        input_grad,
        attn_gain_share,
        query_share,
        key_share,
        value_share,
        output_share,
        ffn_gain_share,
        gate_share,
        up_share,
        down_share,
    )


GROUP = 4
LANES = 128


def whole_up(size, step):
    return -(-size // step) * step


def partner(values, key):
    pairs = [(at, at ^ key) for at in range(lax.axis_size("dp"))]
    return lax.ppermute(values, "dp", pairs)


def across(values, key):
    pairs = [(at, at ^ (key * GROUP)) for at in range(lax.axis_size("dp"))]
    return lax.ppermute(values, "dp", pairs)


def after(value, *marks):
    return lax.optimization_barrier((value,) + marks)[0]


def narrowed(values, scale):
    return (values * scale).astype(jnp.float16)


def added(total, messages, undo):
    come = sum(message.astype(jnp.float32) for message in messages)
    return total + (come * undo).reshape(total.shape)


def messages_of(blocks, scale, at):
    return [
        narrowed(lax.dynamic_index_in_dim(blocks, at ^ key, 0, keepdims=False), scale)
        for key in range(1, blocks.shape[0])
    ]


def noted(values, scale, notes):
    return jnp.concatenate([values * scale, notes], axis=0).astype(jnp.float16)


def undo_of(message):
    return jnp.prod(message[-8:].astype(jnp.float32), axis=0, keepdims=True)


def group_messages(blocks, place, scale, notes):
    cols = blocks.shape[3]
    return [
        noted(
            lax.dynamic_index_in_dim(blocks, place ^ key, 1, keepdims=False).reshape(-1, cols),
            scale,
            notes,
        )
        for key in range(1, GROUP)
    ]


def line_messages(blocks, undo, at):
    power = jnp.log2(undo)
    row = lax.broadcasted_iota(jnp.float32, (8, undo.shape[1]), 0)
    notes = jnp.exp2(jnp.floor((jnp.round(power) + row) * 0.125))
    scale, notes = lax.optimization_barrier((1.0 / undo, notes))
    return [
        noted(lax.dynamic_index_in_dim(blocks, at ^ key, 0, keepdims=False), scale, notes)
        for key in range(1, blocks.shape[0])
    ]


def added_noted(total, messages, undos):
    shape, cols = total.shape, total.shape[-1]
    total = total.reshape(-1, cols)
    for message, undo in zip(messages, undos):
        total = total + message[:-8].astype(jnp.float32) * undo
    return total.reshape(shape)


def raised(undo, undos):
    for other in undos:
        undo = jnp.maximum(undo, other)
    return 4.0 * undo


def line_halves(blocks, scale, undo):
    rows, cols = blocks.shape[1:]
    own = lax.axis_index("dp") // GROUP
    high, low = own // 2, lax.rem(own, 2)
    blocks = blocks.reshape(2, 2, rows, cols)
    away = lax.dynamic_index_in_dim(blocks, 1 - low, 1, keepdims=False)
    message = narrowed(away.reshape(2 * rows, cols), scale)
    near = across(message, 1).reshape(2, rows, cols)
    keep = lax.dynamic_index_in_dim(blocks, low, 1, keepdims=False)

    def half(which, near):
        part = lax.dynamic_index_in_dim(near, which, 0, keepdims=False).astype(jnp.float32)
        return lax.dynamic_index_in_dim(keep, which, 0, keepdims=False) + part * undo

    def second(near):
        message = narrowed(half(1 - high, near), 0.5 * scale)
        return message, across(message, 2)

    def ended(near, far):
        return half(high, near) + far.astype(jnp.float32) * (2.0 * undo)

    return message, near, second, ended


def exchanged(messages, exchange):
    return [exchange(message, key + 1) for key, message in enumerate(messages)]


MESH = pl.DeviceIdType.MESH


def flipped(place, key):
    if key == 1:
        return place + 1 - 2 * lax.rem(place, 2)
    if key == 2:
        return place + 2 - 4 * lax.div(place, 2)
    return GROUP - 1 - place


class Wires:
    def __init__(self, send_sem):
        self.send_sem, self.used, self.open = send_sem, 0, []

    def send(self, source, target, arrival, device, when=None):
        copy = pltpu.make_async_remote_copy(
            src_ref=source,
            dst_ref=target,
            send_sem=self.send_sem.at[self.used],
            recv_sem=arrival,
            device_id=device,
            device_id_type=MESH,
        )
        self.used += 1
        self.open.append((copy, when))
        if when is None:
            copy.start()
        else:
            pl.when(when)(copy.start)

    def arrived(self, target, arrival, device, when=None):
        copy = pltpu.make_async_remote_copy(
            src_ref=target,
            dst_ref=target,
            send_sem=self.send_sem.at[0],
            recv_sem=arrival,
            device_id=device,
            device_id_type=MESH,
        )
        if when is None:
            copy.wait_recv()
        else:
            pl.when(when)(copy.wait_recv)

    def drain(self):
        for copy, when in self.open:
            if when is None:
                copy.wait_send()
            else:
                pl.when(when)(copy.wait_send)


class Seat:
    def __init__(self, lines):
        self.index = lax.axis_index("dp")
        self.core = lax.axis_index("mp")
        self.own, self.place = lax.div(self.index, GROUP), lax.rem(self.index, GROUP)
        self.lines = lines

    def mate(self, key):
        return (self.own * GROUP + flipped(self.place, key), self.core)

    def line(self, step):
        return ((self.own + step) * GROUP + self.place, self.core)

    def peer(self, key):
        return (flipped(self.own, key) * GROUP + self.place, self.core)

    def twin(self):
        return (self.index, 1 - self.core)

    def greet(self):
        barrier = pltpu.get_barrier_semaphore()
        for key in range(1, GROUP):
            pl.semaphore_signal(barrier, 1, device_id=self.mate(key), device_id_type=MESH)
        pl.semaphore_signal(barrier, 1, device_id=self.twin(), device_id_type=MESH)
        above, below = self.own < self.lines - 1, self.own > 0

        @pl.when(above)
        def _():
            pl.semaphore_signal(barrier, 1, device_id=self.line(1), device_id_type=MESH)

        @pl.when(below)
        def _():
            pl.semaphore_signal(barrier, 1, device_id=self.line(-1), device_id_type=MESH)

        ends = lax.div(self.own, self.lines - 1) + 1 - lax.div(self.own + self.lines - 1, self.lines)
        pl.semaphore_wait(barrier, GROUP + 2 - ends)


class Staged:
    def __init__(self, sems):
        self.sems, self.used, self.loads, self.stores = sems, 0, [], []

    def add(self, source, middle, target):
        load = pltpu.make_async_copy(source, middle, self.sems.at[self.used])
        store = pltpu.make_async_copy(middle, target, self.sems.at[self.used + 1])
        self.used += 2
        load.start()
        self.loads.append((load, store))

    def forward(self):
        for load, store in self.loads:
            load.wait()
            store.start()
            self.stores.append(store)
        self.loads = []

    def finish(self):
        for store in self.stores:
            store.wait()


def line_hop(wires, seat, arrays, hop):
    lines = seat.lines
    for blocks, arrivals in arrays:
        for step in (1, -1):
            from_block = seat.own - step * (hop - 1)
            into = seat.own + step
            ok = (from_block >= 0) & (from_block < lines) & (into >= 0) & (into < lines)
            block = blocks.at[lax.rem(from_block + lines, lines)]
            wires.send(
                block, block, arrivals.at[lax.rem(from_block + lines, lines)], seat.line(step), ok
            )


def line_landed(wires, seat, arrays, hop):
    lines = seat.lines
    for blocks, arrivals in arrays:
        for step in (1, -1):
            block = seat.own - step * hop
            ok = (block >= 0) & (block < lines)
            block = lax.rem(block + lines, lines)
            wires.arrived(blocks.at[block], arrivals.at[block], seat.twin(), ok)


def spread_own(wires, seat, own, rows, arrivals):
    for key in range(1, GROUP):
        wires.send(own, rows.at[0, key], arrivals.at[0, key], seat.mate(key))
    wires.send(own, rows.at[1, 0], arrivals.at[1, 0], seat.twin())


def spread_on(wires, seat, rows, arrivals):
    for key in range(1, GROUP):
        wires.arrived(rows.at[0, key], arrivals.at[0, key], seat.twin())
        wires.send(rows.at[0, key], rows.at[1, key], arrivals.at[1, key], seat.twin())


def spread_landed(wires, seat, rows, arrivals):
    for key in range(GROUP):
        wires.arrived(rows.at[1, key], arrivals.at[1, key], seat.twin())


def whole_gain(gains, which, rows):
    members = gains.shape[0]
    width = members * rows
    lane = lax.broadcasted_iota(jnp.int32, (1, LANES), 1)
    chunks = []
    for start in range(0, width, LANES):
        block = start // rows
        shift = block * rows - start
        chunk = gains[block, which : which + 1, :].astype(jnp.float32)
        chunk = pltpu.roll(chunk, shift % LANES, 1) if shift else chunk
        edge = rows + shift
        while edge < LANES and block + 1 < members:
            block += 1
            more = gains[block, which : which + 1, :].astype(jnp.float32)
            more = pltpu.roll(more, edge, 1) if edge % LANES else more
            chunk = jnp.where(lane < edge, chunk, more)
            edge += rows
        chunks.append(chunk)
    return jnp.concatenate(chunks, axis=1)


def turned(values, cosine, sine):
    half = HD // 2
    lane = lax.broadcasted_iota(jnp.int32, values.shape, 1)
    ahead = pltpu.roll(values, LANES - half, 1)
    behind = pltpu.roll(values, half, 1)
    other = jnp.where(lax.rem(lane, HD) < half, ahead, behind)
    return values * cosine + other * sine


def masked_scores(query, key):
    scores = lax.dot_general(
        query, key, (((1,), (1,)), ((), ())), preferred_element_type=jnp.float32
    ) * (HD**-0.5)
    row = lax.broadcasted_iota(jnp.int32, scores.shape, 0)
    column = lax.broadcasted_iota(jnp.int32, scores.shape, 1)
    return jnp.where(row >= column, scores, -jnp.inf)


def probabilities(query, key):
    scores = masked_scores(query, key)
    top = jnp.max(scores, axis=1, keepdims=True)
    log_norm = top + jnp.log(jnp.sum(jnp.exp(scores - top), axis=1, keepdims=True))
    return jnp.exp(scores - log_norm)


def norm_rows(source, start, count):
    values = source[pl.ds(start, count), :].astype(jnp.float32)
    inverse = lax.rsqrt(jnp.mean(values * values, axis=1, keepdims=True) + EPSILON)
    return values, inverse


STEP = 32


def attend_forward(normed, narrow, raw, heads, attended, tables):
    pairs = attended.shape[1] // LANES
    raw[...] = jnp.dot(normed[...], narrow[...], preferred_element_type=jnp.float32)
    last = pairs * LANES
    heads[:, last:] = turned(raw[:, last:], tables[2], tables[3]).astype(jnp.bfloat16)

    def pair(at, carry):
        lanes = pl.ds(pl.multiple_of(at * LANES, LANES), LANES)
        query = turned(raw[:, lanes], tables[0], tables[1]).astype(jnp.bfloat16)
        heads[:, lanes] = query
        key, value = heads[:, last : last + HD], heads[:, last + HD : last + 2 * HD]
        parts = []
        for head in range(LANES // HD):
            probs = probabilities(query[:, head * HD : (head + 1) * HD], key)
            parts.append(
                jnp.dot(probs.astype(jnp.bfloat16), value, preferred_element_type=jnp.float32)
            )
        attended[:, lanes] = jnp.concatenate(parts, axis=1).astype(jnp.bfloat16)
        return carry

    lax.fori_loop(0, pairs, pair, 0)


def front_kernel(
    lines,
    gains,
    narrow,
    out,
    gate,
    up,
    down,
    inputs,
    cots,
    tables,
    gains_rows,
    narrow_full,
    out_full,
    wide,
    downs,
    cot_rows,
    rows,
    normed_one,
    heads_out,
    attended_out,
    residual_out,
    gains_v,
    narrow_v,
    out_v,
    pieces,
    shard_v,
    down_v,
    seq_v,
    cot_v,
    gain_v,
    tables_v,
    normed_v,
    raw_v,
    heads_v,
    attended_v,
    away_v,
    come_v,
    residual_v,
    second_v,
    stage_sem,
    load_sem,
    store_sem,
    send_sem,
    block_sem,
    mix_sem,
    line_sem,
    cot_sem,
    row_sem,
    seq_sem,
):
    seat = Seat(lines)
    wires, staged = Wires(send_sem), Staged(stage_sem)
    index, own, place, core = seat.index, seat.own, seat.place, seat.core
    count, half = narrow.shape[0], inputs.shape[0]
    out_count = out.shape[0]

    def slot(target, block):
        if target is gains_v:
            return gains_v.at[block]
        size = count if target is narrow_v else out_count
        return target.at[pl.ds(pl.multiple_of(block * size, 16), size)]

    def half_of(target, which):
        return target.at[pl.ds(pl.multiple_of(which * half, half), half)]

    loads = [
        pltpu.make_async_copy(source, target, load_sem.at[at])
        for at, (source, target) in enumerate(
            (
                (gains, slot(gains_v, index)),
                (narrow, slot(narrow_v, index)),
                (out, slot(out_v, index)),
                (inputs, half_of(seq_v, core)),
                (tables, tables_v),
                (gate, shard_v.at[0]),
                (up, shard_v.at[1]),
            )
        )
    ]
    for load in loads:
        load.start()
    staged.add(down, down_v, downs.at[own])
    staged.add(cots, cot_v, cot_rows.at[0, 0])
    seat.greet()
    whole = ((gains, gains_v, 0, 1, 2), (narrow, narrow_v, 1, 1, 2), (out, out_v, 2, 2, 1))

    def block_of(at, key=0):
        return lax.rem(at + lines, lines) * GROUP + (flipped(place, key) if key else place)

    def pass_on(target, which, block, device, ok=None):
        wires.send(slot(target, block), slot(target, block), block_sem.at[which, block], device, ok)

    def landed(target, which, block, ok=None):
        wires.arrived(slot(target, block), block_sem.at[which, block], seat.twin(), ok)

    for source, target, which, first, second in whole:
        for step in (1, -1):
            ok = (own + step >= 0) & (own + step < lines)
            wires.send(
                source, slot(target, index), block_sem.at[which, index], seat.line(step), ok
            )
        for key in (first, second):
            wires.send(source, slot(target, index), block_sem.at[which, index], seat.mate(key))
    wires.send(inputs, half_of(seq_v, core), seq_sem.at[0], seat.twin())
    for load in loads[5:]:
        load.wait()
    share, unit_rows = down.shape[0] * lines, down.shape[0]
    padded = pieces.shape[2] // 2
    fill = jnp.zeros((count, padded - share), pieces.dtype)
    for which in range(2):
        shard = shard_v[which]
        for other in range(GROUP):
            parts = []
            for at in range(lines):
                first = at * share + other * unit_rows
                parts.append(shard[:, first : first + unit_rows])
            pieces[other, :, which * padded : (which + 1) * padded] = jnp.concatenate(
                parts + [fill], axis=1
            )
    for key in range(1, GROUP):
        wires.send(
            pieces.at[flipped(place, key)], wide.at[own, place], mix_sem.at[key], seat.mate(key)
        )
    placed = pltpu.make_async_copy(pieces.at[place], wide.at[own, place], load_sem.at[7])
    placed.start()
    staged.forward()
    for hop in range(1, lines):
        for _, target, which, first, second in whole:
            for step in (1, -1):
                at = own - step * hop
                ok = (at >= 0) & (at < lines)
                block = block_of(at)
                landed(target, which, block, ok)
                onward = ok & (own + step >= 0) & (own + step < lines)
                pass_on(target, which, block, seat.line(step), onward)
                for key in (first, second):
                    pass_on(target, which, block, seat.mate(key), ok)
        if hop == 1:
            for _, target, which, first, second in whole:
                block = block_of(own, first)
                landed(target, which, block)
                pass_on(target, which, block, seat.mate(second))
    staged.finish()
    placed.wait()
    for key in range(1, GROUP):
        wires.arrived(wide.at[own, flipped(place, key)], mix_sem.at[key], seat.twin())
    ffn = ((wide, line_sem.at[0]), (downs, line_sem.at[1]))
    line_hop(wires, seat, ffn, 1)
    for hop in range(1, lines):
        for _, target, which, first, second in whole:
            for step in (1, -1):
                at = own - step * hop
                ok = (at >= 0) & (at < lines)
                block = block_of(at, first)
                landed(target, which, block, ok)
                pass_on(target, which, block, seat.mate(second), ok)
    spread_own(wires, seat, cots, cot_rows, cot_sem)
    for load in loads[:5]:
        load.wait()
    wires.arrived(half_of(seq_v, 1 - core), seq_sem.at[0], seat.twin())
    for _, target, which, first, second in whole:
        for at in range(lines):
            for key in (second, GROUP - 1):
                landed(target, which, block_of(at, key))
    stores = []

    def put(source, target):
        store = pltpu.make_async_copy(source, target, store_sem.at[len(stores)])
        store.start()
        stores.append(store)

    put(narrow_v, narrow_full)
    put(out_v, out_full)
    for which in range(2):
        gain = whole_gain(gains_v, which, count)
        gain_v[pl.ds(which * 8, 8), :] = jnp.broadcast_to(gain, (8, gain.shape[1]))
    put(gain_v, gains_rows)

    def norm_one(at, carry):
        start = pl.multiple_of(at * STEP, STEP)
        values, inverse = norm_rows(seq_v, start, STEP)
        normed_v[pl.ds(start, STEP), :] = (values * inverse * gain_v[0:1, :]).astype(jnp.bfloat16)
        return carry

    lax.fori_loop(0, 2 * half // STEP, norm_one, 0)
    put(normed_v, normed_one)
    line_landed(wires, seat, ffn, 1)
    line_hop(wires, seat, ffn, 2)
    attend_forward(normed_v, narrow_v, raw_v, heads_v, attended_v, tables_v)
    put(heads_v, heads_out)
    put(attended_v, attended_out)

    def part_of(which):
        rows_of = attended_v[pl.ds(pl.multiple_of(which * half, half), half), :]
        return jnp.dot(rows_of, out_v[...], preferred_element_type=jnp.float32)

    away_v[...] = part_of(1 - core)
    wires.send(away_v, come_v, seq_sem.at[1], seat.twin())
    residual_v[...] = part_of(core)
    wires.arrived(come_v, seq_sem.at[1], seat.twin())

    def norm_two(at, carry):
        start = pl.multiple_of(at * STEP, STEP)
        span = pl.ds(start, STEP)
        values = seq_v[pl.ds(pl.multiple_of(core * half + start, STEP), STEP), :]
        residual_v[span, :] = values.astype(jnp.float32) + (residual_v[span, :] + come_v[span, :])
        values, inverse = norm_rows(residual_v, start, STEP)
        second_v[span, :] = (values * inverse * gain_v[8:9, :]).astype(jnp.bfloat16)
        return carry

    lax.fori_loop(0, half // STEP, norm_two, 0)
    spread_own(wires, seat, second_v, rows, row_sem)
    put(residual_v, residual_out)
    put(second_v, rows.at[0, 0])
    spread_on(wires, seat, cot_rows, cot_sem)
    line_landed(wires, seat, ffn, 2)
    for hop in range(3, lines):
        line_hop(wires, seat, ffn, hop)
    spread_on(wires, seat, rows, row_sem)
    spread_landed(wires, seat, cot_rows, cot_sem)
    spread_landed(wires, seat, rows, row_sem)
    for hop in range(3, lines):
        line_landed(wires, seat, ffn, hop)
    for store in stores:
        store.wait()
    wires.drain()


ANY = pl.BlockSpec(memory_space=pl.ANY)
HBM = pl.BlockSpec(memory_space=pltpu.HBM)


def front(gains, narrow, out, gate, up, down, inputs, cots, tables, padded):
    members = lax.axis_size("dp")
    lines = members // GROUP
    bf16, f32 = gains.dtype, jnp.float32
    sources = (gains, narrow, out, gate, up, down, inputs, cots, tables)
    pieces = jax.ShapeDtypeStruct((GROUP, gate.shape[0], 2 * padded), bf16)
    _, cols = narrow.shape
    half, width = inputs.shape
    depth = members * out.shape[0]
    shape = jax.ShapeDtypeStruct
    results = [
        shape((16, width), f32),
        shape((width, cols), bf16),
        shape((depth, width), bf16),
        shape((lines,) + pieces.shape, bf16),
        shape((lines,) + down.shape, bf16),
        shape((2, GROUP, half, width), bf16),
        shape((2, GROUP, half, width), bf16),
        shape((2 * half, width), bf16),
        shape((2 * half, cols), bf16),
        shape((2 * half, depth), bf16),
        shape((half, width), f32),
    ]
    whole = 3
    sends = whole * (4 + (lines - 1) * 2 * 3 + 1 + (lines - 1) * 2) + 3 + 2 + 4 * (lines - 1) + 2 * 7
    dma = pltpu.SemaphoreType.DMA
    vmem = pltpu.VMEM
    return pl.pallas_call(
        functools.partial(front_kernel, lines),
        out_shape=results,
        in_specs=[ANY] * len(sources),
        out_specs=[HBM] * len(results),
        scratch_shapes=[
            vmem((members,) + gains.shape, bf16),
            vmem((width, cols), bf16),
            vmem((depth, width), bf16),
            vmem(pieces.shape, bf16),
            vmem((2,) + gate.shape, bf16),
            vmem(down.shape, bf16),
            vmem((2 * half, width), bf16),
            vmem(cots.shape, bf16),
            vmem((16, width), f32),
            vmem(tables.shape, f32),
            vmem((2 * half, width), bf16),
            vmem((2 * half, cols), f32),
            vmem((2 * half, cols), bf16),
            vmem((2 * half, depth), bf16),
            vmem((half, width), f32),
            vmem((half, width), f32),
            vmem((half, width), f32),
            vmem((half, width), bf16),
            dma((4,)),
            dma((8,)),
            dma((8,)),
            dma((sends,)),
            dma((whole, members)),
            dma((GROUP,)),
            dma((2, lines)),
            dma((2, GROUP)),
            dma((2, GROUP)),
            dma((2,)),
        ],
        compiler_params=pltpu.CompilerParams(
            collective_id=0, has_side_effects=True, vmem_limit_bytes=60 << 20
        ),
        name="front",
    )(*sources)


SPAN = 14.0


def put_scales(tops, rows):
    power = jnp.clip(jnp.ceil(jnp.log2(jnp.maximum(tops, 1e-33))), -98.0, 126.0) - SPAN
    shape = rows.shape[1:]
    row = lax.broadcasted_iota(jnp.int32, shape, 0).astype(jnp.float32)
    rows[0] = jnp.broadcast_to(jnp.exp2(-power), shape)
    rows[1] = jnp.broadcast_to(jnp.exp2(power), shape)
    rows[2] = jnp.exp2(jnp.floor((power + row) * 0.125))


def tops_of(values):
    return jnp.max(jnp.abs(values), axis=0, keepdims=True)


def meet(seat):
    barrier = pltpu.get_barrier_semaphore()
    others = [seat.mate(key) for key in range(1, GROUP)]
    others += [seat.peer(key) for key in range(1, seat.lines)] + [seat.twin()]
    for other in others:
        pl.semaphore_signal(barrier, 1, device_id=other, device_id_type=MESH)
    pl.semaphore_wait(barrier, len(others))


def meet_twin(seat):
    barrier = pltpu.get_barrier_semaphore()
    pl.semaphore_signal(barrier, 1, device_id=seat.twin(), device_id_type=MESH)
    pl.semaphore_wait(barrier, 1)


def send_bounds(wires, mine, come, sems, devices, first):
    for at, device in enumerate(devices):
        wires.send(mine, come.at[first + at], sems.at[first + at], device)


def take_bounds(wires, seat, mine, come, sems, devices, first):
    bounds = mine[...]
    for at in range(len(devices)):
        wires.arrived(come.at[first + at], sems.at[first + at], seat.twin())
        bounds = jnp.maximum(bounds, come[first + at])
    return bounds


class Moves:
    def __init__(self, sems):
        self.sems, self.used, self.open = sems, 0, []

    def start(self, source, target):
        copy = pltpu.make_async_copy(source, target, self.sems.at[self.used])
        copy.start()
        self.used += 1
        return copy

    def put(self, source, target):
        self.open.append(self.start(source, target))

    def finish(self):
        for copy in self.open:
            copy.wait()


def dot_rows(left, right):
    return jnp.dot(left, right, preferred_element_type=jnp.float32)


def dot_across(left, right):
    return lax.dot_general(left, right, (((1,), (1,)), ((), ())), preferred_element_type=jnp.float32)


def dot_down(left, right):
    return lax.dot_general(left, right, (((0,), (0,)), ((), ())), preferred_element_type=jnp.float32)


CHUNK = 256


def sum_up(near, come):
    def step(at, carry):
        span = pl.ds(pl.multiple_of(at * STEP, STEP), STEP)
        near[span, :] = near[span, :] + come[span, :]
        return carry

    lax.fori_loop(0, near.shape[0] // STEP, step, 0)


def units_kernel(
    lines,
    share,
    rows,
    cots,
    wide,
    down,
    gains,
    hidden_out,
    back_out,
    away_out,
    wide_out,
    factors,
    wide_factors,
    rows_v,
    cots_v,
    wide_v,
    down_v,
    gains_v,
    hidden_v,
    both_v,
    far_v,
    near_v,
    come_v,
    wide_grad_v,
    mine_v,
    bounds_v,
    factors_v,
    wide_factors_v,
    move_sem,
    send_sem,
    come_sem,
    bound_sem,
):
    seat = Seat(lines)
    moves = Moves(move_sem)
    count, width = rows.shape
    half = count // 2
    padded = hidden_v.shape[1]
    chunks = half // CHUNK
    loads = []
    for source, target in ((wide, wide_v), (down, down_v.at[pl.ds(0, share)]), (gains, gains_v)):
        loads.append(moves.start(source, target))
    for at in range(2 * chunks):
        span = pl.ds((at * CHUNK + half) % count, CHUNK)
        loads.append(moves.start(rows.at[span], rows_v.at[span]))
        loads.append(moves.start(cots.at[span], cots_v.at[span]))
    down_v[share:, :] = jnp.zeros((padded - share, width), down_v.dtype)
    meet(seat)
    for load in loads[:3]:
        load.wait()
    wires = Wires(send_sem)
    back_top = jnp.zeros((1, width), jnp.float32)
    cot_top = jnp.zeros((1, width), jnp.bfloat16)
    hidden_sum = jnp.zeros((1, padded), jnp.float32)
    hidden_top = jnp.zeros((1, 1), jnp.float32)
    both_sum = jnp.zeros((1, 2 * padded), jnp.float32)
    for at in range(2 * chunks):
        loads[3 + 2 * at].wait()
        loads[4 + 2 * at].wait()
        start = (at * CHUNK + half) % count
        span = pl.ds(start, CHUNK)
        raw = dot_rows(rows_v[span, :], wide_v[...])
        hidden_cot = dot_across(cots_v[span, :], down_v[...])
        gate, up = raw[:, :padded], raw[:, padded:]
        sigma = jax.nn.sigmoid(gate)
        hidden = (gate * sigma * up).astype(jnp.bfloat16)
        hidden_v[span, :] = hidden
        both_v[span, :padded] = (
            hidden_cot * up * sigma * (1.0 + gate * (1.0 - sigma))
        ).astype(jnp.bfloat16)
        both_v[span, padded:] = (hidden_cot * gate * sigma).astype(jnp.bfloat16)
        part = dot_across(both_v[span, :], wide_v[...])
        back_top = jnp.maximum(back_top, tops_of(part))
        if start >= half:
            piece = pl.ds(start - half, CHUNK)
            far_v[piece, :] = part
            wires.send(far_v.at[piece], come_v.at[piece], come_sem.at[at], seat.twin())
        else:
            near_v[span, :] = part
        hidden_size = jnp.abs(hidden.astype(jnp.float32))
        hidden_sum += jnp.sum(hidden_size, axis=0, keepdims=True)
        across = jnp.sum(hidden_size, axis=1, keepdims=True)
        hidden_top = jnp.maximum(hidden_top, jnp.max(across, axis=0, keepdims=True))
        both_sum += jnp.sum(jnp.abs(both_v[span, :].astype(jnp.float32)), axis=0, keepdims=True)
        cot_top = jnp.maximum(cot_top, jnp.max(jnp.abs(cots_v[span, :]), axis=0, keepdims=True))
    gain_top = jnp.max(jnp.abs(gains_v[8:9, :]), axis=1, keepdims=True)
    down_top = jnp.max(jnp.abs(down_v[...]), axis=0, keepdims=True).astype(jnp.float32)
    mine_v[0:1, :] = 2.0 * back_top
    mine_v[1:2, :] = (
        1.1 * jnp.max(hidden_sum, axis=1, keepdims=True) * cot_top.astype(jnp.float32)
    )
    mine_v[2:3, :] = 2.2 * hidden_top * down_top
    mine_v[3:4, :] = jnp.zeros((1, width), jnp.float32)
    mine_v[3:4, : 2 * padded] = (1.1 * width**0.5) * gain_top * both_sum
    mine_v[4:8, :] = jnp.zeros((4, width), jnp.float32)
    mates = [seat.mate(key) for key in range(1, GROUP)]
    others = [seat.peer(key) for key in range(1, lines)] + [seat.twin()]
    send_bounds(wires, mine_v.at[pl.ds(0, 8)], bounds_v, bound_sem, mates, 0)
    moves.put(hidden_v, hidden_out)

    def wide_step(at, carry):
        span = pl.ds(pl.multiple_of(at * CHUNK, CHUNK), CHUNK)
        wide_grad_v[span, :] = dot_down(rows_v[:, span], both_v[...])
        return carry

    lax.fori_loop(0, width // CHUNK // 2, wide_step, 0)
    mine_v[8:, :] = take_bounds(
        wires, seat, mine_v.at[pl.ds(0, 8)], bounds_v, bound_sem, mates, 0
    )
    send_bounds(wires, mine_v.at[pl.ds(8, 8)], bounds_v, bound_sem, others, len(mates))
    lax.fori_loop(width // CHUNK // 2, width // CHUNK, wide_step, 0)
    moves.put(wide_grad_v, wide_out)
    for at in range(chunks):
        wires.arrived(come_v.at[pl.ds(at * CHUNK, CHUNK)], come_sem.at[at], seat.twin())
    bounds = take_bounds(
        wires, seat, mine_v.at[pl.ds(8, 8)], bounds_v, bound_sem, others[:-1], len(mates)
    )
    last = len(mates) + len(others) - 1
    wires.arrived(bounds_v.at[last], bound_sem.at[last], seat.twin())
    for at in range(3):
        bound = bounds[at : at + 1]
        if at != 1:
            bound = jnp.maximum(bound, bounds_v[last, at : at + 1, :])
        put_scales(bound, factors_v.at[at])
    put_scales(bounds[3:4, : 2 * padded], wide_factors_v)
    each = half // GROUP
    sum_up(near_v.at[pl.ds(0, each)], come_v.at[pl.ds(0, each)])
    moves.put(near_v.at[pl.ds(0, each)], back_out)

    def scaled(at, carry):
        span = pl.ds(pl.multiple_of(each + at * STEP, STEP), STEP)
        near_v[span, :] = (near_v[span, :] + come_v[span, :]) * factors_v[0, 0, 0:1, :]
        return carry

    lax.fori_loop(0, (half - each) // STEP, scaled, 0)
    for at in range(1, GROUP):
        moves.put(near_v.at[pl.ds(at * each, each)], away_out.at[at - 1])
    moves.put(factors_v, factors)
    moves.put(wide_factors_v, wide_factors)
    moves.finish()
    wires.drain()


def units(rows, cots, wide, down, gains, padded):
    count, width = rows.shape
    half = count // 2
    share = down.shape[0]
    lines = lax.axis_size("dp") // GROUP
    f32, bf16 = jnp.float32, rows.dtype
    shape, vmem, dma = jax.ShapeDtypeStruct, pltpu.VMEM, pltpu.SemaphoreType.DMA
    chunks = half // CHUNK
    rounds = GROUP - 1 + lines
    return pl.pallas_call(
        functools.partial(units_kernel, lines, share),
        out_shape=[
            shape((count, padded), bf16),
            shape((half // GROUP, width), f32),
            shape((GROUP - 1, half // GROUP, width), f32),
            shape((width, 2 * padded), f32),
            shape((3, 3, 8, width), f32),
            shape((3, 8, 2 * padded), f32),
        ],
        in_specs=[HBM] * 5,
        out_specs=[HBM] * 6,
        scratch_shapes=[
            vmem((count, width), bf16),
            vmem((count, width), bf16),
            vmem(wide.shape, bf16),
            vmem((padded, width), bf16),
            vmem(gains.shape, f32),
            vmem((count, padded), bf16),
            vmem((count, 2 * padded), bf16),
            vmem((half, width), f32),
            vmem((half, width), f32),
            vmem((half, width), f32),
            vmem((width, 2 * padded), f32),
            vmem((16, width), f32),
            vmem((rounds, 8, width), f32),
            vmem((3, 3, 8, width), f32),
            vmem((3, 8, 2 * padded), f32),
            dma((3 + 4 * chunks + GROUP + 5,)),
            dma((chunks + rounds,)),
            dma((chunks,)),
            dma((rounds,)),
        ],
        compiler_params=pltpu.CompilerParams(
            collective_id=1, has_side_effects=True, vmem_limit_bytes=60 << 20
        ),
        cost_estimate=pl.CostEstimate(flops=10**10, bytes_accessed=2 * 10**7, transcendentals=0),
        name="units",
    )(rows, cots, wide, down, gains)


def grads_kernel(
    lines,
    share,
    cots,
    hidden,
    down,
    down_out,
    forth_out,
    cots_v,
    hidden_v,
    down_v,
    down_grad_v,
    far_v,
    near_v,
    come_v,
    move_sem,
    send_sem,
    come_sem,
):
    seat = Seat(lines)
    moves = Moves(move_sem)
    count, width = cots.shape
    half = count // 2
    padded = hidden_v.shape[1]
    pairs = ((hidden, hidden_v), (down, down_v.at[pl.ds(0, share)]), (cots, cots_v))
    loads = [moves.start(source, target) for source, target in pairs]
    down_v[share:, :] = jnp.zeros((padded - share, width), down_v.dtype)
    meet_twin(seat)
    wires = Wires(send_sem)
    for load in loads[:2]:
        load.wait()
    far_v[...] = dot_rows(hidden_v[half:, :], down_v[...])
    wires.send(far_v, come_v, come_sem.at[0], seat.twin())
    loads[2].wait()

    def down_step(at, carry):
        span = pl.ds(pl.multiple_of(at * LANES, LANES), LANES)
        down_grad_v[span, :] = dot_down(hidden_v[:, span], cots_v[...])
        return carry

    lax.fori_loop(0, padded // LANES, down_step, 0)
    moves.put(down_grad_v.at[pl.ds(0, share)], down_out)
    near_v[...] = dot_rows(hidden_v[:half, :], down_v[...])
    wires.arrived(come_v, come_sem.at[0], seat.twin())
    sum_up(near_v, come_v)
    moves.put(near_v, forth_out)
    moves.finish()
    wires.drain()


def grads(cots, hidden, down):
    count, width = cots.shape
    half = count // 2
    padded = hidden.shape[1]
    share = down.shape[0]
    lines = lax.axis_size("dp") // GROUP
    f32, bf16 = jnp.float32, cots.dtype
    shape, vmem, dma = jax.ShapeDtypeStruct, pltpu.VMEM, pltpu.SemaphoreType.DMA
    return pl.pallas_call(
        functools.partial(grads_kernel, lines, share),
        out_shape=[shape((share, width), f32), shape((half, width), f32)],
        in_specs=[HBM] * 3,
        out_specs=[HBM] * 2,
        scratch_shapes=[
            vmem((count, width), bf16),
            vmem((count, padded), bf16),
            vmem((padded, width), bf16),
            vmem((padded, width), f32),
            vmem((half, width), f32),
            vmem((half, width), f32),
            vmem((half, width), f32),
            dma((3 + 2,)),
            dma((1,)),
            dma((1,)),
        ],
        compiler_params=pltpu.CompilerParams(
            collective_id=2, has_side_effects=True, vmem_limit_bytes=60 << 20
        ),
        cost_estimate=pl.CostEstimate(flops=10**10, bytes_accessed=2 * 10**7, transcendentals=0),
        name="grads",
    )(cots, hidden, down)


def split_gain(flat, block, rows):
    start = block * rows
    chunk, offset = start // LANES, start % LANES
    lane = lax.broadcasted_iota(jnp.int32, (1, LANES), 1)
    piece = flat[:, chunk * LANES : (chunk + 1) * LANES]
    piece = pltpu.roll(piece, LANES - offset, 1) if offset else piece
    if offset + rows > LANES:
        more = flat[:, (chunk + 1) * LANES : (chunk + 2) * LANES]
        piece = jnp.where(lane < LANES - offset, piece, pltpu.roll(more, LANES - offset, 1))
    return jnp.where(lane < rows, piece, 0.0)


def norm_back(values, inverse, gain, cot):
    scaled = cot * gain
    share = jnp.mean(scaled * values, axis=1, keepdims=True)
    return inverse * scaled - values * (inverse * inverse * inverse) * share


def folded(values):
    return jnp.sum(values.reshape(-1, 8, values.shape[1]), axis=0)


def step_rows(start, which, half):
    return pl.ds(pl.multiple_of(which * half + start, STEP), STEP)


def half_of(target, which):
    half = target.shape[0] // 2
    return target.at[pl.ds(pl.multiple_of(which * half, half), half)]


def turn_kernel(
    lines,
    come,
    back_own,
    factors,
    residual,
    gains,
    cots,
    attended,
    out_full,
    residual_cot,
    mix_out,
    out_grad,
    sums_out,
    out_factors,
    second_v,
    own_v,
    factors_v,
    residual_v,
    gains_v,
    cots_v,
    attended_v,
    out_v,
    seq_v,
    mix_v,
    out_grad_v,
    sums_v,
    out_rows,
    move_sem,
    send_sem,
    come_sem,
):
    seat = Seat(lines)
    core = seat.core
    moves = Moves(move_sem)
    half, width = residual.shape
    depth = attended.shape[1]
    bf16 = attended_v.dtype
    pairs = (
        (come, second_v),
        (back_own, own_v),
        (factors, factors_v),
        (residual, residual_v),
        (gains, gains_v),
        (cots, cots_v),
        (attended, attended_v),
        (out_full, out_v),
    )
    loads = [moves.start(source, target) for source, target in pairs]
    meet_twin(seat)
    wires = Wires(send_sem)
    for load in loads[:6]:
        load.wait()
    sums_v[...] = jnp.zeros_like(sums_v)

    def norm_two(at, carry):
        start = pl.multiple_of(at * STEP, STEP)
        span = pl.ds(start, STEP)
        values, inverse = norm_rows(residual_v, start, STEP)
        cot = own_v[span, :] + second_v[span, :] * factors_v[0, 1, 0:1, :]
        sums_v[...] += folded(cot * values * inverse)
        total = cots_v[span, :].astype(jnp.float32) + norm_back(
            values, inverse, gains_v[8:9, :], cot
        )
        residual_v[span, :] = total
        seq_v[step_rows(start, core, half), :] = total.astype(bf16)
        return carry

    lax.fori_loop(0, half // STEP, norm_two, 0)
    wires.send(half_of(seq_v, core), half_of(seq_v, core), come_sem.at[0], seat.twin())
    moves.put(residual_v, residual_cot)
    moves.put(sums_v, sums_out)
    for load in loads[6:]:
        load.wait()
    wires.arrived(half_of(seq_v, 1 - core), come_sem.at[0], seat.twin())

    def out_step(at, top):
        span = pl.ds(pl.multiple_of(at * LANES, LANES), LANES)
        part = dot_down(attended_v[:, span], seq_v[...])
        out_grad_v[span, :] = part
        return jnp.maximum(top, tops_of(part))

    top = lax.fori_loop(0, depth // LANES, out_step, jnp.zeros((1, width), jnp.float32))
    moves.put(out_grad_v, out_grad)
    put_scales(top, out_rows)
    moves.put(out_rows, out_factors)
    mix_v[...] = dot_across(seq_v[...], out_v[...]).astype(bf16)
    moves.put(mix_v, mix_out)
    moves.finish()
    wires.drain()


def turn(come, back_own, factors, residual, gains, cots, attended, out_full):
    lines = lax.axis_size("dp") // GROUP
    half, width = residual.shape
    depth = attended.shape[1]
    f32, bf16 = jnp.float32, attended.dtype
    shape, vmem, dma = jax.ShapeDtypeStruct, pltpu.VMEM, pltpu.SemaphoreType.DMA
    sources = (come, back_own, factors, residual, gains, cots, attended, out_full)
    return pl.pallas_call(
        functools.partial(turn_kernel, lines),
        out_shape=[
            shape((half, width), f32),
            shape((2 * half, depth), bf16),
            shape((depth, width), f32),
            shape((8, width), f32),
            shape((3, 8, width), f32),
        ],
        in_specs=[HBM] * len(sources),
        out_specs=[HBM] * 5,
        scratch_shapes=[vmem(part.shape, part.dtype) for part in sources]
        + [
            vmem((2 * half, width), bf16),
            vmem((2 * half, depth), bf16),
            vmem((depth, width), f32),
            vmem((8, width), f32),
            vmem((3, 8, width), f32),
            dma((len(sources) + 5,)),
            dma((1,)),
            dma((1,)),
        ],
        compiler_params=pltpu.CompilerParams(
            collective_id=3, has_side_effects=True, vmem_limit_bytes=24 << 20
        ),
        cost_estimate=pl.CostEstimate(flops=10**10, bytes_accessed=2 * 10**7, transcendentals=0),
        name="turn",
    )(*sources)


def rear_kernel(
    lines,
    members,
    residual_cot,
    mix,
    sums,
    gains,
    inputs,
    heads,
    attended,
    narrow_full,
    normed,
    tables,
    input_grad,
    narrow_grad,
    narrow_factors,
    residual_v,
    mix_v,
    sums_in_v,
    gains_v,
    inputs_v,
    heads_v,
    attended_v,
    narrow_v,
    normed_v,
    tables_v,
    cot_v,
    pair_v,
    far_v,
    near_v,
    come_v,
    narrow_grad_v,
    sums_v,
    sums_come_v,
    gain_grad_v,
    narrow_rows,
    move_sem,
    send_sem,
    come_sem,
):
    seat = Seat(lines)
    core = seat.core
    moves = Moves(move_sem)
    half, width = inputs.shape
    depth = attended.shape[1]
    cols = heads.shape[1]
    count = width // members
    bf16 = heads_v.dtype
    pairs = (
        (mix, mix_v),
        (heads, heads_v),
        (attended, attended_v),
        (tables, tables_v),
        (narrow_full, narrow_v),
        (normed, normed_v),
        (residual_cot, residual_v),
        (sums, sums_in_v),
        (gains, gains_v),
        (inputs, inputs_v),
    )
    loads = [moves.start(source, target) for source, target in pairs]
    meet_twin(seat)
    wires = Wires(send_sem)
    for load in loads[:4]:
        load.wait()
    pair_v[...] = jnp.zeros_like(pair_v)

    def pair(at, carry):
        lanes = pl.ds(pl.multiple_of(at * LANES, LANES), LANES)
        key, value = heads_v[:, depth : depth + HD], heads_v[:, depth + HD : depth + 2 * HD]
        query_both, mix_both = heads_v[:, lanes], mix_v[:, lanes]
        delta_both = mix_both.astype(jnp.float32) * attended_v[:, lanes].astype(jnp.float32)
        parts = []
        for head in range(LANES // HD):
            own = slice(head * HD, (head + 1) * HD)
            query, mix_own = query_both[:, own], mix_both[:, own]
            probs = probabilities(query, key)
            value_part = dot_down(probs.astype(bf16), mix_own)
            delta = jnp.sum(delta_both[:, own], axis=1, keepdims=True)
            score_cot = (probs * (dot_across(mix_own, value) - delta)).astype(bf16)
            parts.append(dot_rows(score_cot, key) * (HD**-0.5))
            key_part = dot_down(score_cot, query) * (HD**-0.5)
            pair_v[...] += jnp.concatenate([key_part, value_part], axis=1)
        query_cot = turned(jnp.concatenate(parts, axis=1), tables_v[0], -tables_v[1])
        cot_v[:, lanes] = query_cot.astype(bf16)
        return carry

    lax.fori_loop(0, depth // LANES, pair, 0)
    cot_v[:, depth:] = turned(pair_v[...], tables_v[2], -tables_v[3]).astype(bf16)
    for load in loads[4:]:
        load.wait()

    def part_of(which):
        rows_of = cot_v[pl.ds(pl.multiple_of(which * half, half), half), :]
        return dot_across(rows_of, narrow_v[...])

    far_v[...] = part_of(1 - core)
    wires.send(far_v, come_v, come_sem.at[0], seat.twin())
    near_v[...] = part_of(core)

    def narrow_step(at, top):
        span = pl.ds(pl.multiple_of(at * CHUNK, CHUNK), CHUNK)
        part = dot_down(normed_v[:, span], cot_v[...])
        narrow_grad_v[span, :] = part
        return jnp.maximum(top, tops_of(part))

    top = lax.fori_loop(0, width // CHUNK, narrow_step, jnp.zeros((1, cols), jnp.float32))
    for block in range(members):
        moves.put(
            narrow_grad_v.at[pl.ds(block * count, count)], narrow_grad.at[block, pl.ds(0, count)]
        )
    wires.arrived(come_v, come_sem.at[0], seat.twin())
    sums_v[8:, :] = sums_in_v[...]
    sums_v[:8, :] = jnp.zeros_like(sums_in_v)

    def norm_one(at, carry):
        start = pl.multiple_of(at * STEP, STEP)
        span = pl.ds(start, STEP)
        values, inverse = norm_rows(inputs_v, start, STEP)
        cot = near_v[span, :] + come_v[span, :]
        sums_v[:8, :] += folded(cot * values * inverse)
        near_v[span, :] = residual_v[span, :] + norm_back(values, inverse, gains_v[0:1, :], cot)
        return carry

    lax.fori_loop(0, half // STEP, norm_one, 0)
    wires.send(sums_v, sums_come_v, come_sem.at[1], seat.twin())
    moves.put(near_v, input_grad)
    wires.arrived(sums_come_v, come_sem.at[1], seat.twin())
    both = sums_v[...] + sums_come_v[...]
    flat = [jnp.sum(both[8 * at : 8 * at + 8, :], axis=0, keepdims=True) for at in range(2)]
    gain_grad_v[...] = jnp.zeros_like(gain_grad_v)
    for block in range(members):
        for at in range(2):
            piece = split_gain(flat[at], block, count)
            gain_grad_v[block, 0:1, at * LANES : (at + 1) * LANES] = piece
            lanes = slice(at * LANES, (at + 1) * LANES)
            raised = jnp.maximum(top[:, lanes], jnp.abs(piece))
            top = jnp.concatenate(
                [part for part in (top[:, : at * LANES], raised, top[:, (at + 1) * LANES :]) if part.size],
                axis=1,
            )
    moves.put(gain_grad_v, narrow_grad.at[:, pl.ds(count, 8), :])
    put_scales(top, narrow_rows)
    moves.put(narrow_rows, narrow_factors)
    moves.finish()
    wires.drain()


def rear(residual_cot, mix, sums, gains, inputs, heads, attended, narrow_full, normed, tables):
    members = lax.axis_size("dp")
    lines = members // GROUP
    half, width = inputs.shape
    cols = heads.shape[1]
    count = width // members
    f32, bf16 = jnp.float32, heads.dtype
    shape, vmem, dma = jax.ShapeDtypeStruct, pltpu.VMEM, pltpu.SemaphoreType.DMA
    sources = (
        residual_cot,
        mix,
        sums,
        gains,
        inputs,
        heads,
        attended,
        narrow_full,
        normed,
        tables,
    )
    return pl.pallas_call(
        functools.partial(rear_kernel, lines, members),
        out_shape=[
            shape((half, width), f32),
            shape((members, count + 8, cols), f32),
            shape((3, 8, cols), f32),
        ],
        in_specs=[HBM] * len(sources),
        out_specs=[HBM] * 3,
        scratch_shapes=[vmem(part.shape, part.dtype) for part in sources]
        + [
            vmem((2 * half, cols), bf16),
            vmem((2 * half, LANES), f32),
            vmem((half, width), f32),
            vmem((half, width), f32),
            vmem((half, width), f32),
            vmem((width, cols), f32),
            vmem((16, width), f32),
            vmem((16, width), f32),
            vmem((members, 8, cols), f32),
            vmem((3, 8, cols), f32),
            dma((len(sources) + members + 3,)),
            dma((2,)),
            dma((2,)),
        ],
        compiler_params=pltpu.CompilerParams(
            collective_id=4, has_side_effects=True, vmem_limit_bytes=32 << 20
        ),
        cost_estimate=pl.CostEstimate(flops=10**10, bytes_accessed=2 * 10**7, transcendentals=0),
        name="rear",
    )(*sources)


def unshare_kernel(share, lines, pieces, gate, up):
    place = lax.rem(lax.axis_index("dp"), GROUP)
    unit_rows = share // lines
    padded = pieces.shape[2] // 2
    for start, target in ((0, gate), (padded, up)):
        parts = []
        for at in range(lines):
            for other in range(GROUP):
                piece = pieces[flipped(place, other) if other else place]
                first = start + at * unit_rows
                parts.append(piece[:, first : first + unit_rows])
        target[...] = jnp.concatenate(parts, axis=1)


def unshare(pieces, share, lines):
    rows = pieces.shape[1]
    result = jax.ShapeDtypeStruct((rows, GROUP * share), pieces.dtype)
    return pl.pallas_call(
        functools.partial(unshare_kernel, share, lines), out_shape=[result] * 2, name="unshare"
    )(pieces)


def grouped_layer(
    block_input,
    attn_gain,
    query_weight,
    key_weight,
    value_weight,
    output_weight,
    ffn_gain,
    gate_weight,
    up_weight,
    down_weight,
    output_cotangent,
):
    f32, bf16 = jnp.float32, jnp.bfloat16
    members = lax.axis_size("dp")
    lines = members // GROUP
    index = lax.axis_index("dp")
    own, place = index // GROUP, lax.rem(index, GROUP)
    rows, _ = gate_weight.shape
    width = rows * members
    query_cols, key_cols = query_weight.shape[1], key_weight.shape[1]
    unit_rows = down_weight.shape[0]
    share = unit_rows * lines
    padded = whole_up(share, LANES)

    narrow = jnp.concatenate([query_weight, key_weight, value_weight], axis=1)
    cols = narrow.shape[1]
    gains = jnp.stack([attn_gain, ffn_gain])
    gains = jnp.pad(gains, ((0, 6), (0, whole_up(rows, LANES) - rows)))

    length = 2 * block_input.shape[0]
    cosine, sine = rope_tables(length, HD)
    still, none = jnp.ones((length, HD), f32), jnp.zeros((length, HD), f32)
    twice = jnp.concatenate([cosine] * 4, axis=1)
    signed = jnp.concatenate([-sine, sine] * 2, axis=1)
    tables = jnp.stack(
        [
            twice,
            signed,
            jnp.concatenate([twice[:, :HD], still], axis=1),
            jnp.concatenate([signed[:, :HD], none], axis=1),
        ]
    )
    (
        gains_rows,
        narrow_full,
        out_full,
        wide,
        downs,
        cot_rows,
        ffn_rows,
        normed_one,
        heads,
        attn_rows,
        residual,
    ) = front(
        gains,
        narrow,
        output_weight,
        gate_weight,
        up_weight,
        down_weight,
        block_input,
        output_cotangent,
        tables,
        padded,
    )
    cot_rows = cot_rows.reshape(-1, width)
    ffn_rows = ffn_rows.reshape(-1, width)
    wide_full = wide.reshape(width, 2 * padded)
    down_share = downs.reshape(share, width)
    half = block_input.shape[0]

    hidden, back_own, back_away, wide_grad, factors, wide_factors = units(
        ffn_rows, cot_rows, wide_full, down_share, gains_rows, padded
    )
    back_out = [back_away[key].astype(jnp.float16) for key in range(GROUP - 1)]
    back_in = exchanged(back_out, partner)

    wide_grad = after(wide_grad.reshape(lines, GROUP * rows, 2 * padded), *back_out)
    wide_undo = wide_factors[1, :1]
    wide_out, wide_near, wide_second, wide_ended = line_halves(
        wide_grad, wide_factors[0, :1], wide_undo
    )
    hidden = after(hidden, wide_out)
    down_grad, forth_sum = grads(cot_rows, hidden, down_share)
    down_out, down_near, down_second, down_ended = line_halves(
        down_grad.reshape(lines, unit_rows, width), factors[1, 0, :1], factors[1, 1, :1]
    )

    back_in = after(back_in, down_out)
    come = sum(message.astype(f32) for message in back_in)
    forth_sum = after(forth_sum.reshape(GROUP, half, width), come)
    forth_out = [narrowed(forth_sum[key], factors[2, 0, :1]) for key in range(1, GROUP)]
    forth_in = exchanged(forth_out, partner)
    back_own = after(back_own, *forth_out)
    residual_cot, mix, out_grad, sums, out_factors = turn(
        come, back_own, factors, residual, gains_rows, output_cotangent, attn_rows, out_full
    )
    out_grad = out_grad.reshape(lines, GROUP, -1, width)
    out_out = group_messages(out_grad, place, out_factors[0, :1], out_factors[2])
    out_in = exchanged(out_out, partner)
    wide_near = after(wide_near, *out_out)
    wide_next, wide_far = wide_second(wide_near)
    residual_cot = after(residual_cot, wide_next)
    input_grad, narrow_grad, narrow_factors = rear(
        residual_cot,
        mix,
        sums,
        gains_rows,
        block_input,
        heads,
        attn_rows,
        narrow_full,
        normed_one,
        tables,
    )
    narrow_grad = narrow_grad.reshape(lines, GROUP, -1, cols)
    narrow_out = group_messages(narrow_grad, place, narrow_factors[0, :1], narrow_factors[2])
    narrow_in = exchanged(narrow_out, partner)

    down_near = after(down_near, *narrow_out)
    down_next, down_far = down_second(down_near)
    out_in = after(out_in, down_next)
    out_undos = [undo_of(message) for message in out_in]
    out_sum = lax.dynamic_index_in_dim(out_grad, place, 1, keepdims=False)
    out_sum = added_noted(out_sum, out_in, out_undos)
    out_line = line_messages(out_sum, raised(out_factors[1, :1], out_undos), own)
    out_line_in = exchanged(out_line, across)
    wide_far = after(wide_far, *out_line)
    wide_own = wide_ended(wide_near, wide_far).reshape(GROUP, rows, 2 * padded)
    share_out = messages_of(wide_own, 0.25 * wide_factors[0, :1], place)
    forth_in = after(forth_in, *share_out)
    block_output = (residual + added(forth_sum[0], forth_in, factors[2, 1, :1])).astype(bf16)
    narrow_in = after(narrow_in, block_output)
    narrow_undos = [undo_of(message) for message in narrow_in]
    narrow_sum = lax.dynamic_index_in_dim(narrow_grad, place, 1, keepdims=False)
    narrow_sum = added_noted(narrow_sum, narrow_in, narrow_undos)
    narrow_line = line_messages(narrow_sum, raised(narrow_factors[1, :1], narrow_undos), own)
    narrow_line_in = exchanged(narrow_line, across)
    share_in = exchanged(after(share_out, *narrow_line), partner)
    down_far = after(down_far, *narrow_line)
    down_own = down_ended(down_near, down_far)
    share_in = after(share_in, down_own)
    pieces = [lax.dynamic_index_in_dim(wide_own, place, 0, keepdims=False)]
    pieces += [message.astype(f32) * (4.0 * wide_undo) for message in share_in]
    gate_own, up_own = unshare(jnp.stack(pieces), share, lines)
    out_line_in = after(out_line_in, gate_own, up_own)
    out_own = added_noted(
        lax.dynamic_index_in_dim(out_sum, own, 0, keepdims=False),
        out_line_in,
        [undo_of(message) for message in out_line_in],
    )
    narrow_line_in = after(narrow_line_in, out_own)
    narrow_own = added_noted(
        lax.dynamic_index_in_dim(narrow_sum, own, 0, keepdims=False),
        narrow_line_in,
        [undo_of(message) for message in narrow_line_in],
    )
    return (
        block_output,
        input_grad,
        narrow_own[rows, :rows],
        narrow_own[:rows, :query_cols],
        narrow_own[:rows, query_cols : query_cols + key_cols],
        narrow_own[:rows, query_cols + key_cols :],
        out_own,
        narrow_own[rows, LANES : LANES + rows],
        gate_own,
        up_own,
        down_own,
    )


def grouped_shards(*arrays):
    return grouped_layer(*arrays)


def solution(mesh):
    placed = (
        P(("dp", "mp"), None),
        P("dp"),
        P("dp", "mp"),
        P("dp", "mp"),
        P("dp", "mp"),
        P(("mp", "dp"), None),
        P("dp"),
        P("dp", "mp"),
        P("dp", "mp"),
        P(("mp", "dp"), None),
        P(("dp", "mp"), None),
    )
    members = mesh.shape["dp"]
    fits = mesh.shape["mp"] == 2 and members == GROUP * GROUP
    return jax.shard_map(
        grouped_shards if fits else plain_shards,
        mesh=mesh,
        in_specs=placed,
        out_specs=(
            P(("dp", "mp"), None),
            P(("dp", "mp"), None),
            P("dp"),
            P("dp", "mp"),
            P("dp", "mp"),
            P("dp", "mp"),
            P(("mp", "dp"), None),
            P("dp"),
            P("dp", "mp"),
            P("dp", "mp"),
            P(("mp", "dp"), None),
        ),
        check_vma=False,
    )
```
